128 devices in a mesh: gx: 4 (over z), gy: 32 (over y, x, core).
Axes of the slice: x: 4, y: 4, z: 4, core: 2. Of those that a mesh axis runs over, the one named last changes fastest.
Arguments:
- a_blocks: float32 [1024, 4, 128, 128], P(('gx', 'gy')), may hold values from -0.25 to 0.25
- a_cols: int32 [1024, 4], replicated, may hold values from 0 to 1023, as said below
- t_blocks: float32 [1024, 128, 128], P(('gx', 'gy')), may hold values from -0.5 to 0.5
- t_agg: int32 [1024], replicated, may hold values from 0 to 1, as said below
- dinv: float32 [1024, 128, 128], P(('gx', 'gy')), may hold values from -0.5 to 0.5
- coarse_inv: float32 [256, 128, 128], P(('gx', 'gy')), may hold values from -1.5 to 1.5
Outputs:
- coarse: float32 [256, 14, 128, 128], P(('gx', 'gy'))
The draws below stay inside these ranges and needn't reach their ends.
Inputs may be any that keep to these rules, and one draw needn't show every extreme that they name: `a_cols`: block column 0 of row g is g itself; column 1 lies in g's own slab; column 2 lies in the slab below (on the cycle) and column 3 in the slab above; over the rows of one slab, columns 2 name exactly 4 distinct rows of the slab below, and columns 3 exactly 4 distinct rows of the slab above. `t_agg`: every slab's 2 aggregates each hold 4 of its rows.
All inputs are finite; a program needn't handle non-finite values.
Results may differ from the reference program's by a relative error of at most 0.0001.
Values sent between devices are 32-bit elements; how exact they have to be, the bound alone decides.
No kernel may reach another device: no remote copies, remote signals or barrier semaphores. Data moves between devices by JAX's collectives and lax.ppermute only.
A program may use at most 64 MiB of HBM per device.

```python
import jax
import jax.numpy as jnp
from jax import lax

BLOCK = 128
SLOTS = 4
ROWS_DEV = 8
AGG_DEV = 2
FETCH = 4
COARSE_SLOTS = 14
FINE_ROWS = 1024
AGGREGATES = 256


def row_orders(key, count):
    return jax.vmap(lambda subkey: jax.random.permutation(subkey, ROWS_DEV))(jax.random.split(key, count))


def build_graph(key):
    slab_count = FINE_ROWS // ROWS_DEV
    chosen = row_orders(jax.random.fold_in(key, 101), slab_count * 2)
    fetched = jnp.sort(chosen[:, :FETCH], axis=1).reshape(slab_count, 2, FETCH).astype(jnp.int32)
    ordering = row_orders(jax.random.fold_in(key, 202), slab_count * 2).reshape(slab_count, 2, ROWS_DEV)
    own_pick = jax.random.randint(jax.random.fold_in(key, 303), (slab_count, ROWS_DEV), 0, ROWS_DEV)
    slab_ids = jnp.arange(slab_count, dtype=jnp.int32)[:, None]
    row_ids = jnp.arange(ROWS_DEV, dtype=jnp.int32)[None, :]
    lower_slab = (slab_ids + slab_count - 1) % slab_count
    upper_slab = (slab_ids + 1) % slab_count
    pick_lower = jnp.take_along_axis(fetched[:, 0, :], ordering[:, 0, :] % FETCH, axis=1)
    pick_upper = jnp.take_along_axis(fetched[:, 1, :], ordering[:, 1, :] % FETCH, axis=1)
    columns = jnp.stack([slab_ids * ROWS_DEV + row_ids, slab_ids * ROWS_DEV + own_pick, lower_slab * ROWS_DEV + pick_lower, upper_slab * ROWS_DEV + pick_upper], axis=-1)
    return columns.reshape(FINE_ROWS, SLOTS).astype(jnp.int32)


def draw_a_cols(key, part):
    return build_graph(key)


def draw_t_agg(key, part):
    slab_count = FINE_ROWS // ROWS_DEV
    orders = row_orders(jax.random.fold_in(key, 404), slab_count)
    return (orders % AGG_DEV).reshape(FINE_ROWS).astype(jnp.int32)


def level_of(rng, dims, shards, least, top_value):
    def one(axis_at, parts):
        heights = jax.random.uniform(jax.random.fold_in(jax.random.fold_in(rng, 6), axis_at), (parts,), jnp.float32, least / len(shards), top_value / len(shards))
        return jnp.repeat(jnp.exp(heights), dims[axis_at] // parts).reshape((-1,) + (1,) * (len(dims) - axis_at - 1))

    gain = one(*shards[0])
    for cut in shards[1:]:
        gain = gain * one(*cut)
    return gain


def scatter_about(key, extent, deviation, bound, shards=(), kind=jnp.bfloat16):
    factor_of = level_of(key, extent, shards, -0.22, 0.18) if shards else 1.0
    values = jax.random.normal(key, extent, jnp.float32) * deviation * factor_of
    return jnp.minimum(jnp.maximum(values, -bound), bound).astype(kind)


def setup_inputs(seed: int = 0) -> dict:
    streams_of = jax.random.split(jax.random.key(seed), 7)
    return {
        "a_blocks": scatter_about(streams_of[0], (FINE_ROWS, SLOTS, BLOCK, BLOCK), (SLOTS * BLOCK) ** -0.5, 0.25, ((0, 128),), jnp.float32),
        "a_cols": draw_a_cols(jax.random.fold_in(streams_of[6], 71), 0),
        "t_blocks": scatter_about(streams_of[2], (FINE_ROWS, BLOCK, BLOCK), BLOCK ** -0.5, 0.5, ((0, 128),), jnp.float32),
        "t_agg": draw_t_agg(jax.random.fold_in(streams_of[6], 71), 0),
        "dinv": scatter_about(streams_of[4], (FINE_ROWS, BLOCK, BLOCK), BLOCK ** -0.5, 0.5, ((0, 128),), jnp.float32),
        "coarse_inv": scatter_about(streams_of[5], (AGGREGATES, BLOCK, BLOCK), 0.25, 1.5, ((0, 128),), jnp.float32),
    }


OMEGA = 0.6


def reference(a_blocks, a_cols, t_blocks, t_agg, dinv, coarse_inv):
    highest = lax.Precision.HIGHEST
    slab_count = FINE_ROWS // ROWS_DEV
    labels = (jnp.arange(FINE_ROWS, dtype=jnp.int32) // ROWS_DEV) * AGG_DEV + t_agg
    t_cols = t_blocks[a_cols]
    prod_at = jnp.einsum("gkab,gkbc->gkac", a_blocks, t_cols, precision=highest)
    smoothed = jnp.einsum("gab,gkbc->gkac", dinv, prod_at, precision=highest)
    first = (jnp.arange(SLOTS) == 0).astype(jnp.float32)
    prolong = first[None, :, None, None] * t_blocks[:, None] - OMEGA * smoothed
    near_labels = labels[a_cols]

    def accumulate(row, galerkin):
        columns = a_cols[row]
        gathered = prolong[columns]
        partial_value = jnp.einsum("kab,kqbc->kqac", a_blocks[row], gathered, precision=highest)
        contrib = jnp.einsum("pba,kqbc->pkqac", prolong[row], partial_value, precision=highest)
        near = near_labels[row]
        far = near_labels[columns]
        slot = ((far[None] // AGG_DEV - near[:, None, None] // AGG_DEV + 3) % slab_count) * AGG_DEV + far[None] % AGG_DEV
        target = jnp.broadcast_to(near[:, None, None], slot.shape)
        return galerkin.at[target.reshape(-1), slot.reshape(-1)].add(contrib.reshape(-1, BLOCK, BLOCK))

    galerkin = jnp.zeros((AGGREGATES, COARSE_SLOTS, BLOCK, BLOCK), jnp.float32)
    galerkin = lax.fori_loop(0, FINE_ROWS, accumulate, galerkin)
    return jnp.einsum("aij,asjk->asik", coarse_inv, galerkin, precision=highest)
```

```python
import functools

import jax
import jax.numpy as jnp
from jax import lax
from jax.experimental import pallas as pl
from jax.experimental.pallas import tpu as pltpu
from jax.sharding import PartitionSpec as P

OMEGA = 0.6
AXES = ("gx", "gy")
F32 = jnp.float32
BF16 = jnp.bfloat16
COL1, POS2, POS3, UP_LIST, LO_LIST, OWN_LAB, LOW_LAB, UPP_LAB, TAB = 0, 8, 16, 24, 28, 32, 64, 80, 128


def shifted(value, steps):
    count = lax.axis_size(AXES)
    pairs = [(source, (source + steps) % count) for source in range(count)]
    return lax.ppermute(value, AXES, pairs)


def split(x):
    high = x.astype(BF16)
    return high, (x - high.astype(F32)).astype(BF16)


def dot(a, b):
    return jnp.dot(a, b, preferred_element_type=F32)


def dot3(a_high, a_low, b_high, b_low):
    return dot(a_high, b_high) + dot(a_low, b_high) + dot(a_high, b_low)


def dot3k(a_high, a_low, b_high, b_low):
    both = jnp.concatenate([a_high, a_low], axis=1)
    return dot(both, jnp.concatenate([b_high, b_high], axis=0)) + dot(a_high, b_low)


def table_kernel(devices, cols, agg, t, tab, t_up, t_lo):
    rows, width = t.shape[0], t.shape[0] // 2
    minor = devices // lax.axis_size("gx")
    device = lax.axis_index("gx") * minor + lax.axis_index("gy")
    previous = lax.rem(device + devices - 1, devices)
    following = lax.rem(device + 1, devices)

    def col(row, k):
        return cols[(row >> 7) * 512 + k * 128 + (row & 127)]

    def read_mask(slab, k):
        mask = jnp.int32(0)
        for r in range(rows):
            mask = mask | (jnp.int32(1) << (col(slab * rows + r, k) & (rows - 1)))
        return mask

    def ranks(mask):
        found, rank = [], jnp.int32(0)
        for r in range(rows):
            found.append(rank)
            rank = rank + ((mask >> r) & 1)
        return found

    def listed(mask):
        found = ranks(mask)
        result = []
        for j in range(width):
            value = jnp.int32(0)
            for r in range(rows):
                hit = ((mask >> r) & 1) * (found[r] == j).astype(jnp.int32)
                value = value + hit * r
            result.append(value)
        return result

    def count_below(mask, offset):
        below = mask & ((jnp.int32(1) << offset) - 1)
        total = jnp.int32(0)
        for r in range(rows):
            total = total + ((below >> r) & 1)
        return total

    up_list = listed(read_mask(following, 2))
    lo_list = listed(read_mask(previous, 3))
    for j in range(width):
        tab[UP_LIST + j] = up_list[j]
        tab[LO_LIST + j] = lo_list[j]
        t_up[j] = t[up_list[j]]
        t_lo[j] = t[lo_list[j]]
    lower_mask, upper_mask = read_mask(device, 2), read_mask(device, 3)
    for r in range(rows):
        row = device * rows + r
        tab[COL1 + r] = col(row, 1) & (rows - 1)
        tab[POS2 + r] = count_below(lower_mask, col(row, 2) & (rows - 1))
        tab[POS3 + r] = count_below(upper_mask, col(row, 3) & (rows - 1))
        for k in range(4):
            tab[OWN_LAB + 4 * r + k] = agg[col(row, k)]
    lower_list, upper_list = listed(lower_mask), listed(upper_mask)
    for j in range(width):
        for k in range(4):
            tab[LOW_LAB + 4 * j + k] = agg[col(previous * rows + lower_list[j], k)]
            tab[UPP_LAB + 4 * j + k] = agg[col(following * rows + upper_list[j], k)]


def put(value, label, column):
    return jnp.where(label == column, value, jnp.zeros_like(value))


def two_columns(value, label):
    return jnp.concatenate([put(value, label, 0), put(value, label, 1)], axis=1)


def near_kernel(tab, a, t, dinv, own_high, own_low, trans_high, trans_low, near_up, near_lo, t_high, t_low, tile):
    rows, block = t.shape[0], t.shape[1]
    for r in range(rows):
        t_high[r], t_low[r] = split(t[r])
    for r in range(rows):
        near = tab[COL1 + r]
        a0 = split(a[r, 0])
        a1 = split(a[r, 1])
        prod = jnp.concatenate(
            [dot3k(*a0, t_high[r], t_low[r]), dot3k(*a1, t_high[near], t_low[near])], axis=1
        )
        smoothed = dot3k(*split(dinv[r]), *split(prod))
        p0 = t[r] - OMEGA * smoothed[:, :block]
        p1 = -OMEGA * smoothed[:, block:]
        label0, label1 = tab[OWN_LAB + 4 * r], tab[OWN_LAB + 4 * r + 1]
        both = two_columns(p0, label0) + two_columns(p1, label1)
        tile[r] = both
        own_high[r], own_low[r] = split(both)
        turned = both.T
        trans_high[:, r * block : (r + 1) * block], trans_low[:, r * block : (r + 1) * block] = split(turned)
    for j in range(rows // 2):
        near_up[j] = tile[tab[UP_LIST + j]]
        near_lo[j] = tile[tab[LO_LIST + j]]


def far_kernel(
    tab, a, dinv, t_below, t_above,
    below_high, below_low, above_high, above_low, trans_high, trans_low, far_up, far_lo,
    tb_high, tb_low, ta_high, ta_low, tile,
):
    rows, block = dinv.shape[0], dinv.shape[1]
    for j in range(rows // 2):
        tb_high[j], tb_low[j] = split(t_below[j])
        ta_high[j], ta_low[j] = split(t_above[j])
    for r in range(rows):
        below, above = tab[POS2 + r], tab[POS3 + r]
        prod = jnp.concatenate(
            [
                dot3k(*split(a[r, 2]), tb_high[below], tb_low[below]),
                dot3k(*split(a[r, 3]), ta_high[above], ta_low[above]),
            ],
            axis=1,
        )
        both = -OMEGA * dot3k(*split(dinv[r]), *split(prod))
        tile[r] = both
        left = two_columns(both[:, :block], tab[OWN_LAB + 4 * r + 2])
        right = two_columns(both[:, block:], tab[OWN_LAB + 4 * r + 3])
        below_high[r], below_low[r] = split(left)
        above_high[r], above_low[r] = split(right)
        place = slice(r * block, (r + 1) * block)
        trans_high[: 2 * block, place], trans_low[: 2 * block, place] = split(left.T)
        trans_high[2 * block :, place], trans_low[2 * block :, place] = split(right.T)
    for j in range(rows // 2):
        far_up[j] = tile[tab[UP_LIST + j]]
        far_lo[j] = tile[tab[LO_LIST + j]]


def wide(ref, *places):
    return jnp.concatenate([ref[place] for place in places], axis=0)


def first_kernel(
    tab, a, below_high, below_low, above_high, above_low, trans_high, trans_low, near_below, near_above,
    ap_high, ap_low, to_lower, to_upper,
    nb_high, nb_low, na_high, na_low,
):
    rows, block = a.shape[0], a.shape[2]
    for j in range(rows // 2):
        nb_high[j], nb_low[j] = split(near_below[j])
        na_high[j], na_low[j] = split(near_above[j])
    for r in range(rows):
        near, pos2, pos3 = tab[COL1 + r], tab[POS2 + r], tab[POS3 + r]
        a01 = split(jnp.concatenate([a[r, 0], a[r, 1]], axis=1))
        a2, a3 = split(a[r, 2]), split(a[r, 3])
        low = dot3(*a01, wide(below_high, r, near), wide(below_low, r, near)) + dot3k(*a2, nb_high[pos2], nb_low[pos2])
        upp = dot3(*a01, wide(above_high, r, near), wide(above_low, r, near)) + dot3k(*a3, na_high[pos3], na_low[pos3])
        place = slice(r * block, (r + 1) * block)
        ap_high[place, : 2 * block], ap_low[place, : 2 * block] = split(low)
        ap_high[place, 2 * block :], ap_low[place, 2 * block :] = split(upp)
    half = 2 * block
    for side, out in ((0, to_lower), (1, to_upper)):
        lhs = trans_high[side * half : (side + 1) * half], trans_low[side * half : (side + 1) * half]
        for c in range(2):
            cols = slice(c * half, (c + 1) * half)
            out[:, cols] = dot3(*lhs, ap_high[:, cols], ap_low[:, cols])


def second_kernel(
    tab, a, own_high, own_low, trans_high, trans_low, far_below, far_above,
    ap_high, ap_low, to_lower, to_upper,
    fb_high, fb_low, fa_high, fa_low,
):
    rows, block = a.shape[0], a.shape[2]
    half = 2 * block
    for j in range(rows // 2):
        low, upp = LOW_LAB + 4 * j, UPP_LAB + 4 * j
        fb_high[j], fb_low[j] = split(
            jnp.concatenate(
                [two_columns(far_below[j][:, :block], tab[low + 2]), two_columns(far_below[j][:, block:], tab[low + 3])],
                axis=1,
            )
        )
        fa_high[j], fa_low[j] = split(
            jnp.concatenate(
                [two_columns(far_above[j][:, :block], tab[upp + 2]), two_columns(far_above[j][:, block:], tab[upp + 3])],
                axis=1,
            )
        )
    for r in range(rows):
        near, pos2, pos3 = tab[COL1 + r], tab[POS2 + r], tab[POS3 + r]
        a01 = split(jnp.concatenate([a[r, 0], a[r, 1]], axis=1))
        a2, a3 = split(a[r, 2]), split(a[r, 3])
        left = dot3k(*a2, fb_high[pos2], fb_low[pos2])
        right = dot3k(*a3, fa_high[pos3], fa_low[pos3])
        own = dot3(*a01, wide(own_high, r, near), wide(own_low, r, near)) + left[:, half:] + right[:, :half]
        place = slice(r * block, (r + 1) * block)
        ap_high[place, :half], ap_low[place, :half] = split(left[:, :half])
        ap_high[place, half : 2 * half], ap_low[place, half : 2 * half] = split(own)
        ap_high[place, 2 * half :], ap_low[place, 2 * half :] = split(right[:, half:])
    for side, out in ((0, to_lower), (1, to_upper)):
        lhs = trans_high[side * half : (side + 1) * half], trans_low[side * half : (side + 1) * half]
        for c in range(3):
            cols = slice(c * half, (c + 1) * half)
            out[:, cols] = dot3(*lhs, ap_high[:, cols], ap_low[:, cols])


def own_kernel(trans_high, trans_low, ap1_high, ap1_low, ap2_high, ap2_low, own):
    half = trans_high.shape[0]
    lhs = trans_high[...], trans_low[...]
    for d, (high, low, c) in enumerate(
        ((ap2_high, ap2_low, 0), (ap1_high, ap1_low, 0), (ap2_high, ap2_low, 1), (ap1_high, ap1_low, 1), (ap2_high, ap2_low, 2))
    ):
        cols = slice(c * half, (c + 1) * half)
        own[:, d * half : (d + 1) * half] = dot3(*lhs, high[:, cols], low[:, cols])


def last_kernel(inverse, own, next1, next2, prev1, prev2, out):
    block = inverse.shape[1]
    half = 2 * block
    held = ((1, 0), (0, 0), (1, 1), (0, 1), (1, 2))
    for agg in range(2):
        inv = split(inverse[agg])
        line = slice(agg * block, (agg + 1) * block)
        for d in range(-3, 4):
            total = None
            if -2 <= d <= 2:
                total = own[line, (d + 2) * half : (d + 3) * half]
            for shift, bufs in ((1, (next1, next2)), (-1, (prev1, prev2))):
                if -2 <= d - shift <= 2:
                    which, c = held[d - shift + 2]
                    part = bufs[which][line, c * half : (c + 1) * half]
                    total = part if total is None else total + part
            result = dot3k(*inv, *split(total))
            out[agg, 2 * (d + 3)] = result[:, :block]
            out[agg, 2 * (d + 3) + 1] = result[:, block:]


def call(body, outs, ins, scratch=(), name=None, flops=0):
    smem = pl.BlockSpec(memory_space=pltpu.SMEM)
    vmem = pl.BlockSpec(memory_space=pltpu.VMEM)

    def spec(x):
        return smem if x.dtype == jnp.int32 else vmem

    return pl.pallas_call(
        body,
        out_shape=outs,
        in_specs=[spec(x) for x in ins],
        out_specs=jax.tree.map(spec, outs),
        scratch_shapes=[pltpu.VMEM(shape, dtype) for shape, dtype in scratch],
        compiler_params=pltpu.CompilerParams(vmem_limit_bytes=24 * 2**20),
        cost_estimate=pl.CostEstimate(flops=flops, bytes_accessed=2**20, transcendentals=0),
        name=name,
    )(*ins)


def shards(a_blocks, a_cols, t_blocks, t_agg, dinv, coarse_inv):
    devices = lax.axis_size(AXES)
    rows, block = t_blocks.shape[:2]
    width, half, deep = rows // 2, 2 * block, rows * block
    shape = jax.ShapeDtypeStruct
    pair = lambda *dims: [shape(dims, BF16), shape(dims, BF16)]
    cols = a_cols.reshape(-1, 128, 4).transpose(0, 2, 1).reshape(-1)
    product = 2 * block**3 * 3

    tab, t_up, t_lo = call(
        functools.partial(table_kernel, devices),
        [shape((TAB,), jnp.int32), shape((width, block, block), F32), shape((width, block, block), F32)],
        [cols, t_agg, t_blocks],
        name="table",
    )
    t_below = shifted(t_up, 1)
    t_above = shifted(t_lo, -1)
    own_high, own_low, pt_high, pt_low, near_up, near_lo = call(
        near_kernel,
        pair(rows, block, half) + pair(half, deep) + [shape((width, block, half), F32)] * 2,
        [tab, a_blocks, t_blocks, dinv],
        [((rows, block, block), BF16)] * 2 + [((rows, block, half), F32)],
        name="near",
        flops=32 * product,
    )
    near_below = shifted(near_up, 1)
    near_above = shifted(near_lo, -1)
    below_high, below_low, above_high, above_low, side_high, side_low, far_up, far_lo = call(
        far_kernel,
        pair(rows, block, half) * 2 + pair(2 * half, deep) + [shape((width, block, half), F32)] * 2,
        [tab, a_blocks, dinv, t_below, t_above],
        [((width, block, block), BF16)] * 4 + [((rows, block, half), F32)],
        name="far",
        flops=32 * product,
    )
    far_below = shifted(far_up, 1)
    far_above = shifted(far_lo, -1)
    ap1_high, ap1_low, lower1, upper1 = call(
        first_kernel,
        pair(deep, 2 * half) + [shape((half, 2 * half), F32)] * 2,
        [tab, a_blocks, below_high, below_low, above_high, above_low, side_high, side_low, near_below, near_above],
        [((width, block, half), BF16)] * 4,
        name="first",
        flops=200 * product,
    )
    next1 = shifted(lower1, -1)
    prev1 = shifted(upper1, 1)
    ap2_high, ap2_low, lower2, upper2 = call(
        second_kernel,
        pair(deep, 3 * half) + [shape((half, 3 * half), F32)] * 2,
        [tab, a_blocks, own_high, own_low, side_high, side_low, far_below, far_above],
        [((width, block, 2 * half), BF16)] * 4,
        name="second",
        flops=250 * product,
    )
    next2 = shifted(lower2, -1)
    prev2 = shifted(upper2, 1)
    (own,) = call(
        own_kernel,
        [shape((half, 5 * half), F32)],
        [pt_high, pt_low, ap1_high, ap1_low, ap2_high, ap2_low],
        name="own",
        flops=160 * product,
    )
    (out,) = call(
        last_kernel,
        [shape((2, 14, block, block), F32)],
        [coarse_inv, own, next1, next2, prev1, prev2],
        name="last",
        flops=28 * product,
    )
    return out


def solution(mesh):
    placed = (
        P(AXES, None, None, None),
        P(),
        P(AXES, None, None),
        P(),
        P(AXES, None, None),
        P(AXES, None, None),
    )
    return jax.shard_map(
        shards,
        mesh=mesh,
        in_specs=placed,
        out_specs=P(AXES, None, None, None),
        check_vma=False,
    )
```

```python
import functools

import jax
import jax.numpy as jnp
from jax import lax
from jax.experimental import pallas as pl
from jax.experimental.pallas import tpu as pltpu
from jax.sharding import PartitionSpec as P


OMEGA = 0.6
AXES = ("gx", "gy")
F32 = jnp.float32
BF16 = jnp.bfloat16
COL1, POS2, POS3, LISTS, OWN_LAB, SIDE_LAB, TAB = 0, 8, 16, 24, 32, 64, 128
BELOW, ABOVE = 0, 1
ROW_CHUNK = 128


def exchanged(value, first):
    count = lax.axis_size(AXES)
    pairs = []
    for low in range(first, count + first, 2):
        high = (low + 1) % count
        pairs += [(low, high), (high, low)]
    return lax.ppermute(value, AXES, pairs)


def pair_side():
    return 1 - lax.rem(lax.axis_index("gy"), 2)


def split(x):
    high = x.astype(BF16)
    return high, (x - high.astype(F32)).astype(BF16)


def dot(a, b):
    return jnp.dot(a, b, preferred_element_type=F32)


def dot3(a_high, a_low, b_high, b_low):
    return dot(a_high, b_high) + dot(a_low, b_high) + dot(a_high, b_low)


def dot3k(a_high, a_low, b_high, b_low):
    both = jnp.concatenate([a_high, a_low], axis=1)
    return dot(both, jnp.concatenate([b_high, b_high], axis=0)) + dot(a_high, b_low)


def load_kernel(devices, cols_hbm, agg_hbm, t_hbm, dinv_hbm, a_hbm, tab, t_0, t_1, t, dinv, a, cols, agg, sem):
    copies = [
        pltpu.make_async_copy(source, target, sem.at[i])
        for i, (source, target) in enumerate(
            ((cols_hbm, cols), (agg_hbm, agg), (t_hbm, t), (dinv_hbm, dinv), (a_hbm, a))
        )
    ]
    for copy in copies:
        copy.start()
    rows, width = t.shape[0], t.shape[0] // 2
    device = lax.axis_index("gx") * lax.axis_size("gy") + lax.axis_index("gy")
    previous = lax.rem(device + devices - 1, devices)
    following = lax.rem(device + 1, devices)
    side = pair_side()

    def col(row, k):
        return cols[(row // ROW_CHUNK) * (4 * ROW_CHUNK) + k * ROW_CHUNK + lax.rem(row, ROW_CHUNK)]

    def read_mask(slab, k):
        mask = jnp.int32(0)
        for r in range(rows):
            mask = mask | (jnp.int32(1) << (col(slab * rows + r, k) & (rows - 1)))
        return mask

    def listed(mask):
        found, rank = [], jnp.int32(0)
        for r in range(rows):
            found.append(rank)
            rank = rank + ((mask >> r) & 1)
        result = []
        for j in range(width):
            value = jnp.int32(0)
            for r in range(rows):
                hit = ((mask >> r) & 1) * (found[r] == j).astype(jnp.int32)
                value = value + hit * r
            result.append(value)
        return result

    def count_below(mask, offset):
        below = mask & ((jnp.int32(1) << offset) - 1)
        total = jnp.int32(0)
        for r in range(rows):
            total = total + ((below >> r) & 1)
        return total

    copies[0].wait()
    lists = listed(read_mask(previous, 3)), listed(read_mask(following, 2))
    copies[2].wait()
    for j in range(width):
        mine = jnp.where(side == ABOVE, lists[ABOVE][j], lists[BELOW][j])
        other = jnp.where(side == ABOVE, lists[BELOW][j], lists[ABOVE][j])
        tab[LISTS + j] = mine
        tab[LISTS + width + j] = other
        t_0[j] = t[mine]
        t_1[j] = t[other]
    copies[1].wait()
    masks = read_mask(device, 2), read_mask(device, 3)
    for r in range(rows):
        row = device * rows + r
        tab[COL1 + r] = col(row, 1) & (rows - 1)
        tab[POS2 + r] = count_below(masks[BELOW], col(row, 2) & (rows - 1))
        tab[POS3 + r] = count_below(masks[ABOVE], col(row, 3) & (rows - 1))
        for k in range(4):
            tab[OWN_LAB + 4 * r + k] = agg[col(row, k)]
    for which, slab in ((BELOW, previous), (ABOVE, following)):
        held = listed(masks[which])
        for j in range(width):
            for k in range(4):
                tab[SIDE_LAB + 16 * which + 4 * j + k] = agg[col(slab * rows + held[j], k)]
    copies[3].wait()
    copies[4].wait()


def put(value, label, column):
    return jnp.where(label == column, value, jnp.zeros_like(value))


def two_columns(value, label):
    return jnp.concatenate([put(value, label, 0), put(value, label, 1)], axis=1)


def send(tab, tile, out_0, out_1):
    width = out_0.shape[0]
    for j in range(width):
        out_0[j] = tile[tab[LISTS + j]]
        out_1[j] = tile[tab[LISTS + width + j]]


def near_kernel(
    tab, a, t, dinv,
    a_high, a_low, own_high, own_low, trans_high, trans_low, near_0, near_1,
    t_high, t_low, tile,
):
    rows, block = t.shape[0], t.shape[1]
    for r in range(rows):
        t_high[r], t_low[r] = split(t[r])
    for r in range(rows):
        near = tab[COL1 + r]
        a0, a1 = split(a[r, 0]), split(a[r, 1])
        a_high[r] = jnp.concatenate([a0[0], a1[0]], axis=1)
        a_low[r] = jnp.concatenate([a0[1], a1[1]], axis=1)
        prod = jnp.concatenate(
            [dot3k(*a0, t_high[r], t_low[r]), dot3k(*a1, t_high[near], t_low[near])], axis=1
        )
        smoothed = dot3k(*split(dinv[r]), *split(prod))
        p0 = t[r] - OMEGA * smoothed[:, :block]
        p1 = -OMEGA * smoothed[:, block:]
        label0, label1 = tab[OWN_LAB + 4 * r], tab[OWN_LAB + 4 * r + 1]
        both = two_columns(p0, label0) + two_columns(p1, label1)
        tile[r] = both
        own_high[r], own_low[r] = split(both)
        place = slice(r * block, (r + 1) * block)
        trans_high[:, place], trans_low[:, place] = split(both.T)
    send(tab, tile, near_0, near_1)


def far_kernel(
    tab, a, dinv, t_0, t_1, after,
    a_high, a_low, below_high, below_low, above_high, above_low, trans_high, trans_low, far_0, far_1,
    t_high, t_low, tile,
):
    rows, block = dinv.shape[0], dinv.shape[1]
    side = pair_side()
    for j in range(rows // 2):
        t_high[side, j], t_low[side, j] = split(t_0[j])
        t_high[1 - side, j], t_low[1 - side, j] = split(t_1[j])
    for r in range(rows):
        below, above = tab[POS2 + r], tab[POS3 + r]
        a2, a3 = split(a[r, 2]), split(a[r, 3])
        a_high[r] = jnp.concatenate([a2[0], a3[0]], axis=1)
        a_low[r] = jnp.concatenate([a2[1], a3[1]], axis=1)
        prod = jnp.concatenate(
            [
                dot3k(*a2, t_high[BELOW, below], t_low[BELOW, below]),
                dot3k(*a3, t_high[ABOVE, above], t_low[ABOVE, above]),
            ],
            axis=1,
        )
        both = -OMEGA * dot3k(*split(dinv[r]), *split(prod))
        tile[r] = both
        left = two_columns(both[:, :block], tab[OWN_LAB + 4 * r + 2])
        right = two_columns(both[:, block:], tab[OWN_LAB + 4 * r + 3])
        below_high[r], below_low[r] = split(left)
        above_high[r], above_low[r] = split(right)
        place = slice(r * block, (r + 1) * block)
        trans_high[BELOW, :, place], trans_low[BELOW, :, place] = split(left.T)
        trans_high[ABOVE, :, place], trans_low[ABOVE, :, place] = split(right.T)
    send(tab, tile, far_0, far_1)


def wide(ref, *places):
    return jnp.concatenate([ref[place] for place in places], axis=0)


def pre_kernel(
    tab, a_high, a_low, own_high, own_low, below_high, below_low, above_high, above_low,
    part,
):
    rows = a_high.shape[0]
    half = own_high.shape[2]
    for r in range(rows):
        near = tab[COL1 + r]
        pairs = ((below_high, below_low), (own_high, own_low), (above_high, above_low))
        for c, (high, low) in enumerate(pairs):
            part[r, :, c * half : (c + 1) * half] = dot3(a_high[r], a_low[r], wide(high, r, near), wide(low, r, near))


def partial_rows(trans_high, trans_low, ap_high, ap_low, outs):
    side = pair_side()
    half = trans_high.shape[1]
    for which, out in ((side, outs[0]), (1 - side, outs[1])):
        for c in range(ap_high.shape[1] // half):
            cols = slice(c * half, (c + 1) * half)
            out[:, cols] = dot3(trans_high[which], trans_low[which], ap_high[:, cols], ap_low[:, cols])


def first_kernel(
    tab, a_high, a_low, part, trans_high, trans_low, near_0, near_1,
    ap_high, ap_low, out_0, out_1,
    p_high, p_low,
):
    rows, block = a_high.shape[0], a_high.shape[1]
    half = 2 * block
    side = pair_side()
    for j in range(rows // 2):
        p_high[side, j], p_low[side, j] = split(near_0[j])
        p_high[1 - side, j], p_low[1 - side, j] = split(near_1[j])
    for r in range(rows):
        pos2, pos3 = tab[POS2 + r], tab[POS3 + r]
        a2 = a_high[r, :, :block], a_low[r, :, :block]
        a3 = a_high[r, :, block:], a_low[r, :, block:]
        low = part[r, :, :half] + dot3k(*a2, p_high[BELOW, pos2], p_low[BELOW, pos2])
        upp = part[r, :, 2 * half :] + dot3k(*a3, p_high[ABOVE, pos3], p_low[ABOVE, pos3])
        place = slice(r * block, (r + 1) * block)
        ap_high[place, :half], ap_low[place, :half] = split(low)
        ap_high[place, half:], ap_low[place, half:] = split(upp)
    partial_rows(trans_high, trans_low, ap_high, ap_low, (out_0, out_1))


def second_kernel(
    tab, a_high, a_low, part, trans_high, trans_low, far_0, far_1, after,
    ap_high, ap_low, out_0, out_1,
    p_high, p_low,
):
    rows, block = a_high.shape[0], a_high.shape[1]
    half = 2 * block
    side = pair_side()
    for which, ref in ((side, far_0), (1 - side, far_1)):
        for j in range(rows // 2):
            label = SIDE_LAB + 16 * which + 4 * j
            value = ref[j]
            spread = [two_columns(value[:, :block], tab[label + 2]), two_columns(value[:, block:], tab[label + 3])]
            p_high[which, j], p_low[which, j] = split(jnp.concatenate(spread, axis=1))
    for r in range(rows):
        pos2, pos3 = tab[POS2 + r], tab[POS3 + r]
        a2 = a_high[r, :, :block], a_low[r, :, :block]
        a3 = a_high[r, :, block:], a_low[r, :, block:]
        left = dot3k(*a2, p_high[BELOW, pos2], p_low[BELOW, pos2])
        right = dot3k(*a3, p_high[ABOVE, pos3], p_low[ABOVE, pos3])
        own = part[r, :, half : 2 * half] + left[:, half:] + right[:, :half]
        place = slice(r * block, (r + 1) * block)
        ap_high[place, :half], ap_low[place, :half] = split(left[:, :half])
        ap_high[place, half : 2 * half], ap_low[place, half : 2 * half] = split(own)
        ap_high[place, 2 * half :], ap_low[place, 2 * half :] = split(right[:, half:])
    partial_rows(trans_high, trans_low, ap_high, ap_low, (out_0, out_1))


HELD = ((1, 0), (0, 0), (1, 1), (0, 1), (1, 2))


def own_kernel(trans_high, trans_low, ap1_high, ap1_low, ap2_high, ap2_low, own):
    half = trans_high.shape[0]
    aps = (ap1_high, ap1_low), (ap2_high, ap2_low)
    for d, (which, c) in enumerate(HELD):
        cols = slice(c * half, (c + 1) * half)
        high, low = aps[which]
        own[:, d * half : (d + 1) * half] = dot3(trans_high[...], trans_low[...], high[:, cols], low[:, cols])


def last_kernel(inverse, own, first_0, first_1, second_0, second_1, out):
    block = inverse.shape[1]
    half = 2 * block

    def finish(above, below):
        for agg in range(2):
            inv = split(inverse[agg])
            line = slice(agg * block, (agg + 1) * block)
            for d in range(-3, 4):
                total = None
                if -2 <= d <= 2:
                    total = own[line, (d + 2) * half : (d + 3) * half]
                for shift, bufs in ((1, above), (-1, below)):
                    if -2 <= d - shift <= 2:
                        which, c = HELD[d - shift + 2]
                        part = bufs[which][line, c * half : (c + 1) * half]
                        total = part if total is None else total + part
                result = dot3k(*inv, *split(total))
                out[agg, 2 * (d + 3)] = result[:, :block]
                out[agg, 2 * (d + 3) + 1] = result[:, block:]

    side = pair_side()

    @pl.when(side == ABOVE)
    def _():
        finish((first_0, second_0), (first_1, second_1))

    @pl.when(side == BELOW)
    def _():
        finish((first_1, second_1), (first_0, second_0))


def call(body, outs, ins, scratch=(), micros=1.0, hbm=False):
    smem = pl.BlockSpec(memory_space=pltpu.SMEM)
    vmem = pl.BlockSpec(memory_space=pltpu.VMEM)
    flops = int(micros * 1e6 * 100)

    def spec(x):
        return smem if x.dtype == jnp.int32 else vmem

    return pl.pallas_call(
        body,
        out_shape=outs,
        in_specs=[pl.BlockSpec(memory_space=pltpu.HBM) if hbm else spec(x) for x in ins],
        out_specs=jax.tree.map(spec, outs),
        scratch_shapes=[pltpu.VMEM(*x) if isinstance(x, tuple) else x for x in scratch],
        compiler_params=pltpu.CompilerParams(vmem_limit_bytes=24 * 2**20),
        cost_estimate=pl.CostEstimate(flops=flops, bytes_accessed=2**20, transcendentals=0),
    )(*ins)


def shards(a_blocks, a_cols, t_blocks, t_agg, dinv, coarse_inv):
    devices = lax.axis_size(AXES)
    rows, block = t_blocks.shape[:2]
    width, half, deep = rows // 2, 2 * block, rows * block
    shape = jax.ShapeDtypeStruct
    pair = lambda *dims: [shape(dims, BF16), shape(dims, BF16)]
    cols = a_cols.reshape(-1, ROW_CHUNK, 4).transpose(0, 2, 1).reshape(-1)

    def swap(value_0, value_1):
        far = exchanged(value_1, 1)
        return exchanged(value_0, 0), far

    tab, t_0, t_1, t, d, a = call(
        functools.partial(load_kernel, devices),
        [shape((TAB,), jnp.int32)]
        + [shape((width, block, block), F32)] * 2
        + [shape(x.shape, F32) for x in (t_blocks, dinv, a_blocks)],
        [pltpu.with_memory_space_constraint(x, pltpu.HBM) for x in (cols, t_agg, t_blocks, dinv, a_blocks)],
        [pltpu.SMEM(cols.shape, jnp.int32), pltpu.SMEM(t_agg.shape, jnp.int32), pltpu.SemaphoreType.DMA((5,))],
        hbm=True,
    )
    t_0, t_1 = swap(t_0, t_1)
    a01_high, a01_low, own_high, own_low, pt_high, pt_low, near_0, near_1 = call(
        near_kernel,
        pair(rows, block, half) * 2 + pair(half, deep) + [shape((width, block, half), F32)] * 2,
        [tab, a, t, d],
        [((rows, block, block), BF16)] * 2 + [((rows, block, half), F32)],
        micros=3,
    )
    near_0, near_1 = swap(near_0, near_1)
    a23_high, a23_low, below_high, below_low, above_high, above_low, side_high, side_low, far_0, far_1 = call(
        far_kernel,
        pair(rows, block, half) * 3 + pair(2, half, deep) + [shape((width, block, half), F32)] * 2,
        [tab, a, d, t_0, t_1, own_high],
        [((2, width, block, block), BF16)] * 2 + [((rows, block, half), F32)],
        micros=3,
    )
    far_0, far_1 = swap(far_0, far_1)
    (part,) = call(
        pre_kernel,
        [shape((rows, block, 3 * half), F32)],
        [tab, a01_high, a01_low, own_high, own_low, below_high, below_low, above_high, above_low],
        micros=2,
    )
    ap1_high, ap1_low, first_0, first_1 = call(
        first_kernel,
        pair(deep, 2 * half) + [shape((half, 2 * half), F32)] * 2,
        [tab, a23_high, a23_low, part, side_high, side_low, near_0, near_1],
        [((2, width, block, half), BF16)] * 2,
        micros=4,
    )
    first_0, first_1 = swap(first_0, first_1)
    ap2_high, ap2_low, second_0, second_1 = call(
        second_kernel,
        pair(deep, 3 * half) + [shape((half, 3 * half), F32)] * 2,
        [tab, a23_high, a23_low, part, side_high, side_low, far_0, far_1, ap1_high],
        [((2, width, block, 2 * half), BF16)] * 2,
        micros=5,
    )
    second_0, second_1 = swap(second_0, second_1)
    (own,) = call(
        own_kernel, [shape((half, 5 * half), F32)], [pt_high, pt_low, ap1_high, ap1_low, ap2_high, ap2_low], micros=2
    )
    (out,) = call(
        last_kernel,
        [shape((2, 14, block, block), F32)],
        [coarse_inv, own, first_0, first_1, second_0, second_1],
        micros=2,
    )
    return out


def solution(mesh):
    placed = (
        P(AXES, None, None, None),
        P(),
        P(AXES, None, None),
        P(),
        P(AXES, None, None),
        P(AXES, None, None),
    )
    return jax.shard_map(
        shards,
        mesh=mesh,
        in_specs=placed,
        out_specs=P(AXES, None, None, None),
        check_vma=False,
    )
```

```python
import functools

import jax
import jax.numpy as jnp
from jax import lax
from jax.experimental import pallas as pl
from jax.experimental.pallas import tpu as pltpu
from jax.sharding import PartitionSpec as P


OMEGA = 0.6
AXES = ("gx", "gy")
F32 = jnp.float32
BF16 = jnp.bfloat16
ROW, NEAR, POS2, POS3, LIST_0, OWN_LAB, SIDE_LAB, TAB = 0, 8, 16, 24, 32, 48, 80, 128
BELOW, ABOVE = 0, 1
ROW_CHUNK = 128


def exchanged(value, first):
    count = lax.axis_size(AXES)
    pairs = []
    for low in range(first, count + first, 2):
        high = (low + 1) % count
        pairs += [(low, high), (high, low)]
    return lax.ppermute(value, AXES, pairs)


def pair_side():
    return 1 - lax.rem(lax.axis_index("gy"), 2)


def split(x):
    high = x.astype(BF16)
    return high, (x - high.astype(F32)).astype(BF16)


def dot(a, b):
    return jnp.dot(a, b, preferred_element_type=F32)


def dot3(a_high, a_low, b_high, b_low):
    return dot(a_high, b_high) + dot(a_low, b_high) + dot(a_high, b_low)


def dot3k(a_high, a_low, b_high, b_low):
    both = jnp.concatenate([a_high, a_low], axis=1)
    return dot(both, jnp.concatenate([b_high, b_high], axis=0)) + dot(a_high, b_low)


def load_kernel(devices, cols_hbm, agg_hbm, t_hbm, tab, t_0, t_1, t, cols, agg, sem):
    copies = [
        pltpu.make_async_copy(source, target, sem.at[i])
        for i, (source, target) in enumerate(((cols_hbm, cols), (agg_hbm, agg), (t_hbm, t)))
    ]
    for copy in copies:
        copy.start()
    rows, width = t.shape[0], t.shape[0] // 2
    device = lax.axis_index("gx") * lax.axis_size("gy") + lax.axis_index("gy")
    previous = lax.rem(device + devices - 1, devices)
    following = lax.rem(device + 1, devices)
    side = pair_side()

    def col(row, k):
        return cols[(row // ROW_CHUNK) * (4 * ROW_CHUNK) + k * ROW_CHUNK + lax.rem(row, ROW_CHUNK)]

    def read_mask(slab, k):
        mask = jnp.int32(0)
        for r in range(rows):
            mask = mask | (jnp.int32(1) << (col(slab * rows + r, k) & (rows - 1)))
        return mask

    def listed(mask):
        found, rank = [], jnp.int32(0)
        for r in range(rows):
            found.append(rank)
            rank = rank + ((mask >> r) & 1)
        result = []
        for j in range(width):
            value = jnp.int32(0)
            for r in range(rows):
                hit = ((mask >> r) & 1) * (found[r] == j).astype(jnp.int32)
                value = value + hit * r
            result.append(value)
        return result

    def count_below(mask, offset):
        below = mask & ((jnp.int32(1) << offset) - 1)
        total = jnp.int32(0)
        for r in range(rows):
            total = total + ((below >> r) & 1)
        return total

    copies[0].wait()
    read = read_mask(previous, 3), read_mask(following, 2)
    mask_0 = jnp.where(side == ABOVE, read[ABOVE], read[BELOW])
    mask_1 = jnp.where(side == ABOVE, read[BELOW], read[ABOVE])
    order = listed(mask_1) + listed((jnp.int32(1) << rows) - 1 - mask_1)
    list_0 = listed(mask_0)
    copies[2].wait()
    for j in range(width):
        t_1[j] = t[order[j]]
        t_0[j] = t[list_0[j]]

    def place(offset):
        sent = (mask_1 >> offset) & 1
        rank = count_below(mask_1, offset)
        return jnp.where(sent == 1, rank, width + offset - rank)

    copies[1].wait()
    masks = read_mask(device, 2), read_mask(device, 3)
    for j in range(width):
        tab[LIST_0 + j] = place(list_0[j])
    for u in range(rows):
        row = device * rows + order[u]
        tab[ROW + u] = order[u]
        tab[NEAR + u] = place(col(row, 1) & (rows - 1))
        tab[POS2 + u] = count_below(masks[BELOW], col(row, 2) & (rows - 1))
        tab[POS3 + u] = count_below(masks[ABOVE], col(row, 3) & (rows - 1))
        for k in range(4):
            tab[OWN_LAB + 4 * u + k] = agg[col(row, k)]
    for which, slab in ((BELOW, previous), (ABOVE, following)):
        held = listed(masks[which])
        for j in range(width):
            for k in range(2):
                tab[SIDE_LAB + 8 * which + 2 * j + k] = agg[col(slab * rows + held[j], 2 + k)]


def put(value, label, column):
    return jnp.where(label == column, value, jnp.zeros_like(value))


def two_columns(value, label):
    return jnp.concatenate([put(value, label, 0), put(value, label, 1)], axis=1)


def near_tile(tab, a, t, dinv, u):
    block = t.shape[1]
    row = tab[ROW + u]
    near = tab[ROW + tab[NEAR + u]]
    prod = jnp.concatenate(
        [dot3k(*split(a[row, 0]), *split(t[row])), dot3k(*split(a[row, 1]), *split(t[near]))], axis=1
    )
    smoothed = dot3k(*split(dinv[row]), *split(prod))
    p0 = t[row] - OMEGA * smoothed[:, :block]
    p1 = -OMEGA * smoothed[:, block:]
    return two_columns(p0, tab[OWN_LAB + 4 * u]) + two_columns(p1, tab[OWN_LAB + 4 * u + 1])


def near_sent_kernel(tab, a, t, dinv, near_1):
    for u in range(near_1.shape[0]):
        near_1[u] = near_tile(tab, a, t, dinv, u)


def near_rest_kernel(tab, a, t, dinv, near_1, near_0, own):
    width = near_1.shape[0]
    for u in range(width):
        own[u] = near_1[u]
        own[width + u] = near_tile(tab, a, t, dinv, width + u)
    for j in range(width):
        near_0[j] = own[tab[LIST_0 + j]]


def far_tile(tab, a, dinv, t_high, t_low, u):
    row = tab[ROW + u]
    below, above = tab[POS2 + u], tab[POS3 + u]
    prod = jnp.concatenate(
        [
            dot3k(*split(a[row, 2]), t_high[BELOW, below], t_low[BELOW, below]),
            dot3k(*split(a[row, 3]), t_high[ABOVE, above], t_low[ABOVE, above]),
        ],
        axis=1,
    )
    return -OMEGA * dot3k(*split(dinv[row]), *split(prod))


def far_sent_kernel(tab, a, dinv, t_0, t_1, after, far_1, t_high, t_low):
    side = pair_side()
    for j in range(t_0.shape[0]):
        t_high[side, j], t_low[side, j] = split(t_0[j])
        t_high[1 - side, j], t_low[1 - side, j] = split(t_1[j])
    for u in range(far_1.shape[0]):
        far_1[u] = far_tile(tab, a, dinv, t_high, t_low, u)


def far_rest_kernel(tab, a, dinv, t_high, t_low, far_1, far_0, far):
    width = far_1.shape[0]
    for u in range(width):
        far[u] = far_1[u]
        far[width + u] = far_tile(tab, a, dinv, t_high, t_low, width + u)
    for j in range(width):
        far_0[j] = far[tab[LIST_0 + j]]


def far_split_kernel(tab, a, dinv, t_0, t_1, far_1, far_0, far, t_high, t_low):
    side = pair_side()
    for j in range(t_0.shape[0]):
        t_high[side, j], t_low[side, j] = split(t_0[j])
        t_high[1 - side, j], t_low[1 - side, j] = split(t_1[j])
    far_rest_kernel(tab, a, dinv, t_high, t_low, far_1, far_0, far)


def wide(ref, *places):
    return jnp.concatenate([ref[place] for place in places], axis=0)


def store_turned(trans, side, label, place, value):
    block = value.shape[0]
    trans[side, pl.ds(pl.multiple_of(label * block, block), block), place] = value.T
    trans[side, pl.ds(pl.multiple_of((1 - label) * block, block), block), place] = jnp.zeros_like(value)


def pre_kernel(
    tab, a, own, far,
    part, a_high, a_low, trans_high, trans_low,
    own_high, own_low, below_high, below_low, above_high, above_low,
):
    rows, block = own.shape[0], own.shape[1]
    half = 2 * block
    for u in range(rows):
        own_high[u], own_low[u] = split(own[u])
        place = slice(u * block, (u + 1) * block)
        for side, high_ref, low_ref in ((BELOW, below_high, below_low), (ABOVE, above_high, above_low)):
            label = tab[OWN_LAB + 4 * u + 2 + side]
            high, low = split(far[u, :, side * block : (side + 1) * block])
            high_ref[u] = two_columns(high, label)
            low_ref[u] = two_columns(low, label)
            store_turned(trans_high, side, label, place, high)
            store_turned(trans_low, side, label, place, low)
    pairs = ((below_high, below_low), (own_high, own_low), (above_high, above_low))
    for u in range(rows):
        row, near = tab[ROW + u], tab[NEAR + u]
        a01 = split(jnp.concatenate([a[row, 0], a[row, 1]], axis=1))
        a_high[u], a_low[u] = split(jnp.concatenate([a[row, 2], a[row, 3]], axis=1))
        for c, (high, low) in enumerate(pairs):
            part[u, :, c * half : (c + 1) * half] = dot3(*a01, wide(high, u, near), wide(low, u, near))


def coarse_rows(trans_high, trans_low, ap_high, ap_low, which, out):
    half = trans_high.shape[1]
    for c in range(ap_high.shape[1] // half):
        cols = slice(c * half, (c + 1) * half)
        out[:, cols] = dot3(trans_high[which], trans_low[which], ap_high[:, cols], ap_low[:, cols])


def first_kernel(
    tab, a_high, a_low, part, trans_high, trans_low, near_0, near_1,
    ap_high, ap_low, out_1,
    p_high, p_low,
):
    rows, block = a_high.shape[0], a_high.shape[1]
    half = 2 * block
    side = pair_side()
    for j in range(rows // 2):
        p_high[side, j], p_low[side, j] = split(near_0[j])
        p_high[1 - side, j], p_low[1 - side, j] = split(near_1[j])
    for u in range(rows):
        pos2, pos3 = tab[POS2 + u], tab[POS3 + u]
        a2 = a_high[u, :, :block], a_low[u, :, :block]
        a3 = a_high[u, :, block:], a_low[u, :, block:]
        low = part[u, :, :half] + dot3k(*a2, p_high[BELOW, pos2], p_low[BELOW, pos2])
        upp = part[u, :, 2 * half :] + dot3k(*a3, p_high[ABOVE, pos3], p_low[ABOVE, pos3])
        place = slice(u * block, (u + 1) * block)
        ap_high[place, :half], ap_low[place, :half] = split(low)
        ap_high[place, half:], ap_low[place, half:] = split(upp)
    coarse_rows(trans_high, trans_low, ap_high, ap_low, 1 - side, out_1)


def second_kernel(
    tab, a_high, a_low, part, trans_high, trans_low, far_0, far_1, after,
    ap_high, ap_low, out_1,
    p_high, p_low,
):
    rows, block = a_high.shape[0], a_high.shape[1]
    half = 2 * block
    side = pair_side()
    for j in range(rows // 2):
        p_high[side, j], p_low[side, j] = split(far_0[j])
        p_high[1 - side, j], p_low[1 - side, j] = split(far_1[j])
    for u in range(rows):
        pos2, pos3 = tab[POS2 + u], tab[POS3 + u]
        a2 = a_high[u, :, :block], a_low[u, :, :block]
        a3 = a_high[u, :, block:], a_low[u, :, block:]
        left = dot3k(*a2, p_high[BELOW, pos2], p_low[BELOW, pos2])
        right = dot3k(*a3, p_high[ABOVE, pos3], p_low[ABOVE, pos3])
        labels = [tab[SIDE_LAB + 8 * which + 2 * pos + k] for which, pos in ((BELOW, pos2), (ABOVE, pos3)) for k in (0, 1)]
        own = part[u, :, half : 2 * half] + two_columns(left[:, block:], labels[1]) + two_columns(right[:, :block], labels[2])
        place = slice(u * block, (u + 1) * block)
        ap_high[place, half : 2 * half], ap_low[place, half : 2 * half] = split(own)
        for cols, value, label in (
            (slice(0, half), left[:, :block], labels[0]),
            (slice(2 * half, 3 * half), right[:, block:], labels[3]),
        ):
            high, low = split(value)
            ap_high[place, cols] = two_columns(high, label)
            ap_low[place, cols] = two_columns(low, label)
    coarse_rows(trans_high, trans_low, ap_high, ap_low, 1 - side, out_1)


def other_kernel(trans_high, trans_low, ap_high, ap_low, out_0):
    coarse_rows(trans_high, trans_low, ap_high, ap_low, pair_side(), out_0)


HELD = ((1, 0), (0, 0), (1, 1), (0, 1), (1, 2))


def own_kernel(own, ap1_high, ap1_low, ap2_high, ap2_low, out, trans_high, trans_low):
    rows, block = own.shape[0], own.shape[1]
    half = 2 * block
    for u in range(rows):
        place = slice(u * block, (u + 1) * block)
        high, low = split(own[u])
        trans_high[:, place] = high.T
        trans_low[:, place] = low.T
    aps = (ap1_high, ap1_low), (ap2_high, ap2_low)
    for d, (which, c) in enumerate(HELD):
        cols = slice(c * half, (c + 1) * half)
        high, low = aps[which]
        out[:, d * half : (d + 1) * half] = dot3(trans_high[...], trans_low[...], high[:, cols], low[:, cols])


def write_slots(inv, total, result, agg, d, out, sem):
    block = total.shape[0]
    value = dot3k(*inv, *split(total))
    result[0] = value[:, :block]
    result[1] = value[:, block:]
    copy = pltpu.make_async_copy(result, out.at[agg, pl.ds(2 * (d + 3), 2)], sem)
    copy.start()
    return copy


def both_sides(run):
    side = pair_side()
    pl.when(side == ABOVE)(lambda: run(ABOVE))
    pl.when(side == BELOW)(lambda: run(BELOW))


def early_kernel(inverse, own, first_0, first_1, second_0, out, waiting, results, sems):
    block = inverse.shape[1]
    half = 2 * block

    def run(side):
        shift_0, shift_1 = (1, -1) if side == ABOVE else (-1, 1)
        copies = []
        for agg in range(2):
            inv = split(inverse[agg])
            line = slice(agg * block, (agg + 1) * block)
            for d in range(-3, 4):
                total = None
                if -2 <= d <= 2:
                    total = own[line, (d + 2) * half : (d + 3) * half]
                late = None
                for shift, bufs in ((shift_0, (first_0, second_0)), (shift_1, (first_1, None))):
                    if -2 <= d - shift <= 2:
                        which, c = HELD[d - shift + 2]
                        if bufs[which] is None:
                            late = c
                            continue
                        part = bufs[which][line, c * half : (c + 1) * half]
                        total = part if total is None else total + part
                if late is not None:
                    waiting[agg, late] = jnp.zeros((block, half), F32) if total is None else total
                else:
                    n = len(copies)
                    copies.append(write_slots(inv, total, results.at[n], agg, d, out, sems.at[n]))
        for copy in copies:
            copy.wait()

    both_sides(run)


def late_kernel(inverse, waiting, second_1, partly, out, results, sems):
    block = inverse.shape[1]
    half = 2 * block

    def run(side):
        shift = -1 if side == ABOVE else 1
        copies = []
        for agg in range(2):
            inv = split(inverse[agg])
            line = slice(agg * block, (agg + 1) * block)
            for c in range(3):
                total = waiting[agg, c] + second_1[line, c * half : (c + 1) * half]
                n = len(copies)
                copies.append(write_slots(inv, total, results.at[n], agg, 2 * c - 2 + shift, out, sems.at[n]))
        for copy in copies:
            copy.wait()

    both_sides(run)


SMEM = pl.BlockSpec(memory_space=pltpu.SMEM)
VMEM = pl.BlockSpec(memory_space=pltpu.VMEM)
HBM = pl.BlockSpec(memory_space=pltpu.HBM)


def call(body, outs, ins, scratch=(), micros=1.0, in_hbm=(), out_hbm=(), aliases={}):
    def specs(values, in_place):
        return [HBM if i in in_place else SMEM if x.dtype == jnp.int32 else VMEM for i, x in enumerate(values)]

    return pl.pallas_call(
        body,
        out_shape=outs,
        in_specs=specs(ins, in_hbm),
        out_specs=specs(outs, out_hbm),
        scratch_shapes=[pltpu.VMEM(*x) if isinstance(x, tuple) else x for x in scratch],
        input_output_aliases=aliases,
        compiler_params=pltpu.CompilerParams(vmem_limit_bytes=24 * 2**20),
        cost_estimate=pl.CostEstimate(flops=int(micros * 1e9), bytes_accessed=2**20, transcendentals=0),
    )(*ins)


def shards(a, a_cols, t_blocks, t_agg, dinv, coarse_inv):
    devices = lax.axis_size(AXES)
    rows, block = t_blocks.shape[:2]
    width, half, deep = rows // 2, 2 * block, rows * block
    shape = jax.ShapeDtypeStruct
    full = lambda *dims: shape(dims, F32)
    pair = lambda *dims: [shape(dims, BF16), shape(dims, BF16)]
    two = lambda *dims: [(dims, BF16)] * 2
    tile = full(width, block, half)
    cols = a_cols.reshape(-1, ROW_CHUNK, 4).transpose(0, 2, 1).reshape(-1)

    tab, t_0, t_1, t = call(
        functools.partial(load_kernel, devices),
        [shape((TAB,), jnp.int32)] + [full(width, block, block)] * 2 + [full(*t_blocks.shape)],
        [pltpu.with_memory_space_constraint(x, pltpu.HBM) for x in (cols, t_agg, t_blocks)],
        [pltpu.SMEM(cols.shape, jnp.int32), pltpu.SMEM(t_agg.shape, jnp.int32), pltpu.SemaphoreType.DMA((3,))],
        micros=3,
        in_hbm=(0, 1, 2),
    )
    t_1 = exchanged(t_1, 1)
    t_0 = exchanged(t_0, 0)
    (near_1,) = call(near_sent_kernel, [tile], [tab, a, t, dinv], micros=2)
    got_near_1 = exchanged(near_1, 1)
    near_0, own = call(near_rest_kernel, [tile, full(rows, block, half)], [tab, a, t, dinv, near_1], micros=2)
    near_0, near_1 = exchanged(near_0, 0), got_near_1
    (far_1,) = call(far_sent_kernel, [tile], [tab, a, dinv, t_0, t_1, own], two(2, width, block, block), micros=2)
    got_far_1 = exchanged(far_1, 1)
    far_0, far = call(
        far_split_kernel,
        [tile, full(rows, block, half)],
        [tab, a, dinv, t_0, t_1, far_1],
        two(2, width, block, block),
        micros=2,
    )
    far_0, far_1 = exchanged(far_0, 0), got_far_1
    part, a23_high, a23_low, side_high, side_low = call(
        pre_kernel,
        [full(rows, block, 3 * half)] + pair(rows, block, half) + pair(2, half, deep),
        [tab, a, own, far],
        two(rows, block, half) * 3,
        micros=3,
    )
    ap1_high, ap1_low, first_1 = call(
        first_kernel,
        pair(deep, 2 * half) + [full(half, 2 * half)],
        [tab, a23_high, a23_low, part, side_high, side_low, near_0, near_1],
        two(2, width, block, half),
        micros=3,
    )
    first_1 = exchanged(first_1, 1)
    (first_0,) = call(other_kernel, [full(half, 2 * half)], [side_high, side_low, ap1_high, ap1_low], micros=1)
    first_0 = exchanged(first_0, 0)
    ap2_high, ap2_low, second_1 = call(
        second_kernel,
        pair(deep, 3 * half) + [full(half, 3 * half)],
        [tab, a23_high, a23_low, part, side_high, side_low, far_0, far_1, ap1_high],
        two(2, width, block, half),
        micros=3,
    )
    second_1 = exchanged(second_1, 1)
    (second_0,) = call(other_kernel, [full(half, 3 * half)], [side_high, side_low, ap2_high, ap2_low], micros=1)
    second_0 = exchanged(second_0, 0)
    (total,) = call(
        own_kernel, [full(half, 5 * half)], [own, ap1_high, ap1_low, ap2_high, ap2_low], two(half, deep), micros=2
    )
    result = full(2, 14, block, block)
    partly, waiting = call(
        early_kernel,
        [result, full(2, 3, block, half)],
        [coarse_inv, total, first_0, first_1, second_0],
        [((8, 2, block, block), F32), pltpu.SemaphoreType.DMA((8,))],
        micros=2,
        out_hbm=(0,),
    )
    (out,) = call(
        late_kernel,
        [result],
        [coarse_inv, waiting, second_1, partly],
        [((6, 2, block, block), F32), pltpu.SemaphoreType.DMA((6,))],
        micros=1,
        in_hbm=(3,),
        out_hbm=(0,),
        aliases={3: 0},
    )
    return out


def solution(mesh):
    placed = (
        P(AXES, None, None, None),
        P(),
        P(AXES, None, None),
        P(),
        P(AXES, None, None),
        P(AXES, None, None),
    )
    return jax.shard_map(
        shards,
        mesh=mesh,
        in_specs=placed,
        out_specs=P(AXES, None, None, None),
        check_vma=False,
    )
```

```python
import functools

import jax
import jax.numpy as jnp
from jax import lax
from jax.experimental import pallas as pl
from jax.experimental.pallas import tpu as pltpu
from jax.sharding import PartitionSpec as P


OMEGA = 0.6
AXES = ("gx", "gy")
F32 = jnp.float32
BF16 = jnp.bfloat16
ROW, NEAR, POS2, POS3, LIST_0, OWN_LAB, SIDE_LAB, TAB = 0, 8, 16, 24, 32, 48, 80, 128
BELOW, ABOVE = 0, 1
ROW_CHUNK = 128


def exchanged(value, first):
    count = lax.axis_size(AXES)
    pairs = []
    for low in range(first, count + first, 2):
        high = (low + 1) % count
        pairs += [(low, high), (high, low)]
    return lax.ppermute(value, AXES, pairs)


def pair_side():
    return 1 - lax.rem(lax.axis_index("gy"), 2)


def split(x):
    high = x.astype(BF16)
    return high, (x - high.astype(F32)).astype(BF16)


def dot(a, b):
    return jnp.dot(a, b, preferred_element_type=F32)


def dot3(a_high, a_low, b_high, b_low):
    return dot(a_high, b_high) + dot(a_low, b_high) + dot(a_high, b_low)


def dot3k(a_high, a_low, b_high, b_low):
    both = jnp.concatenate([a_high, a_low], axis=1)
    return dot(both, jnp.concatenate([b_high, b_high], axis=0)) + dot(a_high, b_low)


def load_kernel(devices, cols_hbm, agg_hbm, t_hbm, tab, t_0, t_1, t, cols, agg, rank, sem):
    rows, width = t.shape[0], t.shape[0] // 2
    device = lax.axis_index("gx") * lax.axis_size("gy") + lax.axis_index("gy")
    previous = lax.rem(device + devices - 1, devices)
    following = lax.rem(device + 1, devices)
    slabs = previous, following, device
    side = pair_side()
    shift = ROW_CHUNK.bit_length() - 1
    chunk = 4 * ROW_CHUNK
    copies = [
        pltpu.make_async_copy(
            cols_hbm.at[pl.ds(pl.multiple_of(((slab * rows) >> shift) * chunk, chunk), chunk)],
            cols.at[pl.ds(i * chunk, chunk)],
            sem.at[i],
        )
        for i, slab in enumerate(slabs)
    ]
    copies += [pltpu.make_async_copy(t_hbm, t, sem.at[3]), pltpu.make_async_copy(agg_hbm, agg, sem.at[4])]
    for copy in copies:
        copy.start()

    def col(i, r, k):
        return cols[i * chunk + k * ROW_CHUNK + ((slabs[i] * rows) & (ROW_CHUNK - 1)) + r]

    def rank_rows(i, k, where):
        mask = jnp.int32(0)
        for r in range(rows):
            mask = mask | (jnp.int32(1) << (col(i, r, k) & (rows - 1)))
        named, other = jnp.int32(0), jnp.int32(width)
        for r in range(rows):
            hit = (mask >> r) & 1
            place = jnp.where(hit == 1, named, other)
            rank[where * rows + r] = place
            rank[(where + 1) * rows + place] = r
            named = named + hit
            other = other + 1 - hit

    def ranked(where, r):
        return rank[where * rows + r]

    copies[0].wait()
    copies[1].wait()
    rank_rows(0, 3, 0)
    rank_rows(1, 2, 2)
    sent_1, sent_0 = jnp.where(side == ABOVE, 0, 2), jnp.where(side == ABOVE, 2, 0)
    copies[3].wait()
    for j in range(width):
        t_1[j] = t[ranked(sent_1 + 1, j)]
        t_0[j] = t[ranked(sent_0 + 1, j)]
    copies[2].wait()
    copies[4].wait()
    rank_rows(2, 2, 4)
    rank_rows(2, 3, 6)
    for j in range(width):
        tab[LIST_0 + j] = ranked(sent_1, ranked(sent_0 + 1, j))
        for which in (BELOW, ABOVE):
            for k in range(2):
                tab[SIDE_LAB + 8 * which + 2 * j + k] = agg[col(which, ranked(5 + 2 * which, j), 2 + k)]
    for u in range(rows):
        row = ranked(sent_1 + 1, u)
        tab[ROW + u] = row
        tab[NEAR + u] = ranked(sent_1, col(2, row, 1) & (rows - 1))
        tab[POS2 + u] = ranked(4, col(2, row, 2) & (rows - 1))
        tab[POS3 + u] = ranked(6, col(2, row, 3) & (rows - 1))
        for k in range(4):
            tab[OWN_LAB + 4 * u + k] = agg[col(2, row, k)]


def put(value, label, column):
    return jnp.where(label == column, value, jnp.zeros_like(value))


def two_columns(value, label):
    return jnp.concatenate([put(value, label, 0), put(value, label, 1)], axis=1)


def near_tile(tab, a, t, dinv, u):
    block = t.shape[1]
    row = tab[ROW + u]
    near = tab[ROW + tab[NEAR + u]]
    prod = jnp.concatenate(
        [dot3k(*split(a[row, 0]), *split(t[row])), dot3k(*split(a[row, 1]), *split(t[near]))], axis=1
    )
    smoothed = dot3k(*split(dinv[row]), *split(prod))
    p0 = t[row] - OMEGA * smoothed[:, :block]
    p1 = -OMEGA * smoothed[:, block:]
    return two_columns(p0, tab[OWN_LAB + 4 * u]) + two_columns(p1, tab[OWN_LAB + 4 * u + 1])


def near_sent_kernel(tab, a, t, dinv, near_1):
    for u in range(near_1.shape[0]):
        near_1[u] = near_tile(tab, a, t, dinv, u)


def wide(ref, *places):
    return jnp.concatenate([ref[place] for place in places], axis=0)


def near_rest_kernel(tab, a, t, dinv, near_1, near_0, own, part, a_high, a_low, own_high, own_low):
    width = near_1.shape[0]
    for u in range(width):
        own[u] = near_1[u]
        own[width + u] = near_tile(tab, a, t, dinv, width + u)
    for j in range(width):
        near_0[j] = own[tab[LIST_0 + j]]
    for u in range(2 * width):
        own_high[u], own_low[u] = split(own[u])
    for u in range(2 * width):
        row, near = tab[ROW + u], tab[NEAR + u]
        a_high[u], a_low[u] = split(jnp.concatenate([a[row, 0], a[row, 1]], axis=1))
        part[u] = dot3(a_high[u], a_low[u], wide(own_high, u, near), wide(own_low, u, near))


def far_kernel(tab, a, dinv, t_0, t_1, after, far_0, far_1, far, a_high, a_low, t_high, t_low):
    rows, block = dinv.shape[0], dinv.shape[1]
    width = rows // 2
    side = pair_side()
    for j in range(width):
        t_high[side, j], t_low[side, j] = split(t_0[j])
        t_high[1 - side, j], t_low[1 - side, j] = split(t_1[j])
    for u in range(rows):
        row = tab[ROW + u]
        below, above = tab[POS2 + u], tab[POS3 + u]
        a2, a3 = split(a[row, 2]), split(a[row, 3])
        a_high[u] = jnp.concatenate([a2[0], a3[0]], axis=1)
        a_low[u] = jnp.concatenate([a2[1], a3[1]], axis=1)
        prod = jnp.concatenate(
            [
                dot3k(*a2, t_high[BELOW, below], t_low[BELOW, below]),
                dot3k(*a3, t_high[ABOVE, above], t_low[ABOVE, above]),
            ],
            axis=1,
        )
        both = -OMEGA * dot3k(*split(dinv[row]), *split(prod))
        far[u, BELOW] = both[:, :block]
        far[u, ABOVE] = both[:, block:]
    for j in range(width):
        far_1[j] = far[j]
        far_0[j] = far[tab[LIST_0 + j]]


def store_turned(trans, label, place, value):
    block = value.shape[0]
    trans[pl.ds(pl.multiple_of(label * block, block), block), place] = value.T
    trans[pl.ds(pl.multiple_of((1 - label) * block, block), block), place] = jnp.zeros_like(value)


def turn(tab, far, side, trans_high, trans_low):
    for u in range(far.shape[0]):
        block = far.shape[2]
        label = tab[OWN_LAB + 4 * u + 2 + side]
        high, low = split(far[u, side])
        place = slice(u * block, (u + 1) * block)
        store_turned(trans_high, label, place, high)
        store_turned(trans_low, label, place, low)


def pre_kernel(
    tab, a_high, a_low, far,
    part, trans_high, trans_low,
    far_high, far_low,
):
    rows, block = far.shape[0], far.shape[2]
    half = 2 * block
    for u in range(rows):
        for side in (BELOW, ABOVE):
            label = tab[OWN_LAB + 4 * u + 2 + side]
            high, low = split(far[u, side])
            far_high[side, u] = two_columns(high, label)
            far_low[side, u] = two_columns(low, label)
    turn(tab, far, 1 - pair_side(), trans_high, trans_low)
    for u in range(rows):
        near = tab[NEAR + u]
        for side in (BELOW, ABOVE):
            part[u, :, side * half : (side + 1) * half] = dot3(
                a_high[u], a_low[u], wide(far_high.at[side], u, near), wide(far_low.at[side], u, near)
            )


def coarse_rows(trans_high, trans_low, ap_high, ap_low, out, start=0):
    half = trans_high.shape[0]
    for c in range(ap_high.shape[1] // half):
        cols = slice(c * half, (c + 1) * half)
        out[:, start + c * half : start + (c + 1) * half] = dot3(
            trans_high[...], trans_low[...], ap_high[:, cols], ap_low[:, cols]
        )


def first_kernel(
    tab, a_high, a_low, part, trans_high, trans_low, near_0, near_1,
    ap_high, ap_low, out_1,
    p_high, p_low,
):
    rows, block = a_high.shape[0], a_high.shape[1]
    half = 2 * block
    side = pair_side()
    for j in range(rows // 2):
        p_high[side, j], p_low[side, j] = split(near_0[j])
        p_high[1 - side, j], p_low[1 - side, j] = split(near_1[j])
    for u in range(rows):
        pos2, pos3 = tab[POS2 + u], tab[POS3 + u]
        a2 = a_high[u, :, :block], a_low[u, :, :block]
        a3 = a_high[u, :, block:], a_low[u, :, block:]
        low = part[u, :, :half] + dot3k(*a2, p_high[BELOW, pos2], p_low[BELOW, pos2])
        upp = part[u, :, half:] + dot3k(*a3, p_high[ABOVE, pos3], p_low[ABOVE, pos3])
        place = slice(u * block, (u + 1) * block)
        ap_high[place, :half], ap_low[place, :half] = split(low)
        ap_high[place, half:], ap_low[place, half:] = split(upp)
    coarse_rows(trans_high, trans_low, ap_high, ap_low, out_1)


def second_kernel(
    tab, a_high, a_low, part, trans_high, trans_low, far_0, far_1, after,
    ap_high, ap_low, out_1,
    p_high, p_low,
):
    rows, block = a_high.shape[0], a_high.shape[1]
    half = 2 * block
    side = pair_side()
    for j in range(rows // 2):
        for q in range(2):
            cols = slice(q * block, (q + 1) * block)
            p_high[side, j, :, cols], p_low[side, j, :, cols] = split(far_0[j, q])
            p_high[1 - side, j, :, cols], p_low[1 - side, j, :, cols] = split(far_1[j, q])
    for u in range(rows):
        pos2, pos3 = tab[POS2 + u], tab[POS3 + u]
        a2 = a_high[u, :, :block], a_low[u, :, :block]
        a3 = a_high[u, :, block:], a_low[u, :, block:]
        left = dot3k(*a2, p_high[BELOW, pos2], p_low[BELOW, pos2])
        right = dot3k(*a3, p_high[ABOVE, pos3], p_low[ABOVE, pos3])
        labels = [tab[SIDE_LAB + 8 * which + 2 * pos + k] for which, pos in ((BELOW, pos2), (ABOVE, pos3)) for k in (0, 1)]
        own = part[u] + two_columns(left[:, block:], labels[1]) + two_columns(right[:, :block], labels[2])
        place = slice(u * block, (u + 1) * block)
        ap_high[place, half : 2 * half], ap_low[place, half : 2 * half] = split(own)
        for cols, value, label in (
            (slice(0, half), left[:, :block], labels[0]),
            (slice(2 * half, 3 * half), right[:, block:], labels[3]),
        ):
            high, low = split(value)
            ap_high[place, cols] = two_columns(high, label)
            ap_low[place, cols] = two_columns(low, label)
    coarse_rows(trans_high, trans_low, ap_high, ap_low, out_1)


def other_kernel(tab, far, ap1_high, ap1_low, ap2_high, ap2_low, out_0, trans_high, trans_low):
    turn(tab, far, pair_side(), trans_high, trans_low)
    coarse_rows(trans_high, trans_low, ap1_high, ap1_low, out_0)
    coarse_rows(trans_high, trans_low, ap2_high, ap2_low, out_0, ap1_high.shape[1])


HELD = ((1, 0), (0, 0), (1, 1), (0, 1), (1, 2))


def own_kernel(own, ap1_high, ap1_low, ap2_high, ap2_low, out, trans_high, trans_low):
    rows, block = own.shape[0], own.shape[1]
    half = 2 * block
    for u in range(rows):
        place = slice(u * block, (u + 1) * block)
        high, low = split(own[u])
        trans_high[:, place] = high.T
        trans_low[:, place] = low.T
    aps = (ap1_high, ap1_low), (ap2_high, ap2_low)
    for d, (which, c) in enumerate(HELD):
        cols = slice(c * half, (c + 1) * half)
        high, low = aps[which]
        out[:, d * half : (d + 1) * half] = dot3(trans_high[...], trans_low[...], high[:, cols], low[:, cols])


def write_slots(inv, total, result, agg, d, out, sem):
    block = total.shape[0]
    value = dot3k(*inv, *split(total))
    result[0] = value[:, :block]
    result[1] = value[:, block:]
    copy = pltpu.make_async_copy(result, out.at[agg, pl.ds(2 * (d + 3), 2)], sem)
    copy.start()
    return copy


def both_sides(run):
    side = pair_side()
    pl.when(side == ABOVE)(lambda: run(ABOVE))
    pl.when(side == BELOW)(lambda: run(BELOW))


def early_kernel(inverse, own, both_0, first_1, out, waiting, results, sems):
    block = inverse.shape[1]
    half = 2 * block

    def run(side):
        shift_0, shift_1 = (1, -1) if side == ABOVE else (-1, 1)
        copies = []
        for agg in range(2):
            inv = split(inverse[agg])
            line = slice(agg * block, (agg + 1) * block)
            for d in range(-3, 4):
                parts, late = [], None
                if -2 <= d <= 2:
                    parts.append(own[line, (d + 2) * half : (d + 3) * half])
                if -2 <= d - shift_0 <= 2:
                    which, c = HELD[d - shift_0 + 2]
                    c = c + 2 * which
                    parts.append(both_0[line, c * half : (c + 1) * half])
                if -2 <= d - shift_1 <= 2:
                    which, c = HELD[d - shift_1 + 2]
                    if which:
                        late = c
                    else:
                        parts.append(first_1[line, c * half : (c + 1) * half])
                total = sum(parts[1:], parts[0]) if parts else jnp.zeros((block, half), F32)
                if late is not None:
                    waiting[agg, late] = total
                else:
                    n = len(copies)
                    copies.append(write_slots(inv, total, results.at[n], agg, d, out, sems.at[n]))
        for copy in copies:
            copy.wait()

    both_sides(run)


def late_kernel(inverse, waiting, second_1, partly, out, results, sems):
    block = inverse.shape[1]
    half = 2 * block

    def run(side):
        shift = -1 if side == ABOVE else 1
        copies = []
        for agg in range(2):
            inv = split(inverse[agg])
            line = slice(agg * block, (agg + 1) * block)
            for c in range(3):
                total = waiting[agg, c] + second_1[line, c * half : (c + 1) * half]
                n = len(copies)
                copies.append(write_slots(inv, total, results.at[n], agg, 2 * c - 2 + shift, out, sems.at[n]))
        for copy in copies:
            copy.wait()

    both_sides(run)


SMEM = pl.BlockSpec(memory_space=pltpu.SMEM)
VMEM = pl.BlockSpec(memory_space=pltpu.VMEM)
HBM = pl.BlockSpec(memory_space=pltpu.HBM)


def call(body, outs, ins, scratch=(), micros=1.0, in_hbm=(), out_hbm=(), aliases={}):
    def specs(values, in_place):
        return [HBM if i in in_place else SMEM if x.dtype == jnp.int32 else VMEM for i, x in enumerate(values)]

    return pl.pallas_call(
        body,
        out_shape=outs,
        in_specs=specs(ins, in_hbm),
        out_specs=specs(outs, out_hbm),
        scratch_shapes=[pltpu.VMEM(*x) if isinstance(x, tuple) else x for x in scratch],
        input_output_aliases=aliases,
        compiler_params=pltpu.CompilerParams(vmem_limit_bytes=24 * 2**20),
        cost_estimate=pl.CostEstimate(flops=int(micros * 1e9), bytes_accessed=2**20, transcendentals=0),
    )(*ins)


def shards(a, a_cols, t_blocks, t_agg, dinv, coarse_inv):
    devices = lax.axis_size(AXES)
    rows, block = t_blocks.shape[:2]
    width, half, deep = rows // 2, 2 * block, rows * block
    shape = jax.ShapeDtypeStruct
    full = lambda *dims: shape(dims, F32)
    pair = lambda *dims: [shape(dims, BF16), shape(dims, BF16)]
    two = lambda *dims: [(dims, BF16)] * 2
    tile = full(width, block, half)
    cols = a_cols.reshape(-1, ROW_CHUNK, 4).transpose(0, 2, 1).reshape(-1)

    tab, t_0, t_1, t = call(
        functools.partial(load_kernel, devices),
        [shape((TAB,), jnp.int32)] + [full(width, block, block)] * 2 + [full(*t_blocks.shape)],
        [pltpu.with_memory_space_constraint(x, pltpu.HBM) for x in (cols, t_agg, t_blocks)],
        [
            pltpu.SMEM((3 * 4 * ROW_CHUNK,), jnp.int32),
            pltpu.SMEM(t_agg.shape, jnp.int32),
            pltpu.SMEM((8 * rows,), jnp.int32),
            pltpu.SemaphoreType.DMA((5,)),
        ],
        micros=3,
        in_hbm=(0, 1, 2),
    )
    t_1 = exchanged(t_1, 1)
    t_0 = exchanged(t_0, 0)
    (near_1,) = call(near_sent_kernel, [tile], [tab, a, t, dinv], micros=2)
    got_near_1 = exchanged(near_1, 1)
    near_0, own, part_own, a01_high, a01_low = call(
        near_rest_kernel,
        [tile] + [full(rows, block, half)] * 2 + pair(rows, block, half),
        [tab, a, t, dinv, near_1],
        two(rows, block, half),
        micros=2,
    )
    near_0, near_1 = exchanged(near_0, 0), got_near_1
    sent = full(width, 2, block, block)
    far_0, far_1, far, a23_high, a23_low = call(
        far_kernel,
        [sent, sent, full(rows, 2, block, block)] + pair(rows, block, half),
        [tab, a, dinv, t_0, t_1, own],
        two(2, width, block, block),
        micros=2,
    )
    far_1 = exchanged(far_1, 1)
    far_0 = exchanged(far_0, 0)
    part, out_high, out_low = call(
        pre_kernel,
        [full(rows, block, 2 * half)] + pair(half, deep),
        [tab, a01_high, a01_low, far],
        two(2, rows, block, half),
        micros=3,
    )
    ap1_high, ap1_low, first_1 = call(
        first_kernel,
        pair(deep, 2 * half) + [full(half, 2 * half)],
        [tab, a23_high, a23_low, part, out_high, out_low, near_0, near_1],
        two(2, width, block, half),
        micros=3,
    )
    first_1 = exchanged(first_1, 1)
    ap2_high, ap2_low, second_1 = call(
        second_kernel,
        pair(deep, 3 * half) + [full(half, 3 * half)],
        [tab, a23_high, a23_low, part_own, out_high, out_low, far_0, far_1, ap1_high],
        two(2, width, block, half),
        micros=3,
    )
    second_1 = exchanged(second_1, 1)
    (both_0,) = call(
        other_kernel,
        [full(half, 5 * half)],
        [tab, far, ap1_high, ap1_low, ap2_high, ap2_low],
        two(half, deep),
        micros=2,
    )
    both_0 = exchanged(both_0, 0)
    (total,) = call(
        own_kernel, [full(half, 5 * half)], [own, ap1_high, ap1_low, ap2_high, ap2_low], two(half, deep), micros=2
    )
    result = full(2, 14, block, block)
    partly, waiting = call(
        early_kernel,
        [result, full(2, 3, block, half)],
        [coarse_inv, total, both_0, first_1],
        [((8, 2, block, block), F32), pltpu.SemaphoreType.DMA((8,))],
        micros=2,
        out_hbm=(0,),
    )
    (out,) = call(
        late_kernel,
        [result],
        [coarse_inv, waiting, second_1, partly],
        [((6, 2, block, block), F32), pltpu.SemaphoreType.DMA((6,))],
        micros=1,
        in_hbm=(3,),
        out_hbm=(0,),
        aliases={3: 0},
    )
    return out


def solution(mesh):
    placed = (
        P(AXES, None, None, None),
        P(),
        P(AXES, None, None),
        P(),
        P(AXES, None, None),
        P(AXES, None, None),
    )
    return jax.shard_map(
        shards,
        mesh=mesh,
        in_specs=placed,
        out_specs=P(AXES, None, None, None),
        check_vma=False,
    )
```

```python
import functools

import jax
import jax.numpy as jnp
from jax import lax
from jax.experimental import pallas as pl
from jax.experimental.pallas import tpu as pltpu
from jax.sharding import PartitionSpec as P


OMEGA = 0.6
AXES = ("gx", "gy")
F32 = jnp.float32
BF16 = jnp.bfloat16
ROW, NEAR, POS2, POS3, LIST_0, OWN_LAB, SIDE_LAB, TAB = 0, 8, 16, 24, 32, 40, 72, 88
LANES = 128
BELOW, ABOVE = 0, 1
ROW_CHUNK = 128


def exchanged(value, first):
    count = lax.axis_size(AXES)
    pairs = []
    for low in range(first, count + first, 2):
        high = (low + 1) % count
        pairs += [(low, high), (high, low)]
    return lax.ppermute(value, AXES, pairs)


def pair_side():
    return 1 - lax.rem(lax.axis_index("gy"), 2)


def split(x):
    high = x.astype(BF16)
    return high, (x - high.astype(F32)).astype(BF16)


def dot(a, b):
    return jnp.dot(a, b, preferred_element_type=F32)


def dot3(a_high, a_low, b_high, b_low):
    return dot(a_high, b_high) + dot(a_low, b_high) + dot(a_high, b_low)


def dot3k(a_high, a_low, b_high, b_low):
    both = jnp.concatenate([a_high, a_low], axis=1)
    return dot(both, jnp.concatenate([b_high, b_high], axis=0)) + dot(a_high, b_low)


def note(tab, i, value):
    tab[pl.ds(i, 1), :] = jnp.full((1, tab.shape[1]), value, jnp.int32)


def entry(tab, i):
    return tab[pl.ds(i, 1), :][0, 0]


def load_kernel(devices, cols_hbm, agg_hbm, t_hbm, tab, t_0, t_1, t, cols, agg, rank, sem):
    rows, width = t.shape[0], t.shape[0] // 2
    device = lax.axis_index("gx") * lax.axis_size("gy") + lax.axis_index("gy")
    previous = lax.rem(device + devices - 1, devices)
    following = lax.rem(device + 1, devices)
    slabs = previous, following, device
    side = pair_side()
    shift = ROW_CHUNK.bit_length() - 1
    chunk = 4 * ROW_CHUNK
    copies = [
        pltpu.make_async_copy(
            cols_hbm.at[pl.ds(pl.multiple_of(((slab * rows) >> shift) * chunk, chunk), chunk)],
            cols.at[pl.ds(i * chunk, chunk)],
            sem.at[i],
        )
        for i, slab in enumerate(slabs)
    ]
    copies += [pltpu.make_async_copy(t_hbm, t, sem.at[3]), pltpu.make_async_copy(agg_hbm, agg, sem.at[4])]
    for copy in copies:
        copy.start()

    def col(i, r, k):
        return cols[i * chunk + k * ROW_CHUNK + ((slabs[i] * rows) & (ROW_CHUNK - 1)) + r]

    def rank_rows(i, k, where):
        mask = jnp.int32(0)
        for r in range(rows):
            mask = mask | (jnp.int32(1) << (col(i, r, k) & (rows - 1)))
        named, other = jnp.int32(0), jnp.int32(width)
        for r in range(rows):
            hit = (mask >> r) & 1
            place = jnp.where(hit == 1, named, other)
            rank[where * rows + r] = place
            rank[(where + 1) * rows + place] = r
            named = named + hit
            other = other + 1 - hit

    def ranked(where, r):
        return rank[where * rows + r]

    copies[0].wait()
    copies[1].wait()
    rank_rows(0, 3, 0)
    rank_rows(1, 2, 2)
    sent_1, sent_0 = jnp.where(side == ABOVE, 0, 2), jnp.where(side == ABOVE, 2, 0)
    copies[3].wait()
    for j in range(width):
        t_1[j] = t[ranked(sent_1 + 1, j)]
        t_0[j] = t[ranked(sent_0 + 1, j)]
    copies[2].wait()
    copies[4].wait()
    rank_rows(2, 2, 4)
    rank_rows(2, 3, 6)
    for j in range(width):
        note(tab, LIST_0 + j, ranked(sent_1, ranked(sent_0 + 1, j)))
        for which in (BELOW, ABOVE):
            for k in range(2):
                note(tab, SIDE_LAB + 8 * which + 2 * j + k, agg[col(which, ranked(5 + 2 * which, j), 2 + k)])
    for u in range(rows):
        row = ranked(sent_1 + 1, u)
        note(tab, ROW + u, row)
        note(tab, NEAR + u, ranked(sent_1, col(2, row, 1) & (rows - 1)))
        note(tab, POS2 + u, ranked(4, col(2, row, 2) & (rows - 1)))
        note(tab, POS3 + u, ranked(6, col(2, row, 3) & (rows - 1)))
        for k in range(4):
            note(tab, OWN_LAB + 4 * u + k, agg[col(2, row, k)])


def put(value, label, column):
    return jnp.where(label == column, value, jnp.zeros_like(value))


def two_columns(value, label):
    return jnp.concatenate([put(value, label, 0), put(value, label, 1)], axis=1)


def near_tile(tab, a, t, dinv, u):
    block = t.shape[1]
    row = entry(tab, ROW + u)
    near = entry(tab, ROW + entry(tab, NEAR + u))
    prod = jnp.concatenate(
        [dot3k(*split(a[row, 0]), *split(t[row])), dot3k(*split(a[row, 1]), *split(t[near]))], axis=1
    )
    smoothed = dot3k(*split(dinv[row]), *split(prod))
    p0 = t[row] - OMEGA * smoothed[:, :block]
    p1 = -OMEGA * smoothed[:, block:]
    return two_columns(p0, entry(tab, OWN_LAB + 4 * u)) + two_columns(p1, entry(tab, OWN_LAB + 4 * u + 1))


def near_sent_kernel(tab, a, t, dinv, near_1):
    for u in range(near_1.shape[0]):
        near_1[u] = near_tile(tab, a, t, dinv, u)


def wide(ref, *places):
    return jnp.concatenate([ref[place] for place in places], axis=0)


def near_rest_kernel(tab, a, t, dinv, near_1, near_0, own, part, a_high, a_low, own_high, own_low):
    width = near_1.shape[0]
    for u in range(width):
        own[u] = near_1[u]
        own[width + u] = near_tile(tab, a, t, dinv, width + u)
    for j in range(width):
        near_0[j] = own[entry(tab, LIST_0 + j)]
    for u in range(2 * width):
        own_high[u], own_low[u] = split(own[u])
    for u in range(2 * width):
        row, near = entry(tab, ROW + u), entry(tab, NEAR + u)
        a_high[u], a_low[u] = split(jnp.concatenate([a[row, 0], a[row, 1]], axis=1))
        part[u] = dot3(a_high[u], a_low[u], wide(own_high, u, near), wide(own_low, u, near))


def far_kernel(tab, a, dinv, t_0, t_1, after, far_0, far_1, far, a_high, a_low, t_high, t_low):
    rows, block = dinv.shape[0], dinv.shape[1]
    width = rows // 2
    side = pair_side()
    for j in range(width):
        t_high[side, j], t_low[side, j] = split(t_0[j])
        t_high[1 - side, j], t_low[1 - side, j] = split(t_1[j])
    for u in range(rows):
        row = entry(tab, ROW + u)
        below, above = entry(tab, POS2 + u), entry(tab, POS3 + u)
        a2, a3 = split(a[row, 2]), split(a[row, 3])
        a_high[u] = jnp.concatenate([a2[0], a3[0]], axis=1)
        a_low[u] = jnp.concatenate([a2[1], a3[1]], axis=1)
        prod = jnp.concatenate(
            [
                dot3k(*a2, t_high[BELOW, below], t_low[BELOW, below]),
                dot3k(*a3, t_high[ABOVE, above], t_low[ABOVE, above]),
            ],
            axis=1,
        )
        both = -OMEGA * dot3k(*split(dinv[row]), *split(prod))
        far[u, BELOW] = both[:, :block]
        far[u, ABOVE] = both[:, block:]
    for j in range(width):
        far_1[j] = far[j]
        far_0[j] = far[entry(tab, LIST_0 + j)]


def store_turned(trans, label, place, value):
    block = value.shape[0]
    trans[pl.ds(pl.multiple_of(label * block, block), block), place] = value.T
    trans[pl.ds(pl.multiple_of((1 - label) * block, block), block), place] = jnp.zeros_like(value)


def turn(tab, far, side, trans_high, trans_low):
    for u in range(far.shape[0]):
        block = far.shape[2]
        label = entry(tab, OWN_LAB + 4 * u + 2 + side)
        high, low = split(far[u, side])
        place = slice(u * block, (u + 1) * block)
        store_turned(trans_high, label, place, high)
        store_turned(trans_low, label, place, low)


def pre_kernel(
    tab, a_high, a_low, far,
    part, trans_high, trans_low,
    far_high, far_low,
):
    rows, block = far.shape[0], far.shape[2]
    half = 2 * block
    for u in range(rows):
        for side in (BELOW, ABOVE):
            label = entry(tab, OWN_LAB + 4 * u + 2 + side)
            high, low = split(far[u, side])
            far_high[side, u] = two_columns(high, label)
            far_low[side, u] = two_columns(low, label)
    turn(tab, far, 1 - pair_side(), trans_high, trans_low)
    for u in range(rows):
        near = entry(tab, NEAR + u)
        for side in (BELOW, ABOVE):
            part[u, :, side * half : (side + 1) * half] = dot3(
                a_high[u], a_low[u], wide(far_high.at[side], u, near), wide(far_low.at[side], u, near)
            )


def coarse_rows(trans_high, trans_low, ap_high, ap_low, out, start=0):
    half = trans_high.shape[0]
    for c in range(ap_high.shape[1] // half):
        cols = slice(c * half, (c + 1) * half)
        out[:, start + c * half : start + (c + 1) * half] = dot3(
            trans_high[...], trans_low[...], ap_high[:, cols], ap_low[:, cols]
        )


def first_kernel(
    tab, a_high, a_low, part, trans_high, trans_low, near_0, near_1,
    ap_high, ap_low, out_1,
    p_high, p_low,
):
    rows, block = a_high.shape[0], a_high.shape[1]
    half = 2 * block
    side = pair_side()
    for j in range(rows // 2):
        p_high[side, j], p_low[side, j] = split(near_0[j])
        p_high[1 - side, j], p_low[1 - side, j] = split(near_1[j])
    for u in range(rows):
        pos2, pos3 = entry(tab, POS2 + u), entry(tab, POS3 + u)
        a2 = a_high[u, :, :block], a_low[u, :, :block]
        a3 = a_high[u, :, block:], a_low[u, :, block:]
        low = part[u, :, :half] + dot3k(*a2, p_high[BELOW, pos2], p_low[BELOW, pos2])
        upp = part[u, :, half:] + dot3k(*a3, p_high[ABOVE, pos3], p_low[ABOVE, pos3])
        place = slice(u * block, (u + 1) * block)
        ap_high[place, :half], ap_low[place, :half] = split(low)
        ap_high[place, half:], ap_low[place, half:] = split(upp)
    coarse_rows(trans_high, trans_low, ap_high, ap_low, out_1)


def second_kernel(
    tab, a_high, a_low, part, trans_high, trans_low, far_0, far_1, after,
    ap_high, ap_low, out_1,
    p_high, p_low,
):
    rows, block = a_high.shape[0], a_high.shape[1]
    half = 2 * block
    side = pair_side()
    for j in range(rows // 2):
        for q in range(2):
            cols = slice(q * block, (q + 1) * block)
            p_high[side, j, :, cols], p_low[side, j, :, cols] = split(far_0[j, q])
            p_high[1 - side, j, :, cols], p_low[1 - side, j, :, cols] = split(far_1[j, q])
    for u in range(rows):
        pos2, pos3 = entry(tab, POS2 + u), entry(tab, POS3 + u)
        a2 = a_high[u, :, :block], a_low[u, :, :block]
        a3 = a_high[u, :, block:], a_low[u, :, block:]
        left = dot3k(*a2, p_high[BELOW, pos2], p_low[BELOW, pos2])
        right = dot3k(*a3, p_high[ABOVE, pos3], p_low[ABOVE, pos3])
        labels = [entry(tab, SIDE_LAB + 8 * which + 2 * pos + k) for which, pos in ((BELOW, pos2), (ABOVE, pos3)) for k in (0, 1)]
        own = part[u] + two_columns(left[:, block:], labels[1]) + two_columns(right[:, :block], labels[2])
        place = slice(u * block, (u + 1) * block)
        ap_high[place, half : 2 * half], ap_low[place, half : 2 * half] = split(own)
        for cols, value, label in (
            (slice(0, half), left[:, :block], labels[0]),
            (slice(2 * half, 3 * half), right[:, block:], labels[3]),
        ):
            high, low = split(value)
            ap_high[place, cols] = two_columns(high, label)
            ap_low[place, cols] = two_columns(low, label)
    coarse_rows(trans_high, trans_low, ap_high, ap_low, out_1)


def other_kernel(tab, far, ap1_high, ap1_low, ap2_high, ap2_low, out_0, trans_high, trans_low):
    turn(tab, far, pair_side(), trans_high, trans_low)
    coarse_rows(trans_high, trans_low, ap1_high, ap1_low, out_0)
    coarse_rows(trans_high, trans_low, ap2_high, ap2_low, out_0, ap1_high.shape[1])


HELD = ((1, 0), (0, 0), (1, 1), (0, 1), (1, 2))


def own_kernel(own, ap1_high, ap1_low, ap2_high, ap2_low, out, trans_high, trans_low):
    rows, block = own.shape[0], own.shape[1]
    half = 2 * block
    for u in range(rows):
        place = slice(u * block, (u + 1) * block)
        high, low = split(own[u])
        trans_high[:, place] = high.T
        trans_low[:, place] = low.T
    aps = (ap1_high, ap1_low), (ap2_high, ap2_low)
    for d, (which, c) in enumerate(HELD):
        cols = slice(c * half, (c + 1) * half)
        high, low = aps[which]
        out[:, d * half : (d + 1) * half] = dot3(trans_high[...], trans_low[...], high[:, cols], low[:, cols])


def write_slots(inv, total, result, agg, d, out, sem):
    block = total.shape[0]
    value = dot3k(*inv, *split(total))
    result[0] = value[:, :block]
    result[1] = value[:, block:]
    copy = pltpu.make_async_copy(result, out.at[agg, pl.ds(2 * (d + 3), 2)], sem)
    copy.start()
    return copy


def both_sides(run):
    side = pair_side()
    pl.when(side == ABOVE)(lambda: run(ABOVE))
    pl.when(side == BELOW)(lambda: run(BELOW))


def early_kernel(inverse, own, both_0, first_1, out, waiting, results, sems):
    block = inverse.shape[1]
    half = 2 * block

    def run(side):
        shift_0, shift_1 = (1, -1) if side == ABOVE else (-1, 1)
        copies = []
        for agg in range(2):
            inv = split(inverse[agg])
            line = slice(agg * block, (agg + 1) * block)
            for d in range(-3, 4):
                parts, late = [], None
                if -2 <= d <= 2:
                    parts.append(own[line, (d + 2) * half : (d + 3) * half])
                if -2 <= d - shift_0 <= 2:
                    which, c = HELD[d - shift_0 + 2]
                    c = c + 2 * which
                    parts.append(both_0[line, c * half : (c + 1) * half])
                if -2 <= d - shift_1 <= 2:
                    which, c = HELD[d - shift_1 + 2]
                    if which:
                        late = c
                    else:
                        parts.append(first_1[line, c * half : (c + 1) * half])
                total = sum(parts[1:], parts[0]) if parts else jnp.zeros((block, half), F32)
                if late is not None:
                    waiting[agg, late] = total
                else:
                    n = len(copies)
                    copies.append(write_slots(inv, total, results.at[n], agg, d, out, sems.at[n]))
        for copy in copies:
            copy.wait()

    both_sides(run)


def late_kernel(inverse, waiting, second_1, partly, out, results, sems):
    block = inverse.shape[1]
    half = 2 * block

    def run(side):
        shift = -1 if side == ABOVE else 1
        copies = []
        for agg in range(2):
            inv = split(inverse[agg])
            line = slice(agg * block, (agg + 1) * block)
            for c in range(3):
                total = waiting[agg, c] + second_1[line, c * half : (c + 1) * half]
                n = len(copies)
                copies.append(write_slots(inv, total, results.at[n], agg, 2 * c - 2 + shift, out, sems.at[n]))
        for copy in copies:
            copy.wait()

    both_sides(run)


VMEM = pl.BlockSpec(memory_space=pltpu.VMEM)
HBM = pl.BlockSpec(memory_space=pltpu.HBM)


def call(body, outs, ins, scratch=(), micros=1.0, in_hbm=(), out_hbm=(), aliases={}):
    def specs(values, in_place):
        return [HBM if i in in_place else VMEM for i, x in enumerate(values)]

    return pl.pallas_call(
        body,
        out_shape=outs,
        in_specs=specs(ins, in_hbm),
        out_specs=specs(outs, out_hbm),
        scratch_shapes=[pltpu.VMEM(*x) if isinstance(x, tuple) else x for x in scratch],
        input_output_aliases=aliases,
        compiler_params=pltpu.CompilerParams(vmem_limit_bytes=24 * 2**20),
        cost_estimate=pl.CostEstimate(flops=int(micros * 1e9), bytes_accessed=2**20, transcendentals=0),
    )(*ins)


def shards(a, a_cols, t_blocks, t_agg, dinv, coarse_inv):
    devices = lax.axis_size(AXES)
    rows, block = t_blocks.shape[:2]
    width, half, deep = rows // 2, 2 * block, rows * block
    shape = jax.ShapeDtypeStruct
    full = lambda *dims: shape(dims, F32)
    pair = lambda *dims: [shape(dims, BF16), shape(dims, BF16)]
    two = lambda *dims: [(dims, BF16)] * 2
    tile = full(width, block, half)
    cols = a_cols.reshape(-1, ROW_CHUNK, 4).transpose(0, 2, 1).reshape(-1)

    tab, t_0, t_1, t = call(
        functools.partial(load_kernel, devices),
        [shape((TAB, LANES), jnp.int32)] + [full(width, block, block)] * 2 + [full(*t_blocks.shape)],
        [pltpu.with_memory_space_constraint(x, pltpu.HBM) for x in (cols, t_agg, t_blocks)],
        [
            pltpu.SMEM((3 * 4 * ROW_CHUNK,), jnp.int32),
            pltpu.SMEM(t_agg.shape, jnp.int32),
            pltpu.SMEM((8 * rows,), jnp.int32),
            pltpu.SemaphoreType.DMA((5,)),
        ],
        micros=3,
        in_hbm=(0, 1, 2),
    )
    t_1 = exchanged(t_1, 1)
    t_0 = exchanged(t_0, 0)
    (near_1,) = call(near_sent_kernel, [tile], [tab, a, t, dinv], micros=2)
    got_near_1 = exchanged(near_1, 1)
    near_0, own, part_own, a01_high, a01_low = call(
        near_rest_kernel,
        [tile] + [full(rows, block, half)] * 2 + pair(rows, block, half),
        [tab, a, t, dinv, near_1],
        two(rows, block, half),
        micros=2,
    )
    near_0, near_1 = exchanged(near_0, 0), got_near_1
    sent = full(width, 2, block, block)
    far_0, far_1, far, a23_high, a23_low = call(
        far_kernel,
        [sent, sent, full(rows, 2, block, block)] + pair(rows, block, half),
        [tab, a, dinv, t_0, t_1, own],
        two(2, width, block, block),
        micros=2,
    )
    far_1 = exchanged(far_1, 1)
    far_0 = exchanged(far_0, 0)
    part, out_high, out_low = call(
        pre_kernel,
        [full(rows, block, 2 * half)] + pair(half, deep),
        [tab, a01_high, a01_low, far],
        two(2, rows, block, half),
        micros=3,
    )
    ap1_high, ap1_low, first_1 = call(
        first_kernel,
        pair(deep, 2 * half) + [full(half, 2 * half)],
        [tab, a23_high, a23_low, part, out_high, out_low, near_0, near_1],
        two(2, width, block, half),
        micros=3,
    )
    first_1 = exchanged(first_1, 1)
    ap2_high, ap2_low, second_1 = call(
        second_kernel,
        pair(deep, 3 * half) + [full(half, 3 * half)],
        [tab, a23_high, a23_low, part_own, out_high, out_low, far_0, far_1, ap1_high],
        two(2, width, block, half),
        micros=3,
    )
    second_1 = exchanged(second_1, 1)
    (both_0,) = call(
        other_kernel,
        [full(half, 5 * half)],
        [tab, far, ap1_high, ap1_low, ap2_high, ap2_low],
        two(half, deep),
        micros=2,
    )
    both_0 = exchanged(both_0, 0)
    (total,) = call(
        own_kernel, [full(half, 5 * half)], [own, ap1_high, ap1_low, ap2_high, ap2_low], two(half, deep), micros=2
    )
    result = full(2, 14, block, block)
    partly, waiting = call(
        early_kernel,
        [result, full(2, 3, block, half)],
        [coarse_inv, total, both_0, first_1],
        [((8, 2, block, block), F32), pltpu.SemaphoreType.DMA((8,))],
        micros=2,
        out_hbm=(0,),
    )
    (out,) = call(
        late_kernel,
        [result],
        [coarse_inv, waiting, second_1, partly],
        [((6, 2, block, block), F32), pltpu.SemaphoreType.DMA((6,))],
        micros=1,
        in_hbm=(3,),
        out_hbm=(0,),
        aliases={3: 0},
    )
    return out


def solution(mesh):
    placed = (
        P(AXES, None, None, None),
        P(),
        P(AXES, None, None),
        P(),
        P(AXES, None, None),
        P(AXES, None, None),
    )
    return jax.shard_map(
        shards,
        mesh=mesh,
        in_specs=placed,
        out_specs=P(AXES, None, None, None),
        check_vma=False,
    )
```

```python
import functools

import jax
import jax.numpy as jnp
from jax import lax
from jax.experimental import pallas as pl
from jax.experimental.pallas import tpu as pltpu
from jax.sharding import PartitionSpec as P


OMEGA = 0.6
AXES = ("gx", "gy")
F32 = jnp.float32
BF16 = jnp.bfloat16
ROW, NEAR, POS2, POS3, LIST_0, OWN_LAB, SIDE_LAB, TAB = 0, 8, 16, 24, 32, 40, 72, 88
LANES = 128
BELOW, ABOVE = 0, 1
ROW_CHUNK = 128


def exchanged(value, first):
    count = lax.axis_size(AXES)
    pairs = []
    for low in range(first, count + first, 2):
        high = (low + 1) % count
        pairs += [(low, high), (high, low)]
    return lax.ppermute(value, AXES, pairs)


def pair_side():
    return 1 - lax.rem(lax.axis_index("gy"), 2)


def split(x):
    high = x.astype(BF16)
    return high, (x - high.astype(F32)).astype(BF16)


def dot(a, b):
    return jnp.dot(a, b, preferred_element_type=F32)


def dot3(a_high, a_low, b_high, b_low):
    return dot(a_high, b_high) + dot(a_low, b_high) + dot(a_high, b_low)


def dot3k(a_high, a_low, b_high, b_low):
    both = jnp.concatenate([a_high, a_low], axis=1)
    return dot(both, jnp.concatenate([b_high, b_high], axis=0)) + dot(a_high, b_low)


def note(tab, i, value):
    tab[pl.ds(i, 1), :] = jnp.full((1, tab.shape[1]), value, jnp.int32)


def entry(tab, i):
    return tab[pl.ds(i, 1), :][0, 0]


def load_kernel(devices, cols_hbm, agg_hbm, t_hbm, tab, t_0, t_1, t, cols, agg, rank, sem):
    rows, width = t.shape[0], t.shape[0] // 2
    device = lax.axis_index("gx") * lax.axis_size("gy") + lax.axis_index("gy")
    previous = lax.rem(device + devices - 1, devices)
    following = lax.rem(device + 1, devices)
    slabs = previous, following, device
    side = pair_side()
    shift = ROW_CHUNK.bit_length() - 1
    chunk = 4 * ROW_CHUNK
    copies = [
        pltpu.make_async_copy(
            cols_hbm.at[pl.ds(pl.multiple_of(((slab * rows) >> shift) * chunk, chunk), chunk)],
            cols.at[pl.ds(i * chunk, chunk)],
            sem.at[i],
        )
        for i, slab in enumerate(slabs)
    ]
    copies += [pltpu.make_async_copy(t_hbm, t, sem.at[3]), pltpu.make_async_copy(agg_hbm, agg, sem.at[4])]
    for copy in copies:
        copy.start()

    def col(i, r, k):
        return cols[i * chunk + k * ROW_CHUNK + ((slabs[i] * rows) & (ROW_CHUNK - 1)) + r]

    def rank_rows(i, k, where):
        mask = jnp.int32(0)
        for r in range(rows):
            mask = mask | (jnp.int32(1) << (col(i, r, k) & (rows - 1)))
        named, other = jnp.int32(0), jnp.int32(width)
        for r in range(rows):
            hit = (mask >> r) & 1
            place = jnp.where(hit == 1, named, other)
            rank[where * rows + r] = place
            rank[(where + 1) * rows + place] = r
            named = named + hit
            other = other + 1 - hit

    def ranked(where, r):
        return rank[where * rows + r]

    copies[0].wait()
    copies[1].wait()
    rank_rows(0, 3, 0)
    rank_rows(1, 2, 2)
    sent_1, sent_0 = jnp.where(side == ABOVE, 0, 2), jnp.where(side == ABOVE, 2, 0)
    copies[3].wait()
    for j in range(width):
        t_1[j] = t[ranked(sent_1 + 1, j)]
        t_0[j] = t[ranked(sent_0 + 1, j)]
    copies[2].wait()
    copies[4].wait()
    rank_rows(2, 2, 4)
    rank_rows(2, 3, 6)
    for j in range(width):
        note(tab, LIST_0 + j, ranked(sent_1, ranked(sent_0 + 1, j)))
        for which in (BELOW, ABOVE):
            for k in range(2):
                note(tab, SIDE_LAB + 8 * which + 2 * j + k, agg[col(which, ranked(5 + 2 * which, j), 2 + k)])
    for u in range(rows):
        row = ranked(sent_1 + 1, u)
        note(tab, ROW + u, row)
        note(tab, NEAR + u, ranked(sent_1, col(2, row, 1) & (rows - 1)))
        note(tab, POS2 + u, ranked(4, col(2, row, 2) & (rows - 1)))
        note(tab, POS3 + u, ranked(6, col(2, row, 3) & (rows - 1)))
        for k in range(4):
            note(tab, OWN_LAB + 4 * u + k, agg[col(2, row, k)])


def put(value, label, column):
    return jnp.where(label == column, value, jnp.zeros_like(value))


def two_columns(value, label):
    return jnp.concatenate([put(value, label, 0), put(value, label, 1)], axis=1)


def near_tile(tab, a, t, dinv, u):
    block = t.shape[1]
    row = entry(tab, ROW + u)
    near = entry(tab, ROW + entry(tab, NEAR + u))
    prod = jnp.concatenate(
        [dot3k(*split(a[row, 0]), *split(t[row])), dot3k(*split(a[row, 1]), *split(t[near]))], axis=1
    )
    smoothed = dot3k(*split(dinv[row]), *split(prod))
    p0 = t[row] - OMEGA * smoothed[:, :block]
    p1 = -OMEGA * smoothed[:, block:]
    return two_columns(p0, entry(tab, OWN_LAB + 4 * u)) + two_columns(p1, entry(tab, OWN_LAB + 4 * u + 1))


def near_sent_kernel(tab, a, t, dinv, near_1):
    for u in range(near_1.shape[0]):
        near_1[u] = near_tile(tab, a, t, dinv, u)


def wide(ref, *places):
    return jnp.concatenate([ref[place] for place in places], axis=0)


def near_rest_kernel(tab, a, t, dinv, near_1, near_0, own, part, a_high, a_low, own_high, own_low):
    width = near_1.shape[0]
    for u in range(width):
        own[u] = near_1[u]
        own[width + u] = near_tile(tab, a, t, dinv, width + u)
    for j in range(width):
        near_0[j] = own[entry(tab, LIST_0 + j)]
    for u in range(2 * width):
        own_high[u], own_low[u] = split(own[u])
    for u in range(2 * width):
        row, near = entry(tab, ROW + u), entry(tab, NEAR + u)
        a_high[u], a_low[u] = split(jnp.concatenate([a[row, 0], a[row, 1]], axis=1))
        part[u] = dot3(a_high[u], a_low[u], wide(own_high, u, near), wide(own_low, u, near))


def far_blocks(tab, a, dinv, t_high, t_low, u):
    row = entry(tab, ROW + u)
    prod = jnp.concatenate(
        [
            dot3k(*split(a[row, 2 + which]), t_high[which, pos], t_low[which, pos])
            for which, pos in ((BELOW, entry(tab, POS2 + u)), (ABOVE, entry(tab, POS3 + u)))
        ],
        axis=1,
    )
    return -OMEGA * dot3k(*split(dinv[row]), *split(prod))


def split_both(side, value_0, value_1, high, low):
    for j in range(value_0.shape[0]):
        high[side, j], low[side, j] = split(value_0[j])
        high[1 - side, j], low[1 - side, j] = split(value_1[j])


def far_sent_kernel(tab, a, dinv, t_0, t_1, after, far_1, t_high, t_low):
    block = dinv.shape[1]
    split_both(pair_side(), t_0, t_1, t_high, t_low)
    for u in range(far_1.shape[0]):
        both = far_blocks(tab, a, dinv, t_high, t_low, u)
        far_1[u, BELOW] = both[:, :block]
        far_1[u, ABOVE] = both[:, block:]


def store_turned(trans, label, place, value):
    block = value.shape[0]
    trans[pl.ds(pl.multiple_of(label * block, block), block), place] = value.T
    trans[pl.ds(pl.multiple_of((1 - label) * block, block), block), place] = jnp.zeros_like(value)


def turn(tab, far, side, trans_high, trans_low):
    for u in range(far.shape[0]):
        block = far.shape[2]
        label = entry(tab, OWN_LAB + 4 * u + 2 + side)
        high, low = split(far[u, side])
        place = slice(u * block, (u + 1) * block)
        store_turned(trans_high, label, place, high)
        store_turned(trans_low, label, place, low)


def coarse_group(trans_high, trans_low, ap_high, ap_low):
    return dot3(trans_high[...], trans_low[...], ap_high[...], ap_low[...])


def mid_kernel(
    tab, a, dinv, t_0, t_1, far_1, a01_high, a01_low, near_0,
    far_0, far, a_high, a_low, trans_high, trans_low, part, ap_high, ap_low, group,
    t_high, t_low, far_high, far_low, p_high, p_low,
):
    rows, block = far.shape[0], far.shape[2]
    width = rows // 2
    side = pair_side()
    split_both(side, t_0, t_1, t_high, t_low)
    for u in range(width):
        far[u] = far_1[u]
        both = far_blocks(tab, a, dinv, t_high, t_low, width + u)
        far[width + u, BELOW] = both[:, :block]
        far[width + u, ABOVE] = both[:, block:]
    for j in range(width):
        far_0[j] = far[entry(tab, LIST_0 + j)]
        p_high[j], p_low[j] = split(near_0[j])
    for u in range(rows):
        row = entry(tab, ROW + u)
        for which in (BELOW, ABOVE):
            a_high[which, u], a_low[which, u] = split(a[row, 2 + which])
            label = entry(tab, OWN_LAB + 4 * u + 2 + which)
            high, low = split(far[u, which])
            far_high[which, u] = two_columns(high, label)
            far_low[which, u] = two_columns(low, label)
    turn(tab, far, 1 - side, trans_high, trans_low)
    for u in range(rows):
        near, pos = entry(tab, NEAR + u), entry(tab, POS2 + 8 * side + u)
        place = slice(u * block, (u + 1) * block)
        mine = [
            dot3(a01_high[u], a01_low[u], wide(far_high.at[which], u, near), wide(far_low.at[which], u, near))
            for which in (side, 1 - side)
        ]
        part[u] = mine[1]
        total = mine[0] + dot3k(a_high[side, u], a_low[side, u], p_high[pos], p_low[pos])
        ap_high[place], ap_low[place] = split(total)
    group[...] = coarse_group(trans_high, trans_low, ap_high, ap_low)


def first_kernel(
    tab, a_high, a_low, part, trans_high, trans_low, near_1, group,
    ap_high, ap_low, out_1,
    p_high, p_low,
):
    rows, block = part.shape[0], part.shape[1]
    half = 2 * block
    side = 1 - pair_side()
    out_1[:, :half] = group[...]
    for j in range(rows // 2):
        p_high[j], p_low[j] = split(near_1[j])
    for u in range(rows):
        pos = entry(tab, POS2 + 8 * side + u)
        place = slice(u * block, (u + 1) * block)
        total = part[u] + dot3k(a_high[side, u], a_low[side, u], p_high[pos], p_low[pos])
        ap_high[place], ap_low[place] = split(total)
    out_1[:, half:] = coarse_group(trans_high, trans_low, ap_high, ap_low)


def take_far(side, far_in, p_high, p_low):
    block = far_in.shape[2]
    for j in range(far_in.shape[0]):
        p_high[j, :, :block], p_low[j, :, :block] = split(far_in[j, 1 - side])
        p_high[j, :, block:], p_low[j, :, block:] = split(far_in[j, side])


def far_columns(tab, side, u, a_high, a_low, p_high, p_low):
    block = a_high.shape[3]
    pos = entry(tab, POS2 + 8 * side + u)
    value = dot3k(a_high[side, u], a_low[side, u], p_high[pos], p_low[pos])
    labels = SIDE_LAB + 8 * side + 2 * pos
    here = two_columns(value[:, :block], entry(tab, labels + 1 - side))
    high, low = split(value[:, block:])
    label = entry(tab, labels + side)
    return here, two_columns(high, label), two_columns(low, label)


def second_pre_kernel(
    tab, a_high, a_low, part, trans_high, trans_low, far_0, after,
    own_part, ap_high, ap_low, group,
    p_high, p_low,
):
    rows, block = part.shape[0], part.shape[1]
    side = pair_side()
    take_far(side, far_0, p_high, p_low)
    for u in range(rows):
        place = slice(u * block, (u + 1) * block)
        here, ap_high[place], ap_low[place] = far_columns(tab, side, u, a_high, a_low, p_high, p_low)
        own_part[u] = part[u] + here
    group[...] = coarse_group(trans_high, trans_low, ap_high, ap_low)


def second_kernel(
    tab, a_high, a_low, own_part, trans_high, trans_low, far_1, group,
    own_high, own_low, ap_high, ap_low, out_1,
    p_high, p_low,
):
    rows, block = own_part.shape[0], own_part.shape[1]
    half = 2 * block
    side = 1 - pair_side()
    out_1[:, :half] = group[...]
    take_far(side, far_1, p_high, p_low)
    for u in range(rows):
        place = slice(u * block, (u + 1) * block)
        here, ap_high[place], ap_low[place] = far_columns(tab, side, u, a_high, a_low, p_high, p_low)
        own_high[place], own_low[place] = split(own_part[u] + here)
    out_1[:, half : 2 * half] = coarse_group(trans_high, trans_low, own_high, own_low)
    out_1[:, 2 * half :] = coarse_group(trans_high, trans_low, ap_high, ap_low)


def every_group(trans_high, trans_low, aps, out):
    half = trans_high.shape[0]
    for i in range(len(aps) // 2):
        out[:, i * half : (i + 1) * half] = coarse_group(trans_high, trans_low, aps[2 * i], aps[2 * i + 1])


def other_kernel(tab, far, *refs):
    aps, (out_0, trans_high, trans_low) = refs[:10], refs[10:]
    turn(tab, far, pair_side(), trans_high, trans_low)
    every_group(trans_high, trans_low, aps, out_0)


def own_kernel(own, *refs):
    aps, (out, trans_high, trans_low) = refs[:10], refs[10:]
    rows, block = own.shape[0], own.shape[1]
    for u in range(rows):
        place = slice(u * block, (u + 1) * block)
        high, low = split(own[u])
        trans_high[:, place] = high.T
        trans_low[:, place] = low.T
    every_group(trans_high, trans_low, aps, out)


def write_slots(inv, total, result, agg, d, out, sem):
    block = total.shape[0]
    value = dot3k(*inv, *split(total))
    result[0] = value[:, :block]
    result[1] = value[:, block:]
    copy = pltpu.make_async_copy(result, out.at[agg, pl.ds(2 * (d + 3), 2)], sem)
    copy.start()
    return copy


OWN_AT, SAME_AT, OTHER_AT = (1, -1, 2, 0, -2), (0, 2, -1, 1, 3), (-2, 0, -3, -1, 1)


def both_ways(run):
    side = pair_side()
    pl.when(side == ABOVE)(lambda: run(1))
    pl.when(side == BELOW)(lambda: run(-1))


def early_kernel(inverse, own, both_0, first_1, out, waiting, results, sems):
    block = inverse.shape[1]
    half = 2 * block

    def run(way):
        copies = []
        for agg in range(2):
            inv = split(inverse[agg])
            line = slice(agg * block, (agg + 1) * block)
            for d in range(-3, 4):
                places = [(ref, at.index(d)) for ref, at in ((own, OWN_AT), (both_0, SAME_AT), (first_1, OTHER_AT[:2])) if d in at]
                parts = [ref[line, i * half : (i + 1) * half] for ref, i in places]
                total = sum(parts[1:], parts[0]) if parts else jnp.zeros((block, half), F32)
                if d in OTHER_AT[2:]:
                    waiting[agg, OTHER_AT.index(d) - 2] = total
                else:
                    n = len(copies)
                    copies.append(write_slots(inv, total, results.at[n], agg, way * d, out, sems.at[n]))
        for copy in copies:
            copy.wait()

    both_ways(run)


def late_kernel(inverse, waiting, second_1, partly, out, results, sems):
    block = inverse.shape[1]
    half = 2 * block

    def run(way):
        copies = []
        for agg in range(2):
            inv = split(inverse[agg])
            line = slice(agg * block, (agg + 1) * block)
            for i in range(3):
                total = waiting[agg, i] + second_1[line, i * half : (i + 1) * half]
                n = len(copies)
                copies.append(write_slots(inv, total, results.at[n], agg, way * OTHER_AT[2 + i], out, sems.at[n]))
        for copy in copies:
            copy.wait()

    both_ways(run)


VMEM = pl.BlockSpec(memory_space=pltpu.VMEM)
HBM = pl.BlockSpec(memory_space=pltpu.HBM)


def call(body, outs, ins, scratch=(), micros=1.0, in_hbm=(), out_hbm=(), aliases={}):
    def specs(values, in_place):
        return [HBM if i in in_place else VMEM for i, x in enumerate(values)]

    return pl.pallas_call(
        body,
        out_shape=outs,
        in_specs=specs(ins, in_hbm),
        out_specs=specs(outs, out_hbm),
        scratch_shapes=[pltpu.VMEM(*x) if isinstance(x, tuple) else x for x in scratch],
        input_output_aliases=aliases,
        compiler_params=pltpu.CompilerParams(vmem_limit_bytes=24 * 2**20),
        cost_estimate=pl.CostEstimate(flops=int(micros * 1e9), bytes_accessed=2**20, transcendentals=0),
    )(*ins)


def shards(a, a_cols, t_blocks, t_agg, dinv, coarse_inv):
    devices = lax.axis_size(AXES)
    rows, block = t_blocks.shape[:2]
    width, half, deep = rows // 2, 2 * block, rows * block
    shape = jax.ShapeDtypeStruct
    full = lambda *dims: shape(dims, F32)
    pair = lambda *dims: [shape(dims, BF16), shape(dims, BF16)]
    two = lambda *dims: [(dims, BF16)] * 2
    tile = full(width, block, half)
    cols = a_cols.reshape(-1, ROW_CHUNK, 4).transpose(0, 2, 1).reshape(-1)

    tab, t_0, t_1, t = call(
        functools.partial(load_kernel, devices),
        [shape((TAB, LANES), jnp.int32)] + [full(width, block, block)] * 2 + [full(*t_blocks.shape)],
        [pltpu.with_memory_space_constraint(x, pltpu.HBM) for x in (cols, t_agg, t_blocks)],
        [
            pltpu.SMEM((3 * 4 * ROW_CHUNK,), jnp.int32),
            pltpu.SMEM(t_agg.shape, jnp.int32),
            pltpu.SMEM((8 * rows,), jnp.int32),
            pltpu.SemaphoreType.DMA((5,)),
        ],
        micros=3,
        in_hbm=(0, 1, 2),
    )
    t_1 = exchanged(t_1, 1)
    t_0 = exchanged(t_0, 0)
    (near_1,) = call(near_sent_kernel, [tile], [tab, a, t, dinv], micros=2)
    got_near_1 = exchanged(near_1, 1)
    near_0, own, part_own, a01_high, a01_low = call(
        near_rest_kernel,
        [tile] + [full(rows, block, half)] * 2 + pair(rows, block, half),
        [tab, a, t, dinv, near_1],
        two(rows, block, half),
        micros=2,
    )
    near_0, near_1 = exchanged(near_0, 0), got_near_1
    sent = full(width, 2, block, block)
    (far_1,) = call(far_sent_kernel, [sent], [tab, a, dinv, t_0, t_1, own], two(2, width, block, block), micros=2)
    got_far_1 = exchanged(far_1, 1)
    far_0, far, a23_high, a23_low, out_high, out_low, part, ap_e1_high, ap_e1_low, group = call(
        mid_kernel,
        [sent, full(rows, 2, block, block)]
        + pair(2, rows, block, block)
        + pair(half, deep)
        + [full(rows, block, half)]
        + pair(deep, half)
        + [full(half, half)],
        [tab, a, dinv, t_0, t_1, far_1, a01_high, a01_low, near_0],
        two(2, width, block, block) + two(2, rows, block, half) + two(width, block, half),
        micros=3,
    )
    far_0, far_1 = exchanged(far_0, 0), got_far_1
    ap_o1_high, ap_o1_low, first_1 = call(
        first_kernel,
        pair(deep, half) + [full(half, 2 * half)],
        [tab, a23_high, a23_low, part, out_high, out_low, near_1, group],
        two(width, block, half),
        micros=2,
    )
    first_1 = exchanged(first_1, 1)
    part_own, ap_e2_high, ap_e2_low, group = call(
        second_pre_kernel,
        [full(rows, block, half)] + pair(deep, half) + [full(half, half)],
        [tab, a23_high, a23_low, part_own, out_high, out_low, far_0, ap_o1_high],
        two(width, block, half),
        micros=2,
    )
    ap_own_high, ap_own_low, ap_o2_high, ap_o2_low, second_1 = call(
        second_kernel,
        pair(deep, half) * 2 + [full(half, 3 * half)],
        [tab, a23_high, a23_low, part_own, out_high, out_low, far_1, group],
        two(width, block, half),
        micros=2,
    )
    second_1 = exchanged(second_1, 1)
    aps = [
        ap_e1_high, ap_e1_low, ap_o1_high, ap_o1_low, ap_e2_high, ap_e2_low,
        ap_own_high, ap_own_low, ap_o2_high, ap_o2_low,
    ]
    (both_0,) = call(other_kernel, [full(half, 5 * half)], [tab, far] + aps, two(half, deep), micros=2)
    both_0 = exchanged(both_0, 0)
    (total,) = call(own_kernel, [full(half, 5 * half)], [own] + aps, two(half, deep), micros=2)
    result = full(2, 14, block, block)
    partly, waiting = call(
        early_kernel,
        [result, full(2, 3, block, half)],
        [coarse_inv, total, both_0, first_1],
        [((8, 2, block, block), F32), pltpu.SemaphoreType.DMA((8,))],
        micros=2,
        out_hbm=(0,),
    )
    (out,) = call(
        late_kernel,
        [result],
        [coarse_inv, waiting, second_1, partly],
        [((6, 2, block, block), F32), pltpu.SemaphoreType.DMA((6,))],
        micros=1,
        in_hbm=(3,),
        out_hbm=(0,),
        aliases={3: 0},
    )
    return out


def solution(mesh):
    placed = (
        P(AXES, None, None, None),
        P(),
        P(AXES, None, None),
        P(),
        P(AXES, None, None),
        P(AXES, None, None),
    )
    return jax.shard_map(
        shards,
        mesh=mesh,
        in_specs=placed,
        out_specs=P(AXES, None, None, None),
        check_vma=False,
    )
```

```python
import functools

import jax
import jax.numpy as jnp
from jax import lax
from jax.experimental import pallas as pl
from jax.experimental.pallas import tpu as pltpu
from jax.sharding import PartitionSpec as P


OMEGA = 0.6
AXES = ("gx", "gy")
F32 = jnp.float32
BF16 = jnp.bfloat16
ROW, NEAR, POS2, POS3, LIST_0, OWN_LAB, SIDE_LAB, TAB = 0, 8, 16, 24, 32, 40, 72, 88
LANES = 128
BELOW, ABOVE = 0, 1
ROW_CHUNK = 128


def exchanged(value, first):
    count = lax.axis_size(AXES)
    pairs = []
    for low in range(first, count + first, 2):
        high = (low + 1) % count
        pairs += [(low, high), (high, low)]
    return lax.ppermute(value, AXES, pairs)


def pair_side():
    return 1 - lax.rem(lax.axis_index("gy"), 2)


def split(x):
    high = x.astype(BF16)
    return high, (x - high.astype(F32)).astype(BF16)


def dot(a, b):
    return jnp.dot(a, b, preferred_element_type=F32)


def dot3(a_high, a_low, b_high, b_low):
    return dot(a_high, b_high) + dot(a_low, b_high) + dot(a_high, b_low)


def dot3k(a_high, a_low, b_high, b_low):
    both = jnp.concatenate([a_high, a_low], axis=1)
    return dot(both, jnp.concatenate([b_high, b_high], axis=0)) + dot(a_high, b_low)


def note(tab, i, value):
    tab[pl.ds(i, 1), :] = jnp.full((1, tab.shape[1]), value, jnp.int32)


def entry(tab, i):
    return tab[pl.ds(i, 1), :][0, 0]


def load_kernel(devices, cols_hbm, agg_hbm, t_hbm, tab, t_0, t_1, t, cols, agg, rank, sem):
    rows, width = t.shape[0], t.shape[0] // 2
    device = lax.axis_index("gx") * lax.axis_size("gy") + lax.axis_index("gy")
    previous = lax.rem(device + devices - 1, devices)
    following = lax.rem(device + 1, devices)
    slabs = previous, following, device
    side = pair_side()
    shift = ROW_CHUNK.bit_length() - 1
    chunk = 4 * ROW_CHUNK
    copies = [
        pltpu.make_async_copy(
            cols_hbm.at[pl.ds(pl.multiple_of(((slab * rows) >> shift) * chunk, chunk), chunk)],
            cols.at[pl.ds(i * chunk, chunk)],
            sem.at[i],
        )
        for i, slab in enumerate(slabs)
    ]
    copies += [pltpu.make_async_copy(t_hbm, t, sem.at[3]), pltpu.make_async_copy(agg_hbm, agg, sem.at[4])]
    for copy in copies:
        copy.start()

    def col(i, r, k):
        return cols[i * chunk + k * ROW_CHUNK + ((slabs[i] * rows) & (ROW_CHUNK - 1)) + r]

    def rank_rows(i, k, where):
        mask = jnp.int32(0)
        for r in range(rows):
            mask = mask | (jnp.int32(1) << (col(i, r, k) & (rows - 1)))
        named, other = jnp.int32(0), jnp.int32(width)
        for r in range(rows):
            hit = (mask >> r) & 1
            place = jnp.where(hit == 1, named, other)
            rank[where * rows + r] = place
            rank[(where + 1) * rows + place] = r
            named = named + hit
            other = other + 1 - hit

    def ranked(where, r):
        return rank[where * rows + r]

    copies[0].wait()
    copies[1].wait()
    rank_rows(0, 3, 0)
    rank_rows(1, 2, 2)
    sent_1, sent_0 = jnp.where(side == ABOVE, 0, 2), jnp.where(side == ABOVE, 2, 0)
    copies[3].wait()
    for j in range(width):
        t_1[j] = t[ranked(sent_1 + 1, j)]
        t_0[j] = t[ranked(sent_0 + 1, j)]
    copies[2].wait()
    copies[4].wait()
    rank_rows(2, 2, 4)
    rank_rows(2, 3, 6)
    for j in range(width):
        note(tab, LIST_0 + j, ranked(sent_1, ranked(sent_0 + 1, j)))
        for which in (BELOW, ABOVE):
            for k in range(2):
                note(tab, SIDE_LAB + 8 * which + 2 * j + k, agg[col(which, ranked(5 + 2 * which, j), 2 + k)])
    for u in range(rows):
        row = ranked(sent_1 + 1, u)
        note(tab, ROW + u, row)
        note(tab, NEAR + u, ranked(sent_1, col(2, row, 1) & (rows - 1)))
        note(tab, POS2 + u, ranked(4, col(2, row, 2) & (rows - 1)))
        note(tab, POS3 + u, ranked(6, col(2, row, 3) & (rows - 1)))
        for k in range(4):
            note(tab, OWN_LAB + 4 * u + k, agg[col(2, row, k)])


def put(value, label, column):
    return jnp.where(label == column, value, jnp.zeros_like(value))


def two_columns(value, label):
    return jnp.concatenate([put(value, label, 0), put(value, label, 1)], axis=1)


def near_tiles(tab, a, t, dinv, order):
    block = t.shape[1]
    rows = [entry(tab, ROW + u) for u in order]
    prods = []
    for u, row in zip(order, rows):
        near = entry(tab, ROW + entry(tab, NEAR + u))
        prods.append(
            jnp.concatenate(
                [dot3k(*split(a[row, 0]), *split(t[row])), dot3k(*split(a[row, 1]), *split(t[near]))], axis=1
            )
        )
    tiles = []
    for u, row, prod in zip(order, rows, prods):
        smoothed = dot3k(*split(dinv[row]), *split(prod))
        p0 = t[row] - OMEGA * smoothed[:, :block]
        p1 = -OMEGA * smoothed[:, block:]
        tiles.append(two_columns(p0, entry(tab, OWN_LAB + 4 * u)) + two_columns(p1, entry(tab, OWN_LAB + 4 * u + 1)))
    return tiles


def near_sent_kernel(tab, a, t, dinv, near_1):
    for u, value in enumerate(near_tiles(tab, a, t, dinv, range(near_1.shape[0]))):
        near_1[u] = value


def wide(ref, *places):
    return jnp.concatenate([ref[place] for place in places], axis=0)


def near_rest_kernel(tab, a, t, dinv, near_1, near_0, own, a_high, a_low, a01_high, a01_low):
    width = near_1.shape[0]
    for u, value in enumerate(near_tiles(tab, a, t, dinv, range(width, 2 * width))):
        own[u] = near_1[u]
        own[width + u] = value
    for j in range(width):
        near_0[j] = own[entry(tab, LIST_0 + j)]
    for u in range(2 * width):
        row = entry(tab, ROW + u)
        a01_high[u], a01_low[u] = split(jnp.concatenate([a[row, 0], a[row, 1]], axis=1))
        for which in (BELOW, ABOVE):
            a_high[which, u], a_low[which, u] = split(a[row, 2 + which])


def far_blocks(tab, a_high, a_low, dinv, t_high, t_low, order):
    prods = [
        jnp.concatenate(
            [
                dot3k(a_high[which, u], a_low[which, u], t_high[which, pos], t_low[which, pos])
                for which, pos in ((BELOW, entry(tab, POS2 + u)), (ABOVE, entry(tab, POS3 + u)))
            ],
            axis=1,
        )
        for u in order
    ]
    return [-OMEGA * dot3k(*split(dinv[entry(tab, ROW + u)]), *split(prod)) for u, prod in zip(order, prods)]


def split_both(side, value_0, value_1, high, low):
    for j in range(value_0.shape[0]):
        high[side, j], low[side, j] = split(value_0[j])
        high[1 - side, j], low[1 - side, j] = split(value_1[j])


def far_sent_kernel(tab, a_high, a_low, dinv, t_0, t_1, far_1, t_high, t_low):
    block = dinv.shape[1]
    split_both(pair_side(), t_0, t_1, t_high, t_low)
    for u, both in enumerate(far_blocks(tab, a_high, a_low, dinv, t_high, t_low, range(far_1.shape[0]))):
        far_1[u, BELOW] = both[:, :block]
        far_1[u, ABOVE] = both[:, block:]


def store_turned(trans, label, place, value):
    block = value.shape[0]
    trans[pl.ds(pl.multiple_of(label * block, block), block), place] = value.T
    trans[pl.ds(pl.multiple_of((1 - label) * block, block), block), place] = jnp.zeros_like(value)


def turn(tab, far, side, trans_high, trans_low):
    for u in range(far.shape[0]):
        block = far.shape[2]
        label = entry(tab, OWN_LAB + 4 * u + 2 + side)
        high, low = split(far[u, side])
        place = slice(u * block, (u + 1) * block)
        store_turned(trans_high, label, place, high)
        store_turned(trans_low, label, place, low)


def coarse_group(trans_high, trans_low, ap_high, ap_low):
    return dot3(trans_high[...], trans_low[...], ap_high[...], ap_low[...])


def mid_kernel(
    tab, a01_high, a01_low, a_high, a_low, dinv, t_high, t_low, far_1, near_0,
    far_0, far, trans_high, trans_low, part, ap_high, ap_low, group,
    far_high, far_low, p_high, p_low,
):
    rows, block = far.shape[0], far.shape[2]
    width = rows // 2
    side = pair_side()
    for u, both in enumerate(far_blocks(tab, a_high, a_low, dinv, t_high, t_low, range(width, rows))):
        far[u] = far_1[u]
        far[width + u, BELOW] = both[:, :block]
        far[width + u, ABOVE] = both[:, block:]
    for j in range(width):
        far_0[j] = far[entry(tab, LIST_0 + j)]
        p_high[j], p_low[j] = split(near_0[j])
    for u in range(rows):
        for which in (BELOW, ABOVE):
            label = entry(tab, OWN_LAB + 4 * u + 2 + which)
            high, low = split(far[u, which])
            far_high[which, u] = two_columns(high, label)
            far_low[which, u] = two_columns(low, label)

    def mine(u, which):
        near = entry(tab, NEAR + u)
        return dot3(a01_high[u], a01_low[u], wide(far_high.at[which], u, near), wide(far_low.at[which], u, near))

    totals = []
    for u in range(rows):
        pos = entry(tab, POS2 + 8 * side + u)
        totals.append(mine(u, side) + dot3k(a_high[side, u], a_low[side, u], p_high[pos], p_low[pos]))
    for u in range(rows):
        place = slice(u * block, (u + 1) * block)
        ap_high[place], ap_low[place] = split(totals[u])
    turn(tab, far, 1 - side, trans_high, trans_low)
    for u in range(rows):
        part[u] = mine(u, 1 - side)
    group[...] = coarse_group(trans_high, trans_low, ap_high, ap_low)


def first_kernel(
    tab, a_high, a_low, part, trans_high, trans_low, near_1, group,
    ap_high, ap_low, out_1,
    p_high, p_low,
):
    rows, block = part.shape[0], part.shape[1]
    half = 2 * block
    side = 1 - pair_side()
    out_1[:, :half] = group[...]
    for j in range(rows // 2):
        p_high[j], p_low[j] = split(near_1[j])
    totals = []
    for u in range(rows):
        pos = entry(tab, POS2 + 8 * side + u)
        totals.append(part[u] + dot3k(a_high[side, u], a_low[side, u], p_high[pos], p_low[pos]))
    for u in range(rows):
        place = slice(u * block, (u + 1) * block)
        ap_high[place], ap_low[place] = split(totals[u])
    out_1[:, half:] = coarse_group(trans_high, trans_low, ap_high, ap_low)


def take_far(side, far_in, p_high, p_low):
    block = far_in.shape[2]
    for j in range(far_in.shape[0]):
        p_high[j, :, :block], p_low[j, :, :block] = split(far_in[j, 1 - side])
        p_high[j, :, block:], p_low[j, :, block:] = split(far_in[j, side])


def far_columns(tab, side, a_high, a_low, p_high, p_low, ap_high, ap_low):
    rows, block = a_high.shape[1], a_high.shape[3]
    values, here = [], []
    for u in range(rows):
        pos = entry(tab, POS2 + 8 * side + u)
        values.append(dot3k(a_high[side, u], a_low[side, u], p_high[pos], p_low[pos]))
    for u in range(rows):
        labels = SIDE_LAB + 8 * side + 2 * entry(tab, POS2 + 8 * side + u)
        here.append(two_columns(values[u][:, :block], entry(tab, labels + 1 - side)))
        high, low = split(values[u][:, block:])
        label = entry(tab, labels + side)
        place = slice(u * block, (u + 1) * block)
        ap_high[place] = two_columns(high, label)
        ap_low[place] = two_columns(low, label)
    return here


def second_pre_kernel(
    tab, a01_high, a01_low, a_high, a_low, own, trans_high, trans_low, far_0, after,
    own_part, ap_high, ap_low, group,
    p_high, p_low, own_high, own_low,
):
    rows = own.shape[0]
    side = pair_side()
    take_far(side, far_0, p_high, p_low)
    for u in range(rows):
        own_high[u], own_low[u] = split(own[u])
    here = far_columns(tab, side, a_high, a_low, p_high, p_low, ap_high, ap_low)
    for u in range(rows):
        near = entry(tab, NEAR + u)
        own_part[u] = here[u] + dot3(a01_high[u], a01_low[u], wide(own_high, u, near), wide(own_low, u, near))
    group[...] = coarse_group(trans_high, trans_low, ap_high, ap_low)


def second_kernel(
    tab, a_high, a_low, own_part, trans_high, trans_low, far_1, group,
    own_high, own_low, ap_high, ap_low, out_1,
    p_high, p_low,
):
    rows, block = own_part.shape[0], own_part.shape[1]
    half = 2 * block
    side = 1 - pair_side()
    out_1[:, :half] = group[...]
    take_far(side, far_1, p_high, p_low)
    here = far_columns(tab, side, a_high, a_low, p_high, p_low, ap_high, ap_low)
    for u in range(rows):
        place = slice(u * block, (u + 1) * block)
        own_high[place], own_low[place] = split(own_part[u] + here[u])
    out_1[:, half : 2 * half] = coarse_group(trans_high, trans_low, own_high, own_low)
    out_1[:, 2 * half :] = coarse_group(trans_high, trans_low, ap_high, ap_low)


def every_group(trans_high, trans_low, aps, out):
    half = trans_high.shape[0]
    for i in range(len(aps) // 2):
        out[:, i * half : (i + 1) * half] = coarse_group(trans_high, trans_low, aps[2 * i], aps[2 * i + 1])


def other_kernel(tab, far, *refs):
    aps, (out_0, trans_high, trans_low) = refs[:10], refs[10:]
    turn(tab, far, pair_side(), trans_high, trans_low)
    every_group(trans_high, trans_low, aps, out_0)


def own_kernel(own, *refs):
    aps, (out, trans_high, trans_low) = refs[:10], refs[10:]
    rows, block = own.shape[0], own.shape[1]
    for u in range(rows):
        place = slice(u * block, (u + 1) * block)
        high, low = split(own[u])
        trans_high[:, place] = high.T
        trans_low[:, place] = low.T
    every_group(trans_high, trans_low, aps, out)


def write_slots(inverse, totals, results, out, sems):
    block = inverse.shape[1]
    inv = [split(inverse[agg]) for agg in range(2)]
    values = [dot3k(*inv[agg], *split(total)) for agg, _, total in totals]
    copies = []
    for n, ((agg, d, _), value) in enumerate(zip(totals, values)):
        results[n, 0] = value[:, :block]
        results[n, 1] = value[:, block:]
        copies.append(pltpu.make_async_copy(results.at[n], out.at[agg, pl.ds(2 * (d + 3), 2)], sems.at[n]))
        copies[-1].start()
    for copy in copies:
        copy.wait()


OWN_AT, SAME_AT, OTHER_AT = (1, -1, 2, 0, -2), (0, 2, -1, 1, 3), (-2, 0, -3, -1, 1)


def both_ways(run):
    side = pair_side()
    pl.when(side == ABOVE)(lambda: run(1))
    pl.when(side == BELOW)(lambda: run(-1))


def early_kernel(inverse, own, both_0, first_1, out, waiting, results, sems):
    block = inverse.shape[1]
    half = 2 * block

    def run(way):
        done = []
        for agg in range(2):
            line = slice(agg * block, (agg + 1) * block)
            for d in range(-3, 4):
                places = [(ref, at.index(d)) for ref, at in ((own, OWN_AT), (both_0, SAME_AT), (first_1, OTHER_AT[:2])) if d in at]
                parts = [ref[line, i * half : (i + 1) * half] for ref, i in places]
                total = sum(parts[1:], parts[0]) if parts else jnp.zeros((block, half), F32)
                if d in OTHER_AT[2:]:
                    waiting[agg, OTHER_AT.index(d) - 2] = total
                else:
                    done.append((agg, way * d, total))
        write_slots(inverse, done, results, out, sems)

    both_ways(run)


def late_kernel(inverse, waiting, second_1, partly, out, results, sems):
    block = inverse.shape[1]
    half = 2 * block

    def run(way):
        done = []
        for agg in range(2):
            line = slice(agg * block, (agg + 1) * block)
            for i in range(3):
                total = waiting[agg, i] + second_1[line, i * half : (i + 1) * half]
                done.append((agg, way * OTHER_AT[2 + i], total))
        write_slots(inverse, done, results, out, sems)

    both_ways(run)


VMEM = pl.BlockSpec(memory_space=pltpu.VMEM)
HBM = pl.BlockSpec(memory_space=pltpu.HBM)


def call(body, outs, ins, scratch=(), micros=1.0, in_hbm=(), out_hbm=(), aliases={}):
    def specs(values, in_place):
        return [HBM if i in in_place else VMEM for i, x in enumerate(values)]

    return pl.pallas_call(
        body,
        out_shape=outs,
        in_specs=specs(ins, in_hbm),
        out_specs=specs(outs, out_hbm),
        scratch_shapes=[pltpu.VMEM(*x) if isinstance(x, tuple) else x for x in scratch],
        input_output_aliases=aliases,
        compiler_params=pltpu.CompilerParams(vmem_limit_bytes=24 * 2**20),
        cost_estimate=pl.CostEstimate(flops=int(micros * 1e9), bytes_accessed=2**20, transcendentals=0),
    )(*ins)


def shards(a, a_cols, t_blocks, t_agg, dinv, coarse_inv):
    devices = lax.axis_size(AXES)
    rows, block = t_blocks.shape[:2]
    width, half, deep = rows // 2, 2 * block, rows * block
    shape = jax.ShapeDtypeStruct
    full = lambda *dims: shape(dims, F32)
    pair = lambda *dims: [shape(dims, BF16), shape(dims, BF16)]
    two = lambda *dims: [(dims, BF16)] * 2
    tile = full(width, block, half)
    cols = a_cols.reshape(-1, ROW_CHUNK, 4).transpose(0, 2, 1).reshape(-1)

    tab, t_0, t_1, t = call(
        functools.partial(load_kernel, devices),
        [shape((TAB, LANES), jnp.int32)] + [full(width, block, block)] * 2 + [full(*t_blocks.shape)],
        [pltpu.with_memory_space_constraint(x, pltpu.HBM) for x in (cols, t_agg, t_blocks)],
        [
            pltpu.SMEM((3 * 4 * ROW_CHUNK,), jnp.int32),
            pltpu.SMEM(t_agg.shape, jnp.int32),
            pltpu.SMEM((8 * rows,), jnp.int32),
            pltpu.SemaphoreType.DMA((5,)),
        ],
        micros=3,
        in_hbm=(0, 1, 2),
    )
    t_1 = exchanged(t_1, 1)
    t_0 = exchanged(t_0, 0)
    (near_1,) = call(near_sent_kernel, [tile], [tab, a, t, dinv], micros=2)
    got_near_1 = exchanged(near_1, 1)
    near_0, own, a23_high, a23_low, a01_high, a01_low = call(
        near_rest_kernel,
        [tile, full(rows, block, half)] + pair(2, rows, block, block) + pair(rows, block, half),
        [tab, a, t, dinv, near_1],
        micros=2,
    )
    near_0, near_1 = exchanged(near_0, 0), got_near_1
    sent = full(width, 2, block, block)
    far_1, t_high, t_low = call(
        far_sent_kernel, [sent] + pair(2, width, block, block), [tab, a23_high, a23_low, dinv, t_0, t_1], micros=2
    )
    got_far_1 = exchanged(far_1, 1)
    far_0, far, out_high, out_low, part, ap_e1_high, ap_e1_low, group = call(
        mid_kernel,
        [sent, full(rows, 2, block, block)]
        + pair(half, deep)
        + [full(rows, block, half)]
        + pair(deep, half)
        + [full(half, half)],
        [tab, a01_high, a01_low, a23_high, a23_low, dinv, t_high, t_low, far_1, near_0],
        two(2, rows, block, half) + two(width, block, half),
        micros=3,
    )
    far_0, far_1 = exchanged(far_0, 0), got_far_1
    ap_o1_high, ap_o1_low, first_1 = call(
        first_kernel,
        pair(deep, half) + [full(half, 2 * half)],
        [tab, a23_high, a23_low, part, out_high, out_low, near_1, group],
        two(width, block, half),
        micros=2,
    )
    first_1 = exchanged(first_1, 1)
    part_own, ap_e2_high, ap_e2_low, group = call(
        second_pre_kernel,
        [full(rows, block, half)] + pair(deep, half) + [full(half, half)],
        [tab, a01_high, a01_low, a23_high, a23_low, own, out_high, out_low, far_0, ap_o1_high],
        two(width, block, half) + two(rows, block, half),
        micros=2,
    )
    ap_own_high, ap_own_low, ap_o2_high, ap_o2_low, second_1 = call(
        second_kernel,
        pair(deep, half) * 2 + [full(half, 3 * half)],
        [tab, a23_high, a23_low, part_own, out_high, out_low, far_1, group],
        two(width, block, half),
        micros=2,
    )
    second_1 = exchanged(second_1, 1)
    aps = [
        ap_e1_high, ap_e1_low, ap_o1_high, ap_o1_low, ap_e2_high, ap_e2_low,
        ap_own_high, ap_own_low, ap_o2_high, ap_o2_low,
    ]
    (both_0,) = call(other_kernel, [full(half, 5 * half)], [tab, far] + aps, two(half, deep), micros=2)
    both_0 = exchanged(both_0, 0)
    (total,) = call(own_kernel, [full(half, 5 * half)], [own] + aps, two(half, deep), micros=2)
    result = full(2, 14, block, block)
    partly, waiting = call(
        early_kernel,
        [result, full(2, 3, block, half)],
        [coarse_inv, total, both_0, first_1],
        [((8, 2, block, block), F32), pltpu.SemaphoreType.DMA((8,))],
        micros=2,
        out_hbm=(0,),
    )
    (out,) = call(
        late_kernel,
        [result],
        [coarse_inv, waiting, second_1, partly],
        [((6, 2, block, block), F32), pltpu.SemaphoreType.DMA((6,))],
        micros=1,
        in_hbm=(3,),
        out_hbm=(0,),
        aliases={3: 0},
    )
    return out


def solution(mesh):
    placed = (
        P(AXES, None, None, None),
        P(),
        P(AXES, None, None),
        P(),
        P(AXES, None, None),
        P(AXES, None, None),
    )
    return jax.shard_map(
        shards,
        mesh=mesh,
        in_specs=placed,
        out_specs=P(AXES, None, None, None),
        check_vma=False,
    )
```

```python
import functools

import jax
import jax.numpy as jnp
from jax import lax
from jax.experimental import pallas as pl
from jax.experimental.pallas import tpu as pltpu
from jax.sharding import PartitionSpec as P


OMEGA = 0.6
AXES = ("gx", "gy")
F32 = jnp.float32
BF16 = jnp.bfloat16
ROW, NEAR, POS2, POS3, LIST_0, OWN_LAB, SIDE_LAB, BACK, TAB = 0, 8, 16, 24, 32, 40, 72, 88, 96
LANES = 128
BELOW, ABOVE = 0, 1
ROW_CHUNK = 128


def exchanged(value, first):
    count = lax.axis_size(AXES)
    pairs = []
    for low in range(first, count + first, 2):
        high = (low + 1) % count
        pairs += [(low, high), (high, low)]
    return lax.ppermute(value, AXES, pairs)


def pair_side():
    return 1 - lax.rem(lax.axis_index("gy"), 2)


def split(x):
    high = x.astype(BF16)
    return high, (x - high.astype(F32)).astype(BF16)


def dot(a, b):
    return jnp.dot(a, b, preferred_element_type=F32)


def dot3(a_high, a_low, b_high, b_low):
    return dot(a_high, b_high) + dot(a_low, b_high) + dot(a_high, b_low)


def dot3k(a_high, a_low, b_high, b_low):
    both = jnp.concatenate([a_high, a_low], axis=1)
    return dot(both, jnp.concatenate([b_high, b_high], axis=0)) + dot(a_high, b_low)


def note(tab, i, value):
    tab[pl.ds(i, 1), :] = jnp.full((1, tab.shape[1]), value, jnp.int32)


def entry(tab, i):
    return tab[pl.ds(i, 1), :][0, 0]


def load_kernel(devices, cols_hbm, agg_hbm, t_hbm, tab, t_0, t_1, t, cols, agg, rank, sem):
    rows, width = t.shape[0], t.shape[0] // 2
    device = lax.axis_index("gx") * lax.axis_size("gy") + lax.axis_index("gy")
    previous = lax.rem(device + devices - 1, devices)
    following = lax.rem(device + 1, devices)
    slabs = previous, following, device
    side = pair_side()
    shift = ROW_CHUNK.bit_length() - 1
    chunk = 4 * ROW_CHUNK
    copies = [
        pltpu.make_async_copy(
            cols_hbm.at[pl.ds(pl.multiple_of(((slab * rows) >> shift) * chunk, chunk), chunk)],
            cols.at[pl.ds(i * chunk, chunk)],
            sem.at[i],
        )
        for i, slab in enumerate(slabs)
    ]
    copies += [pltpu.make_async_copy(t_hbm, t, sem.at[3]), pltpu.make_async_copy(agg_hbm, agg, sem.at[4])]
    for copy in copies:
        copy.start()

    def col(i, r, k):
        return cols[i * chunk + k * ROW_CHUNK + ((slabs[i] * rows) & (ROW_CHUNK - 1)) + r]

    def rank_rows(i, k, where):
        mask = jnp.int32(0)
        for r in range(rows):
            mask = mask | (jnp.int32(1) << (col(i, r, k) & (rows - 1)))
        named, other = jnp.int32(0), jnp.int32(width)
        for r in range(rows):
            hit = (mask >> r) & 1
            place = jnp.where(hit == 1, named, other)
            rank[where * rows + r] = place
            rank[(where + 1) * rows + place] = r
            named = named + hit
            other = other + 1 - hit

    def ranked(where, r):
        return rank[where * rows + r]

    copies[0].wait()
    copies[1].wait()
    rank_rows(0, 3, 0)
    rank_rows(1, 2, 2)
    sent_1, sent_0 = jnp.where(side == ABOVE, 0, 2), jnp.where(side == ABOVE, 2, 0)
    copies[3].wait()
    for j in range(width):
        t_1[j] = t[ranked(sent_1 + 1, j)]
        t_0[j] = t[ranked(sent_0 + 1, j)]
    copies[2].wait()
    copies[4].wait()
    rank_rows(2, 2, 4)
    rank_rows(2, 3, 6)
    for j in range(width):
        note(tab, LIST_0 + j, ranked(sent_1, ranked(sent_0 + 1, j)))
        for which in (BELOW, ABOVE):
            note(tab, BACK + width * which + j, col(which, ranked(5 + 2 * which, j), 3 - which) & (rows - 1))
            for k in range(2):
                note(tab, SIDE_LAB + 8 * which + 2 * j + k, agg[col(which, ranked(5 + 2 * which, j), 2 + k)])
    for u in range(rows):
        row = ranked(sent_1 + 1, u)
        note(tab, ROW + u, row)
        note(tab, NEAR + u, ranked(sent_1, col(2, row, 1) & (rows - 1)))
        note(tab, POS2 + u, ranked(4, col(2, row, 2) & (rows - 1)))
        note(tab, POS3 + u, ranked(6, col(2, row, 3) & (rows - 1)))
        for k in range(4):
            note(tab, OWN_LAB + 4 * u + k, agg[col(2, row, k)])


def put(value, label, column):
    return jnp.where(label == column, value, jnp.zeros_like(value))


def two_columns(value, label):
    return jnp.concatenate([put(value, label, 0), put(value, label, 1)], axis=1)


def near_tiles(tab, a, t, dinv, order):
    block = t.shape[1]
    rows = [entry(tab, ROW + u) for u in order]
    prods = []
    for u, row in zip(order, rows):
        near = entry(tab, ROW + entry(tab, NEAR + u))
        prods.append(
            jnp.concatenate(
                [dot3k(*split(a[row, 0]), *split(t[row])), dot3k(*split(a[row, 1]), *split(t[near]))], axis=1
            )
        )
    tiles = []
    for u, row, prod in zip(order, rows, prods):
        smoothed = dot3k(*split(dinv[row]), *split(prod))
        p0 = t[row] - OMEGA * smoothed[:, :block]
        p1 = -OMEGA * smoothed[:, block:]
        tiles.append(two_columns(p0, entry(tab, OWN_LAB + 4 * u)) + two_columns(p1, entry(tab, OWN_LAB + 4 * u + 1)))
    return tiles


def wide(ref, *places):
    return jnp.concatenate([ref[place] for place in places], axis=0)


def near_kernel(tab, a, t, dinv, near_0, near_1, own, a_high, a_low, a01_high, a01_low):
    rows, width = own.shape[0], near_1.shape[0]
    for u, value in enumerate(near_tiles(tab, a, t, dinv, range(rows))):
        own[u] = value
        if u < width:
            near_1[u] = value
    for j in range(width):
        near_0[j] = own[entry(tab, LIST_0 + j)]
    for u in range(rows):
        row = entry(tab, ROW + u)
        a01_high[u], a01_low[u] = split(jnp.concatenate([a[row, 0], a[row, 1]], axis=1))
        for which in (BELOW, ABOVE):
            a_high[which, u], a_low[which, u] = split(a[row, 2 + which])


def far_blocks(tab, a_high, a_low, dinv, t_high, t_low, order):
    prods = [
        jnp.concatenate(
            [
                dot3k(a_high[which, u], a_low[which, u], t_high[which, pos], t_low[which, pos])
                for which, pos in ((BELOW, entry(tab, POS2 + u)), (ABOVE, entry(tab, POS3 + u)))
            ],
            axis=1,
        )
        for u in order
    ]
    return [-OMEGA * dot3k(*split(dinv[entry(tab, ROW + u)]), *split(prod)) for u, prod in zip(order, prods)]


def split_rows(value, high, low):
    for j in range(value.shape[0]):
        high[j], low[j] = split(value[j])


def far_sent_kernel(tab, a_high, a_low, dinv, t_0, far_1, t_high, t_low):
    side = pair_side()
    block = dinv.shape[1]
    split_rows(t_0, t_high, t_low)
    order = range(far_1.shape[0])
    prods = []
    for u in order:
        pos = entry(tab, POS2 + 8 * side + u)
        high, low = split(dot3k(a_high[side, u], a_low[side, u], t_high[pos], t_low[pos]))
        prods.append(
            (jnp.concatenate([high, a_high[1 - side, u]], axis=1), jnp.concatenate([low, a_low[1 - side, u]], axis=1))
        )
    for u in order:
        both = -OMEGA * dot3k(*split(dinv[entry(tab, ROW + u)]), *prods[u])
        far_1[u, side] = both[:, :block]
        far_1[u, 1 - side] = both[:, block:]


def store_turned(trans, label, place, value):
    block = value.shape[0]
    trans[pl.ds(pl.multiple_of(label * block, block), block), place] = value.T
    trans[pl.ds(pl.multiple_of((1 - label) * block, block), block), place] = jnp.zeros_like(value)


def turn(tab, far, side, trans_high, trans_low):
    for u in range(far.shape[0]):
        block = far.shape[2]
        label = entry(tab, OWN_LAB + 4 * u + 2 + side)
        high, low = split(far[u, side])
        place = slice(u * block, (u + 1) * block)
        store_turned(trans_high, label, place, high)
        store_turned(trans_low, label, place, low)


def coarse_group(trans_high, trans_low, ap_high, ap_low):
    return dot3(trans_high[...], trans_low[...], ap_high[...], ap_low[...])


def mid_kernel(
    tab, a01_high, a01_low, a_high, a_low, dinv, t0_high, t0_low, t_1, far_1, near_0,
    far_0, far, trans_high, trans_low, part, ap_high, ap_low, group,
    t_high, t_low, far_high, far_low, p_high, p_low,
):
    rows, block = far.shape[0], far.shape[2]
    width = rows // 2
    side = pair_side()
    for j in range(width):
        t_high[side, j], t_low[side, j] = t0_high[j], t0_low[j]
        t_high[1 - side, j], t_low[1 - side, j] = split(t_1[j])
    for u in range(width):
        pos = entry(tab, POS2 + 8 * (1 - side) + u)
        far[u, side] = far_1[u, side]
        far[u, 1 - side] = dot3k(*split(far_1[u, 1 - side]), t_high[1 - side, pos], t_low[1 - side, pos])
    for u, both in enumerate(far_blocks(tab, a_high, a_low, dinv, t_high, t_low, range(width, rows))):
        far[width + u, BELOW] = both[:, :block]
        far[width + u, ABOVE] = both[:, block:]
    for j in range(width):
        far_0[j] = far[entry(tab, LIST_0 + j)]
        p_high[j], p_low[j] = split(near_0[j])
    for u in range(rows):
        for which in (BELOW, ABOVE):
            label = entry(tab, OWN_LAB + 4 * u + 2 + which)
            high, low = split(far[u, which])
            far_high[which, u] = two_columns(high, label)
            far_low[which, u] = two_columns(low, label)

    def mine(u, which):
        near = entry(tab, NEAR + u)
        return dot3(a01_high[u], a01_low[u], wide(far_high.at[which], u, near), wide(far_low.at[which], u, near))

    totals = []
    for u in range(rows):
        pos = entry(tab, POS2 + 8 * side + u)
        totals.append(mine(u, side) + dot3k(a_high[side, u], a_low[side, u], p_high[pos], p_low[pos]))
    for u in range(rows):
        place = slice(u * block, (u + 1) * block)
        ap_high[place], ap_low[place] = split(totals[u])
    turn(tab, far, 1 - side, trans_high, trans_low)
    for u in range(rows):
        part[u] = mine(u, 1 - side)
    group[...] = coarse_group(trans_high, trans_low, ap_high, ap_low)


def first_kernel(
    tab, a_high, a_low, part, trans_high, trans_low, near_1,
    ap_high, ap_low, out_1,
    p_high, p_low,
):
    rows, block = part.shape[0], part.shape[1]
    side = 1 - pair_side()
    split_rows(near_1, p_high, p_low)
    totals = []
    for u in range(rows):
        pos = entry(tab, POS2 + 8 * side + u)
        totals.append(part[u] + dot3k(a_high[side, u], a_low[side, u], p_high[pos], p_low[pos]))
    for u in range(rows):
        place = slice(u * block, (u + 1) * block)
        ap_high[place], ap_low[place] = split(totals[u])
    out_1[...] = coarse_group(trans_high, trans_low, ap_high, ap_low)


def far_columns(tab, side, a_high, a_low, p_high, p_low, ap_high, ap_low):
    rows, block = a_high.shape[1], a_high.shape[3]
    values, here = [], []
    for u in range(rows):
        pos = entry(tab, POS2 + 8 * side + u)
        values.append(dot3k(a_high[side, u], a_low[side, u], p_high[pos], p_low[pos]))
    for u in range(rows):
        labels = SIDE_LAB + 8 * side + 2 * entry(tab, POS2 + 8 * side + u)
        here.append(two_columns(values[u][:, :block], entry(tab, labels + 1 - side)))
        high, low = split(values[u][:, block:])
        label = entry(tab, labels + side)
        place = slice(u * block, (u + 1) * block)
        ap_high[place] = two_columns(high, label)
        ap_low[place] = two_columns(low, label)
    return here


def same_kernel(
    tab, a_high, a_low, trans_high, trans_low, far_0, group,
    own_part, ap_high, ap_low, out_1,
    p_high, p_low,
):
    half = trans_high.shape[0]
    block = half // 2
    side = pair_side()
    out_1[:, :half] = group[...]
    for j in range(far_0.shape[0]):
        p_high[j, :, :block], p_low[j, :, :block] = split(far_0[j, 1 - side])
        p_high[j, :, block:], p_low[j, :, block:] = split(far_0[j, side])
    here = far_columns(tab, side, a_high, a_low, p_high, p_low, ap_high, ap_low)
    for u, value in enumerate(here):
        own_part[u] = value
    out_1[:, half:] = coarse_group(trans_high, trans_low, ap_high, ap_low)


def own_part_kernel(tab, a01_high, a01_low, own, t, so_far, own_part, back_high, back_low, own_high, own_low):
    rows = own.shape[0]
    side = 1 - pair_side()
    for j in range(rows // 2):
        back_high[j], back_low[j] = split(t[entry(tab, BACK + (rows // 2) * side + j)])
    for u in range(rows):
        own_high[u], own_low[u] = split(own[u])
    for u in range(rows):
        near = entry(tab, NEAR + u)
        own_part[u] = so_far[u] + dot3(a01_high[u], a01_low[u], wide(own_high, u, near), wide(own_low, u, near))


def second_kernel(
    tab, a_high, a_low, own_part, back_high, back_low, trans_high, trans_low, far_1,
    own_high, own_low, ap_high, ap_low, out_1,
    p_high, p_low,
):
    rows, block = own_part.shape[0], own_part.shape[1]
    half = 2 * block
    side = 1 - pair_side()
    towards = [dot3k(*split(far_1[j, 1 - side]), back_high[j], back_low[j]) for j in range(rows // 2)]
    for j in range(rows // 2):
        p_high[j, :, :block], p_low[j, :, :block] = split(towards[j])
        p_high[j, :, block:], p_low[j, :, block:] = split(far_1[j, side])
    here = far_columns(tab, side, a_high, a_low, p_high, p_low, ap_high, ap_low)
    for u in range(rows):
        place = slice(u * block, (u + 1) * block)
        own_high[place], own_low[place] = split(own_part[u] + here[u])
    out_1[:, :half] = coarse_group(trans_high, trans_low, own_high, own_low)
    out_1[:, half:] = coarse_group(trans_high, trans_low, ap_high, ap_low)


def every_group(trans_high, trans_low, aps, out):
    half = trans_high.shape[0]
    for i in range(len(aps) // 2):
        out[:, i * half : (i + 1) * half] = coarse_group(trans_high, trans_low, aps[2 * i], aps[2 * i + 1])


def other_kernel(tab, far, *refs):
    aps, (out_0, trans_high, trans_low) = refs[:10], refs[10:]
    turn(tab, far, pair_side(), trans_high, trans_low)
    every_group(trans_high, trans_low, aps, out_0)


def own_kernel(own, *refs):
    aps, (out, trans_high, trans_low) = refs[:10], refs[10:]
    rows, block = own.shape[0], own.shape[1]
    for u in range(rows):
        place = slice(u * block, (u + 1) * block)
        high, low = split(own[u])
        trans_high[:, place] = high.T
        trans_low[:, place] = low.T
    every_group(trans_high, trans_low, aps, out)


def write_slots(inverse, totals, results, out, sems):
    block = inverse.shape[1]
    inv = [split(inverse[agg]) for agg in range(2)]
    values = [dot3k(*inv[agg], *split(total)) for agg, _, total in totals]
    copies = []
    for n, ((agg, d, _), value) in enumerate(zip(totals, values)):
        results[n, 0] = value[:, :block]
        results[n, 1] = value[:, block:]
        copies.append(pltpu.make_async_copy(results.at[n], out.at[agg, pl.ds(2 * (d + 3), 2)], sems.at[n]))
        copies[-1].start()
    for copy in copies:
        copy.wait()


OWN_AT, SAME_AT = (1, -1, 2, 0, -2), (0, 2, -1, 1, 3)
PARTS_AT = (-2, -3), (-1, 1), (0,)


def finish_kernel(offsets, part_at, inverse, own, both_0, part, *refs):
    out, results, sems = refs[-3:]
    block = inverse.shape[1]
    half = 2 * block
    side = pair_side()

    def run(way):
        done = []
        for agg in range(2):
            line = slice(agg * block, (agg + 1) * block)
            for d in offsets:
                places = [(ref, at.index(d)) for ref, at in ((own, OWN_AT), (both_0, SAME_AT), (part, part_at)) if d in at]
                shares = [ref[line, i * half : (i + 1) * half] for ref, i in places]
                done.append((agg, way * d, sum(shares[1:], shares[0])))
        write_slots(inverse, done, results, out, sems)

    pl.when(side == ABOVE)(lambda: run(1))
    pl.when(side == BELOW)(lambda: run(-1))


VMEM = pl.BlockSpec(memory_space=pltpu.VMEM)
HBM = pl.BlockSpec(memory_space=pltpu.HBM)


def call(body, outs, ins, scratch=(), micros=1.0, in_hbm=(), out_hbm=(), aliases={}):
    def specs(values, in_place):
        return [HBM if i in in_place else VMEM for i, x in enumerate(values)]

    return pl.pallas_call(
        body,
        out_shape=outs,
        in_specs=specs(ins, in_hbm),
        out_specs=specs(outs, out_hbm),
        scratch_shapes=[pltpu.VMEM(*x) if isinstance(x, tuple) else x for x in scratch],
        input_output_aliases=aliases,
        compiler_params=pltpu.CompilerParams(vmem_limit_bytes=24 * 2**20),
        cost_estimate=pl.CostEstimate(flops=int(micros * 1e9), bytes_accessed=2**20, transcendentals=0),
    )(*ins)


def shards(a, a_cols, t_blocks, t_agg, dinv, coarse_inv):
    devices = lax.axis_size(AXES)
    rows, block = t_blocks.shape[:2]
    width, half, deep = rows // 2, 2 * block, rows * block
    shape = jax.ShapeDtypeStruct
    full = lambda *dims: shape(dims, F32)
    pair = lambda *dims: [shape(dims, BF16), shape(dims, BF16)]
    two = lambda *dims: [(dims, BF16)] * 2
    tile = full(width, block, half)
    cols = a_cols.reshape(-1, ROW_CHUNK, 4).transpose(0, 2, 1).reshape(-1)

    tab, t_0, t_1, t = call(
        functools.partial(load_kernel, devices),
        [shape((TAB, LANES), jnp.int32)] + [full(width, block, block)] * 2 + [full(*t_blocks.shape)],
        [pltpu.with_memory_space_constraint(x, pltpu.HBM) for x in (cols, t_agg, t_blocks)],
        [
            pltpu.SMEM((3 * 4 * ROW_CHUNK,), jnp.int32),
            pltpu.SMEM(t_agg.shape, jnp.int32),
            pltpu.SMEM((8 * rows,), jnp.int32),
            pltpu.SemaphoreType.DMA((5,)),
        ],
        micros=3,
        in_hbm=(0, 1, 2),
    )
    t_1 = exchanged(t_1, 1)
    t_0 = exchanged(t_0, 0)
    near_0, near_1, own, a23_high, a23_low, a01_high, a01_low = call(
        near_kernel,
        [tile, tile, full(rows, block, half)] + pair(2, rows, block, block) + pair(rows, block, half),
        [tab, a, t, dinv],
        micros=2,
    )
    near_0 = exchanged(near_0, 0)
    sent = full(width, 2, block, block)
    far_1, t0_high, t0_low = call(
        far_sent_kernel, [sent] + pair(width, block, block), [tab, a23_high, a23_low, dinv, t_0], micros=2
    )
    got_far_1 = exchanged(far_1, 1)
    far_0, far, out_high, out_low, part, ap_e1_high, ap_e1_low, group = call(
        mid_kernel,
        [sent, full(rows, 2, block, block)]
        + pair(half, deep)
        + [full(rows, block, half)]
        + pair(deep, half)
        + [full(half, half)],
        [tab, a01_high, a01_low, a23_high, a23_low, dinv, t0_high, t0_low, t_1, far_1, near_0],
        two(2, width, block, block) + two(2, rows, block, half) + two(width, block, half),
        micros=3,
    )
    near_1 = exchanged(near_1, 1)
    far_0, far_1 = exchanged(far_0, 0), got_far_1
    part_own, ap_e2_high, ap_e2_low, part_1 = call(
        same_kernel,
        [full(rows, block, half)] + pair(deep, half) + [full(half, 2 * half)],
        [tab, a23_high, a23_low, out_high, out_low, far_0, group],
        two(width, block, half),
        micros=1,
    )
    part_1 = exchanged(part_1, 1)
    part_own, back_high, back_low = call(
        own_part_kernel,
        [full(rows, block, half)] + pair(width, block, block),
        [tab, a01_high, a01_low, own, t, part_own],
        two(rows, block, half),
        micros=1,
    )
    ap_own_high, ap_own_low, ap_o2_high, ap_o2_low, part_2 = call(
        second_kernel,
        pair(deep, half) * 2 + [full(half, 2 * half)],
        [tab, a23_high, a23_low, part_own, back_high, back_low, out_high, out_low, far_1],
        two(width, block, half),
        micros=2,
    )
    part_2 = exchanged(part_2, 1)
    ap_o1_high, ap_o1_low, part_3 = call(
        first_kernel,
        pair(deep, half) + [full(half, half)],
        [tab, a23_high, a23_low, part, out_high, out_low, near_1],
        two(width, block, half),
        micros=2,
    )
    part_3 = exchanged(part_3, 1)
    aps = [
        ap_e1_high, ap_e1_low, ap_o1_high, ap_o1_low, ap_e2_high, ap_e2_low,
        ap_own_high, ap_own_low, ap_o2_high, ap_o2_low,
    ]
    (both_0,) = call(other_kernel, [full(half, 5 * half)], [tab, far] + aps, two(half, deep), micros=2)
    both_0 = exchanged(both_0, 0)
    (total,) = call(own_kernel, [full(half, 5 * half)], [own] + aps, two(half, deep), micros=2)
    out = []
    for i, (offsets, got) in enumerate((((-3, -2, 2, 3), part_1), ((-1, 1), part_2), ((0,), part_3))):
        n = 2 * len(offsets)
        out = call(
            functools.partial(finish_kernel, offsets, PARTS_AT[i]),
            [full(2, 14, block, block)],
            [coarse_inv, total, both_0, got, *out],
            [((n, 2, block, block), F32), pltpu.SemaphoreType.DMA((n,))],
            micros=1,
            in_hbm=(4,),
            out_hbm=(0,),
            aliases={4: 0} if i else {},
        )
    return out[0]


def solution(mesh):
    placed = (
        P(AXES, None, None, None),
        P(),
        P(AXES, None, None),
        P(),
        P(AXES, None, None),
        P(AXES, None, None),
    )
    return jax.shard_map(
        shards,
        mesh=mesh,
        in_specs=placed,
        out_specs=P(AXES, None, None, None),
        check_vma=False,
    )
```

```python
import functools

import jax
import jax.numpy as jnp
from jax import lax
from jax.experimental import pallas as pl
from jax.experimental.pallas import tpu as pltpu
from jax.sharding import PartitionSpec as P


OMEGA = 0.6
AXES = ("gx", "gy")
F32 = jnp.float32
BF16 = jnp.bfloat16
ROW, NEAR, POS2, POS3, LIST_0, OWN_LAB, SIDE_LAB, BACK, TAB = 0, 8, 16, 24, 32, 40, 72, 88, 96
LANES = 128
BELOW, ABOVE = 0, 1
ROW_CHUNK = 128


def exchanged(value, first):
    count = lax.axis_size(AXES)
    pairs = []
    for low in range(first, count + first, 2):
        high = (low + 1) % count
        pairs += [(low, high), (high, low)]
    return lax.ppermute(value, AXES, pairs)


def pair_side():
    return 1 - lax.rem(lax.axis_index("gy"), 2)


def split(x):
    high = x.astype(BF16)
    return high, (x - high.astype(F32)).astype(BF16)


def dot(a, b):
    return jnp.dot(a, b, preferred_element_type=F32)


def dot3(a_high, a_low, b_high, b_low):
    return dot(a_high, b_high) + dot(a_low, b_high) + dot(a_high, b_low)


def dot3k(a_high, a_low, b_high, b_low):
    both = jnp.concatenate([a_high, a_low], axis=1)
    return dot(both, jnp.concatenate([b_high, b_high], axis=0)) + dot(a_high, b_low)


def note(tab, i, value):
    tab[pl.ds(i, 1), :] = jnp.full((1, tab.shape[1]), value, jnp.int32)


def entry(tab, i):
    return tab[pl.ds(i, 1), :][0, 0]


def load_kernel(devices, cols_hbm, agg_hbm, t_hbm, tab, t_0, t_1, t, cols, agg, rank, sem):
    rows, width = t.shape[0], t.shape[0] // 2
    device = lax.axis_index("gx") * lax.axis_size("gy") + lax.axis_index("gy")
    previous = lax.rem(device + devices - 1, devices)
    following = lax.rem(device + 1, devices)
    slabs = previous, following, device
    side = pair_side()
    shift = ROW_CHUNK.bit_length() - 1
    chunk = 4 * ROW_CHUNK
    copies = [
        pltpu.make_async_copy(
            cols_hbm.at[pl.ds(pl.multiple_of(((slab * rows) >> shift) * chunk, chunk), chunk)],
            cols.at[pl.ds(i * chunk, chunk)],
            sem.at[i],
        )
        for i, slab in enumerate(slabs)
    ]
    copies += [pltpu.make_async_copy(t_hbm, t, sem.at[3]), pltpu.make_async_copy(agg_hbm, agg, sem.at[4])]
    for copy in copies:
        copy.start()

    def col(i, r, k):
        return cols[i * chunk + k * ROW_CHUNK + ((slabs[i] * rows) & (ROW_CHUNK - 1)) + r]

    def rank_rows(i, k, where):
        mask = jnp.int32(0)
        for r in range(rows):
            mask = mask | (jnp.int32(1) << (col(i, r, k) & (rows - 1)))
        named, other = jnp.int32(0), jnp.int32(width)
        for r in range(rows):
            hit = (mask >> r) & 1
            place = jnp.where(hit == 1, named, other)
            rank[where * rows + r] = place
            rank[(where + 1) * rows + place] = r
            named = named + hit
            other = other + 1 - hit

    def ranked(where, r):
        return rank[where * rows + r]

    copies[0].wait()
    copies[1].wait()
    rank_rows(0, 3, 0)
    rank_rows(1, 2, 2)
    sent_1, sent_0 = jnp.where(side == ABOVE, 0, 2), jnp.where(side == ABOVE, 2, 0)
    copies[3].wait()
    for j in range(width):
        t_1[j] = t[ranked(sent_1 + 1, j)]
        t_0[j] = t[ranked(sent_0 + 1, j)]
    copies[2].wait()
    copies[4].wait()
    rank_rows(2, 2, 4)
    rank_rows(2, 3, 6)
    for j in range(width):
        note(tab, LIST_0 + j, ranked(sent_1, ranked(sent_0 + 1, j)))
        for which in (BELOW, ABOVE):
            note(tab, BACK + width * which + j, col(which, ranked(5 + 2 * which, j), 3 - which) & (rows - 1))
            for k in range(2):
                note(tab, SIDE_LAB + 8 * which + 2 * j + k, agg[col(which, ranked(5 + 2 * which, j), 2 + k)])
    for u in range(rows):
        row = ranked(sent_1 + 1, u)
        note(tab, ROW + u, row)
        note(tab, NEAR + u, ranked(sent_1, col(2, row, 1) & (rows - 1)))
        note(tab, POS2 + u, ranked(4, col(2, row, 2) & (rows - 1)))
        note(tab, POS3 + u, ranked(6, col(2, row, 3) & (rows - 1)))
        for k in range(4):
            note(tab, OWN_LAB + 4 * u + k, agg[col(2, row, k)])


def put(value, label, column):
    return jnp.where(label == column, value, jnp.zeros_like(value))


def two_columns(value, label):
    return jnp.concatenate([put(value, label, 0), put(value, label, 1)], axis=1)


def near_tiles(tab, a, t, dinv, order):
    block = t.shape[1]
    rows = [entry(tab, ROW + u) for u in order]
    prods = []
    for u, row in zip(order, rows):
        near = entry(tab, ROW + entry(tab, NEAR + u))
        prods.append(
            jnp.concatenate(
                [dot3k(*split(a[row, 0]), *split(t[row])), dot3k(*split(a[row, 1]), *split(t[near]))], axis=1
            )
        )
    tiles = []
    for u, row, prod in zip(order, rows, prods):
        smoothed = dot3k(*split(dinv[row]), *split(prod))
        p0 = t[row] - OMEGA * smoothed[:, :block]
        p1 = -OMEGA * smoothed[:, block:]
        tiles.append(two_columns(p0, entry(tab, OWN_LAB + 4 * u)) + two_columns(p1, entry(tab, OWN_LAB + 4 * u + 1)))
    return tiles


def wide(ref, *places):
    return jnp.concatenate([ref[place] for place in places], axis=0)


def near_kernel(tab, a, t, dinv, near_0, near_1, own, a_high, a_low, a01_high, a01_low):
    rows, width = own.shape[0], near_1.shape[0]
    for u, value in enumerate(near_tiles(tab, a, t, dinv, range(rows))):
        own[u] = value
        if u < width:
            near_1[u] = value
    for j in range(width):
        near_0[j] = own[entry(tab, LIST_0 + j)]
    for u in range(rows):
        row = entry(tab, ROW + u)
        a01_high[u], a01_low[u] = split(jnp.concatenate([a[row, 0], a[row, 1]], axis=1))
        for which in (BELOW, ABOVE):
            a_high[which, u], a_low[which, u] = split(a[row, 2 + which])


def far_blocks(tab, a_high, a_low, dinv, t_high, t_low, order):
    prods = [
        jnp.concatenate(
            [
                dot3k(a_high[which, u], a_low[which, u], t_high[which, pos], t_low[which, pos])
                for which, pos in ((BELOW, entry(tab, POS2 + u)), (ABOVE, entry(tab, POS3 + u)))
            ],
            axis=1,
        )
        for u in order
    ]
    return [-OMEGA * dot3k(*split(dinv[entry(tab, ROW + u)]), *split(prod)) for u, prod in zip(order, prods)]


def split_rows(value, high, low):
    for j in range(value.shape[0]):
        high[j], low[j] = split(value[j])


def far_sent_kernel(tab, a_high, a_low, dinv, t_0, far_1, t_high, t_low):
    side = pair_side()
    block = dinv.shape[1]
    split_rows(t_0, t_high, t_low)
    order = range(far_1.shape[0])
    prods = []
    for u in order:
        pos = entry(tab, POS2 + 8 * side + u)
        high, low = split(dot3k(a_high[side, u], a_low[side, u], t_high[pos], t_low[pos]))
        prods.append(
            (jnp.concatenate([high, a_high[1 - side, u]], axis=1), jnp.concatenate([low, a_low[1 - side, u]], axis=1))
        )
    for u in order:
        both = -OMEGA * dot3k(*split(dinv[entry(tab, ROW + u)]), *prods[u])
        far_1[u, side] = both[:, :block]
        far_1[u, 1 - side] = both[:, block:]


def store_turned(trans, label, place, value):
    block = value.shape[0]
    trans[pl.ds(pl.multiple_of(label * block, block), block), place] = value.T
    trans[pl.ds(pl.multiple_of((1 - label) * block, block), block), place] = jnp.zeros_like(value)


def turn(tab, far, side, trans_high, trans_low):
    for u in range(far.shape[0]):
        block = far.shape[2]
        label = entry(tab, OWN_LAB + 4 * u + 2 + side)
        high, low = split(far[u, side])
        place = slice(u * block, (u + 1) * block)
        store_turned(trans_high, label, place, high)
        store_turned(trans_low, label, place, low)


def coarse_group(trans_high, trans_low, ap_high, ap_low):
    return dot3(trans_high[...], trans_low[...], ap_high[...], ap_low[...])


def far_kernel(tab, a_high, a_low, dinv, t0_high, t0_low, t_1, far_1, after, far_0, far, t_high, t_low):
    rows, block = far.shape[0], far.shape[2]
    width = rows // 2
    side = pair_side()
    for j in range(width):
        t_high[side, j], t_low[side, j] = t0_high[j], t0_low[j]
        t_high[1 - side, j], t_low[1 - side, j] = split(t_1[j])
    for u in range(width):
        pos = entry(tab, POS2 + 8 * (1 - side) + u)
        far[u, side] = far_1[u, side]
        far[u, 1 - side] = dot3k(*split(far_1[u, 1 - side]), t_high[1 - side, pos], t_low[1 - side, pos])
    for u, both in enumerate(far_blocks(tab, a_high, a_low, dinv, t_high, t_low, range(width, rows))):
        far[width + u, BELOW] = both[:, :block]
        far[width + u, ABOVE] = both[:, block:]
    for j in range(width):
        far_0[j] = far[entry(tab, LIST_0 + j)]


def mid_kernel(
    tab, a01_high, a01_low, a_high, a_low, far, near_0,
    trans_high, trans_low, part, ap_high, ap_low, group,
    far_high, far_low, p_high, p_low,
):
    rows, block = far.shape[0], far.shape[2]
    side = pair_side()
    split_rows(near_0, p_high, p_low)
    for u in range(rows):
        for which in (BELOW, ABOVE):
            label = entry(tab, OWN_LAB + 4 * u + 2 + which)
            high, low = split(far[u, which])
            far_high[which, u] = two_columns(high, label)
            far_low[which, u] = two_columns(low, label)

    def mine(u, which):
        near = entry(tab, NEAR + u)
        return dot3(a01_high[u], a01_low[u], wide(far_high.at[which], u, near), wide(far_low.at[which], u, near))

    totals = []
    for u in range(rows):
        pos = entry(tab, POS2 + 8 * side + u)
        totals.append(mine(u, side) + dot3k(a_high[side, u], a_low[side, u], p_high[pos], p_low[pos]))
    for u in range(rows):
        place = slice(u * block, (u + 1) * block)
        ap_high[place], ap_low[place] = split(totals[u])
    turn(tab, far, 1 - side, trans_high, trans_low)
    for u in range(rows):
        part[u] = mine(u, 1 - side)
    group[...] = coarse_group(trans_high, trans_low, ap_high, ap_low)


def first_kernel(
    tab, a_high, a_low, part, trans_high, trans_low, near_1,
    ap_high, ap_low, out_1,
    p_high, p_low,
):
    rows, block = part.shape[0], part.shape[1]
    side = 1 - pair_side()
    split_rows(near_1, p_high, p_low)
    totals = []
    for u in range(rows):
        pos = entry(tab, POS2 + 8 * side + u)
        totals.append(part[u] + dot3k(a_high[side, u], a_low[side, u], p_high[pos], p_low[pos]))
    for u in range(rows):
        place = slice(u * block, (u + 1) * block)
        ap_high[place], ap_low[place] = split(totals[u])
    out_1[...] = coarse_group(trans_high, trans_low, ap_high, ap_low)


def far_columns(tab, side, a_high, a_low, p_high, p_low, ap_high, ap_low):
    rows, block = a_high.shape[1], a_high.shape[3]
    values, here = [], []
    for u in range(rows):
        pos = entry(tab, POS2 + 8 * side + u)
        values.append(dot3k(a_high[side, u], a_low[side, u], p_high[pos], p_low[pos]))
    for u in range(rows):
        labels = SIDE_LAB + 8 * side + 2 * entry(tab, POS2 + 8 * side + u)
        here.append(two_columns(values[u][:, :block], entry(tab, labels + 1 - side)))
        high, low = split(values[u][:, block:])
        label = entry(tab, labels + side)
        place = slice(u * block, (u + 1) * block)
        ap_high[place] = two_columns(high, label)
        ap_low[place] = two_columns(low, label)
    return here


def same_kernel(
    tab, a_high, a_low, trans_high, trans_low, far_0, group, so_far,
    own_part, ap_high, ap_low, out_1,
    p_high, p_low,
):
    half = trans_high.shape[0]
    block = half // 2
    side = pair_side()
    out_1[:, :half] = group[...]
    for j in range(far_0.shape[0]):
        p_high[j, :, :block], p_low[j, :, :block] = split(far_0[j, 1 - side])
        p_high[j, :, block:], p_low[j, :, block:] = split(far_0[j, side])
    here = far_columns(tab, side, a_high, a_low, p_high, p_low, ap_high, ap_low)
    for u, value in enumerate(here):
        own_part[u] = so_far[u] + value
    out_1[:, half:] = coarse_group(trans_high, trans_low, ap_high, ap_low)


def own_part_kernel(tab, a01_high, a01_low, own, t, own_part, back_high, back_low, own_high, own_low):
    rows = own.shape[0]
    side = 1 - pair_side()
    for j in range(rows // 2):
        back_high[j], back_low[j] = split(t[entry(tab, BACK + (rows // 2) * side + j)])
    for u in range(rows):
        own_high[u], own_low[u] = split(own[u])
    for u in range(rows):
        near = entry(tab, NEAR + u)
        own_part[u] = dot3(a01_high[u], a01_low[u], wide(own_high, u, near), wide(own_low, u, near))


def second_kernel(
    tab, a_high, a_low, own_part, back_high, back_low, trans_high, trans_low, far_1,
    own_high, own_low, ap_high, ap_low, out_1,
    p_high, p_low,
):
    rows, block = own_part.shape[0], own_part.shape[1]
    half = 2 * block
    side = 1 - pair_side()
    towards = [dot3k(*split(far_1[j, 1 - side]), back_high[j], back_low[j]) for j in range(rows // 2)]
    for j in range(rows // 2):
        p_high[j, :, :block], p_low[j, :, :block] = split(towards[j])
        p_high[j, :, block:], p_low[j, :, block:] = split(far_1[j, side])
    here = far_columns(tab, side, a_high, a_low, p_high, p_low, ap_high, ap_low)
    for u in range(rows):
        place = slice(u * block, (u + 1) * block)
        own_high[place], own_low[place] = split(own_part[u] + here[u])
    out_1[:, :half] = coarse_group(trans_high, trans_low, own_high, own_low)
    out_1[:, half:] = coarse_group(trans_high, trans_low, ap_high, ap_low)


def every_group(trans_high, trans_low, aps, out):
    half = trans_high.shape[0]
    for i in range(len(aps) // 2):
        out[:, i * half : (i + 1) * half] = coarse_group(trans_high, trans_low, aps[2 * i], aps[2 * i + 1])


def other_kernel(tab, far, *refs):
    aps, (out_0, trans_high, trans_low) = refs[:10], refs[10:]
    turn(tab, far, pair_side(), trans_high, trans_low)
    every_group(trans_high, trans_low, aps, out_0)


def own_kernel(own, *refs):
    aps, (out, trans_high, trans_low) = refs[:10], refs[10:]
    rows, block = own.shape[0], own.shape[1]
    for u in range(rows):
        place = slice(u * block, (u + 1) * block)
        high, low = split(own[u])
        trans_high[:, place] = high.T
        trans_low[:, place] = low.T
    every_group(trans_high, trans_low, aps, out)


def write_slots(inverse, totals, results, out, sems):
    block = inverse.shape[1]
    inv = [split(inverse[agg]) for agg in range(2)]
    values = [dot3k(*inv[agg], *split(total)) for agg, _, total in totals]
    copies = []
    for n, ((agg, d, _), value) in enumerate(zip(totals, values)):
        results[n, 0] = value[:, :block]
        results[n, 1] = value[:, block:]
        copies.append(pltpu.make_async_copy(results.at[n], out.at[agg, pl.ds(2 * (d + 3), 2)], sems.at[n]))
        copies[-1].start()
    for copy in copies:
        copy.wait()


OWN_AT, SAME_AT = (1, -1, 2, 0, -2), (0, 2, -1, 1, 3)
PARTS_AT = (-2, -3), (-1, 1), (0,)


def finish_kernel(offsets, part_at, inverse, own, *refs):
    refs, (out, results, sems) = refs[:-3], refs[-3:]
    others = ((refs[0], SAME_AT), (refs[1], part_at)) if len(refs) > 1 else ((refs[0], part_at),)
    block = inverse.shape[1]
    half = 2 * block
    side = pair_side()

    def run(way):
        done = []
        for agg in range(2):
            line = slice(agg * block, (agg + 1) * block)
            for d in offsets:
                places = [(ref, at.index(d)) for ref, at in ((own, OWN_AT), *others) if d in at]
                shares = [ref[line, i * half : (i + 1) * half] for ref, i in places]
                done.append((agg, way * d, sum(shares[1:], shares[0])))
        write_slots(inverse, done, results, out, sems)

    pl.when(side == ABOVE)(lambda: run(1))
    pl.when(side == BELOW)(lambda: run(-1))


VMEM = pl.BlockSpec(memory_space=pltpu.VMEM)
HBM = pl.BlockSpec(memory_space=pltpu.HBM)


def call(body, outs, ins, scratch=(), micros=1.0, in_hbm=(), out_hbm=(), aliases={}):
    def specs(values, in_place):
        return [HBM if i in in_place else VMEM for i, x in enumerate(values)]

    return pl.pallas_call(
        body,
        out_shape=outs,
        in_specs=specs(ins, in_hbm),
        out_specs=specs(outs, out_hbm),
        scratch_shapes=[pltpu.VMEM(*x) if isinstance(x, tuple) else x for x in scratch],
        input_output_aliases=aliases,
        compiler_params=pltpu.CompilerParams(vmem_limit_bytes=24 * 2**20),
        cost_estimate=pl.CostEstimate(flops=int(micros * 1e9), bytes_accessed=2**20, transcendentals=0),
    )(*ins)


def shards(a, a_cols, t_blocks, t_agg, dinv, coarse_inv):
    devices = lax.axis_size(AXES)
    rows, block = t_blocks.shape[:2]
    width, half, deep = rows // 2, 2 * block, rows * block
    shape = jax.ShapeDtypeStruct
    full = lambda *dims: shape(dims, F32)
    pair = lambda *dims: [shape(dims, BF16), shape(dims, BF16)]
    two = lambda *dims: [(dims, BF16)] * 2
    tile = full(width, block, half)
    cols = a_cols.reshape(-1, ROW_CHUNK, 4).transpose(0, 2, 1).reshape(-1)

    tab, t_0, t_1, t = call(
        functools.partial(load_kernel, devices),
        [shape((TAB, LANES), jnp.int32)] + [full(width, block, block)] * 2 + [full(*t_blocks.shape)],
        [pltpu.with_memory_space_constraint(x, pltpu.HBM) for x in (cols, t_agg, t_blocks)],
        [
            pltpu.SMEM((3 * 4 * ROW_CHUNK,), jnp.int32),
            pltpu.SMEM(t_agg.shape, jnp.int32),
            pltpu.SMEM((8 * rows,), jnp.int32),
            pltpu.SemaphoreType.DMA((5,)),
        ],
        micros=3,
        in_hbm=(0, 1, 2),
    )
    t_1 = exchanged(t_1, 1)
    t_0 = exchanged(t_0, 0)
    near_0, near_1, own, a23_high, a23_low, a01_high, a01_low = call(
        near_kernel,
        [tile, tile, full(rows, block, half)] + pair(2, rows, block, block) + pair(rows, block, half),
        [tab, a, t, dinv],
        micros=2,
    )
    near_0 = exchanged(near_0, 0)
    sent = full(width, 2, block, block)
    far_1, t0_high, t0_low = call(
        far_sent_kernel, [sent] + pair(width, block, block), [tab, a23_high, a23_low, dinv, t_0], micros=2
    )
    got_far_1 = exchanged(far_1, 1)
    near_1 = exchanged(near_1, 1)
    part_own, back_high, back_low = call(
        own_part_kernel,
        [full(rows, block, half)] + pair(width, block, block),
        [tab, a01_high, a01_low, own, t],
        two(rows, block, half),
        micros=1,
    )
    far_0, far = call(
        far_kernel,
        [sent, full(rows, 2, block, block)],
        [tab, a23_high, a23_low, dinv, t0_high, t0_low, t_1, far_1, part_own],
        two(2, width, block, block),
        micros=1,
    )
    far_0, far_1 = exchanged(far_0, 0), got_far_1
    out_high, out_low, part, ap_e1_high, ap_e1_low, group = call(
        mid_kernel,
        pair(half, deep) + [full(rows, block, half)] + pair(deep, half) + [full(half, half)],
        [tab, a01_high, a01_low, a23_high, a23_low, far, near_0],
        two(2, rows, block, half) + two(width, block, half),
        micros=2,
    )
    part_own, ap_e2_high, ap_e2_low, part_1 = call(
        same_kernel,
        [full(rows, block, half)] + pair(deep, half) + [full(half, 2 * half)],
        [tab, a23_high, a23_low, out_high, out_low, far_0, group, part_own],
        two(width, block, half),
        micros=1,
    )
    part_1 = exchanged(part_1, 1)
    ap_own_high, ap_own_low, ap_o2_high, ap_o2_low, part_2 = call(
        second_kernel,
        pair(deep, half) * 2 + [full(half, 2 * half)],
        [tab, a23_high, a23_low, part_own, back_high, back_low, out_high, out_low, far_1],
        two(width, block, half),
        micros=2,
    )
    part_2 = exchanged(part_2, 1)
    ap_o1_high, ap_o1_low, part_3 = call(
        first_kernel,
        pair(deep, half) + [full(half, half)],
        [tab, a23_high, a23_low, part, out_high, out_low, near_1],
        two(width, block, half),
        micros=2,
    )
    part_3 = exchanged(part_3, 1)
    aps = [
        ap_e1_high, ap_e1_low, ap_o1_high, ap_o1_low, ap_e2_high, ap_e2_low,
        ap_own_high, ap_own_low, ap_o2_high, ap_o2_low,
    ]
    (both_0,) = call(other_kernel, [full(half, 5 * half)], [tab, far] + aps, two(half, deep), micros=2)
    both_0 = exchanged(both_0, 0)
    (total,) = call(own_kernel, [full(half, 5 * half)], [own] + aps, two(half, deep), micros=2)
    out = []
    for i, (offsets, got) in enumerate((((-3, -2), part_1), ((-1, 1, 2, 3), part_2), ((0,), part_3))):
        n = 2 * len(offsets)
        out = call(
            functools.partial(finish_kernel, offsets, PARTS_AT[i]),
            [full(2, 14, block, block)],
            [coarse_inv, total] + ([both_0] if i else []) + [got, *out],
            [((n, 2, block, block), F32), pltpu.SemaphoreType.DMA((n,))],
            micros=1,
            in_hbm=(4,),
            out_hbm=(0,),
            aliases={4: 0} if i else {},
        )
    return out[0]


def solution(mesh):
    placed = (
        P(AXES, None, None, None),
        P(),
        P(AXES, None, None),
        P(),
        P(AXES, None, None),
        P(AXES, None, None),
    )
    return jax.shard_map(
        shards,
        mesh=mesh,
        in_specs=placed,
        out_specs=P(AXES, None, None, None),
        check_vma=False,
    )
```

```python
import functools

import jax
import jax.numpy as jnp
from jax import lax
from jax.experimental import pallas as pl
from jax.experimental.pallas import tpu as pltpu
from jax.sharding import PartitionSpec as P


OMEGA = 0.6
AXES = ("gx", "gy")
F32 = jnp.float32
BF16 = jnp.bfloat16
ROW, NEAR, POS2, POS3, LIST_0, OWN_LAB, SIDE_LAB, BACK, TAB = 0, 8, 16, 24, 32, 40, 72, 88, 96
LANES = 128
BELOW, ABOVE = 0, 1
ROW_CHUNK = 128


def exchanged(value, first):
    count = lax.axis_size(AXES)
    pairs = []
    for low in range(first, count + first, 2):
        high = (low + 1) % count
        pairs += [(low, high), (high, low)]
    return lax.ppermute(value, AXES, pairs)


def pair_side():
    return 1 - lax.rem(lax.axis_index("gy"), 2)


def split(x):
    high = x.astype(BF16)
    return high, (x - high.astype(F32)).astype(BF16)


def dot(a, b):
    return jnp.dot(a, b, preferred_element_type=F32)


def dot3(a_high, a_low, b_high, b_low):
    return dot(a_high, b_high) + dot(a_low, b_high) + dot(a_high, b_low)


def dot3k(a_high, a_low, b_high, b_low):
    both = jnp.concatenate([a_high, a_low], axis=1)
    return dot(both, jnp.concatenate([b_high, b_high], axis=0)) + dot(a_high, b_low)


def note(tab, i, value):
    tab[pl.ds(i, 1), :] = jnp.full((1, tab.shape[1]), value, jnp.int32)


def entry(tab, i):
    return tab[pl.ds(i, 1), :][0, 0]


def load_kernel(devices, cols_hbm, agg_hbm, t_hbm, tab, t_0, t_1, t, cols, agg, rank, sem):
    rows, width = t.shape[0], t.shape[0] // 2
    device = lax.axis_index("gx") * lax.axis_size("gy") + lax.axis_index("gy")
    previous = lax.rem(device + devices - 1, devices)
    following = lax.rem(device + 1, devices)
    slabs = previous, following, device
    side = pair_side()
    shift = ROW_CHUNK.bit_length() - 1
    chunk = 4 * ROW_CHUNK
    copies = [
        pltpu.make_async_copy(
            cols_hbm.at[pl.ds(pl.multiple_of(((slab * rows) >> shift) * chunk, chunk), chunk)],
            cols.at[pl.ds(i * chunk, chunk)],
            sem.at[i],
        )
        for i, slab in enumerate(slabs)
    ]
    copies += [pltpu.make_async_copy(t_hbm, t, sem.at[3]), pltpu.make_async_copy(agg_hbm, agg, sem.at[4])]
    for copy in copies:
        copy.start()

    def col(i, r, k):
        return cols[i * chunk + k * ROW_CHUNK + ((slabs[i] * rows) & (ROW_CHUNK - 1)) + r]

    def rank_rows(i, k, where):
        mask = jnp.int32(0)
        for r in range(rows):
            mask = mask | (jnp.int32(1) << (col(i, r, k) & (rows - 1)))
        named, other = jnp.int32(0), jnp.int32(width)
        for r in range(rows):
            hit = (mask >> r) & 1
            place = jnp.where(hit == 1, named, other)
            rank[where * rows + r] = place
            rank[(where + 1) * rows + place] = r
            named = named + hit
            other = other + 1 - hit

    def ranked(where, r):
        return rank[where * rows + r]

    copies[0].wait()
    copies[1].wait()
    rank_rows(0, 3, 0)
    rank_rows(1, 2, 2)
    sent_1, sent_0 = jnp.where(side == ABOVE, 0, 2), jnp.where(side == ABOVE, 2, 0)
    copies[3].wait()
    for j in range(width):
        t_1[j] = t[ranked(sent_1 + 1, j)]
        t_0[j] = t[ranked(sent_0 + 1, j)]
    copies[2].wait()
    copies[4].wait()
    rank_rows(2, 2, 4)
    rank_rows(2, 3, 6)
    for j in range(width):
        note(tab, LIST_0 + j, ranked(sent_1, ranked(sent_0 + 1, j)))
        for which in (BELOW, ABOVE):
            note(tab, BACK + width * which + j, col(which, ranked(5 + 2 * which, j), 3 - which) & (rows - 1))
            for k in range(2):
                note(tab, SIDE_LAB + 8 * which + 2 * j + k, agg[col(which, ranked(5 + 2 * which, j), 2 + k)])
    for u in range(rows):
        row = ranked(sent_1 + 1, u)
        note(tab, ROW + u, row)
        note(tab, NEAR + u, ranked(sent_1, col(2, row, 1) & (rows - 1)))
        note(tab, POS2 + u, ranked(4, col(2, row, 2) & (rows - 1)))
        note(tab, POS3 + u, ranked(6, col(2, row, 3) & (rows - 1)))
        for k in range(4):
            note(tab, OWN_LAB + 4 * u + k, agg[col(2, row, k)])


def put(value, label, column):
    return jnp.where(label == column, value, jnp.zeros_like(value))


def two_columns(value, label):
    return jnp.concatenate([put(value, label, 0), put(value, label, 1)], axis=1)


def near_tiles(tab, a, t, dinv, order):
    block = t.shape[1]
    rows = [entry(tab, ROW + u) for u in order]
    prods = []
    for u, row in zip(order, rows):
        near = entry(tab, ROW + entry(tab, NEAR + u))
        prods.append(
            jnp.concatenate(
                [dot3k(*split(a[row, 0]), *split(t[row])), dot3k(*split(a[row, 1]), *split(t[near]))], axis=1
            )
        )
    tiles = []
    for u, row, prod in zip(order, rows, prods):
        smoothed = dot3k(*split(dinv[row]), *split(prod))
        p0 = t[row] - OMEGA * smoothed[:, :block]
        p1 = -OMEGA * smoothed[:, block:]
        tiles.append(two_columns(p0, entry(tab, OWN_LAB + 4 * u)) + two_columns(p1, entry(tab, OWN_LAB + 4 * u + 1)))
    return tiles


def wide(ref, *places):
    return jnp.concatenate([ref[place] for place in places], axis=0)


def near_kernel(tab, a, t, dinv, near_0, near_1, own, a_high, a_low, a01_high, a01_low):
    rows, width = own.shape[0], near_1.shape[0]
    for u, value in enumerate(near_tiles(tab, a, t, dinv, range(rows))):
        own[u] = value
        if u < width:
            near_1[u] = value
    for j in range(width):
        near_0[j] = own[entry(tab, LIST_0 + j)]
    for u in range(rows):
        row = entry(tab, ROW + u)
        a01_high[u], a01_low[u] = split(jnp.concatenate([a[row, 0], a[row, 1]], axis=1))
        for which in (BELOW, ABOVE):
            a_high[which, u], a_low[which, u] = split(a[row, 2 + which])


def far_blocks(tab, a_high, a_low, dinv, t_high, t_low, order):
    prods = [
        jnp.concatenate(
            [
                dot3k(a_high[which, u], a_low[which, u], t_high[which, pos], t_low[which, pos])
                for which, pos in ((BELOW, entry(tab, POS2 + u)), (ABOVE, entry(tab, POS3 + u)))
            ],
            axis=1,
        )
        for u in order
    ]
    return [-OMEGA * dot3k(*split(dinv[entry(tab, ROW + u)]), *split(prod)) for u, prod in zip(order, prods)]


def split_rows(value, high, low):
    for j in range(value.shape[0]):
        high[j], low[j] = split(value[j])


def far_sent_kernel(tab, a_high, a_low, dinv, t_0, far_1, t_high, t_low):
    side = pair_side()
    block = dinv.shape[1]
    split_rows(t_0, t_high, t_low)
    order = range(far_1.shape[0])
    prods = []
    for u in order:
        pos = entry(tab, POS2 + 8 * side + u)
        high, low = split(dot3k(a_high[side, u], a_low[side, u], t_high[pos], t_low[pos]))
        prods.append(
            (jnp.concatenate([high, a_high[1 - side, u]], axis=1), jnp.concatenate([low, a_low[1 - side, u]], axis=1))
        )
    for u in order:
        both = -OMEGA * dot3k(*split(dinv[entry(tab, ROW + u)]), *prods[u])
        far_1[u, side] = both[:, :block]
        far_1[u, 1 - side] = both[:, block:]


def store_turned(trans, label, place, value):
    block = value.shape[0]
    trans[pl.ds(pl.multiple_of(label * block, block), block), place] = value.T
    trans[pl.ds(pl.multiple_of((1 - label) * block, block), block), place] = jnp.zeros_like(value)


def turn(tab, far, side, trans_high, trans_low):
    for u in range(far.shape[0]):
        block = far.shape[2]
        label = entry(tab, OWN_LAB + 4 * u + 2 + side)
        high, low = split(far[u, side])
        place = slice(u * block, (u + 1) * block)
        store_turned(trans_high, label, place, high)
        store_turned(trans_low, label, place, low)


def coarse_group(trans_high, trans_low, ap_high, ap_low):
    return dot3(trans_high[...], trans_low[...], ap_high[...], ap_low[...])


def far_kernel(tab, a_high, a_low, dinv, t0_high, t0_low, t_1, far_1, far_0, far, t_high, t_low):
    rows, block = far.shape[0], far.shape[2]
    width = rows // 2
    side = pair_side()
    for j in range(width):
        t_high[side, j], t_low[side, j] = t0_high[j], t0_low[j]
        t_high[1 - side, j], t_low[1 - side, j] = split(t_1[j])
    for u in range(width):
        pos = entry(tab, POS2 + 8 * (1 - side) + u)
        far[u, side] = far_1[u, side]
        far[u, 1 - side] = dot3k(*split(far_1[u, 1 - side]), t_high[1 - side, pos], t_low[1 - side, pos])
    for u, both in enumerate(far_blocks(tab, a_high, a_low, dinv, t_high, t_low, range(width, rows))):
        far[width + u, BELOW] = both[:, :block]
        far[width + u, ABOVE] = both[:, block:]
    for j in range(width):
        far_0[j] = far[entry(tab, LIST_0 + j)]


def mid_kernel(
    tab, a01_high, a01_low, a_high, a_low, far, near_0,
    trans_high, trans_low, part, ap_high, ap_low, group,
    far_high, far_low, p_high, p_low,
):
    rows, block = far.shape[0], far.shape[2]
    side = pair_side()
    split_rows(near_0, p_high, p_low)
    for u in range(rows):
        for which in (BELOW, ABOVE):
            label = entry(tab, OWN_LAB + 4 * u + 2 + which)
            high, low = split(far[u, which])
            far_high[which, u] = two_columns(high, label)
            far_low[which, u] = two_columns(low, label)

    def mine(u, which):
        near = entry(tab, NEAR + u)
        return dot3(a01_high[u], a01_low[u], wide(far_high.at[which], u, near), wide(far_low.at[which], u, near))

    totals = []
    for u in range(rows):
        pos = entry(tab, POS2 + 8 * side + u)
        totals.append(mine(u, side) + dot3k(a_high[side, u], a_low[side, u], p_high[pos], p_low[pos]))
    for u in range(rows):
        place = slice(u * block, (u + 1) * block)
        ap_high[place], ap_low[place] = split(totals[u])
    turn(tab, far, 1 - side, trans_high, trans_low)
    for u in range(rows):
        part[u] = mine(u, 1 - side)
    group[...] = coarse_group(trans_high, trans_low, ap_high, ap_low)


def first_kernel(
    tab, a_high, a_low, part, trans_high, trans_low, near_1,
    ap_high, ap_low, out_1,
    p_high, p_low,
):
    rows, block = part.shape[0], part.shape[1]
    side = 1 - pair_side()
    split_rows(near_1, p_high, p_low)
    totals = []
    for u in range(rows):
        pos = entry(tab, POS2 + 8 * side + u)
        totals.append(part[u] + dot3k(a_high[side, u], a_low[side, u], p_high[pos], p_low[pos]))
    for u in range(rows):
        place = slice(u * block, (u + 1) * block)
        ap_high[place], ap_low[place] = split(totals[u])
    out_1[...] = coarse_group(trans_high, trans_low, ap_high, ap_low)


def far_columns(tab, side, a_high, a_low, p_high, p_low, ap_high, ap_low):
    rows, block = a_high.shape[1], a_high.shape[3]
    values, here = [], []
    for u in range(rows):
        pos = entry(tab, POS2 + 8 * side + u)
        values.append(dot3k(a_high[side, u], a_low[side, u], p_high[pos], p_low[pos]))
    for u in range(rows):
        labels = SIDE_LAB + 8 * side + 2 * entry(tab, POS2 + 8 * side + u)
        here.append(two_columns(values[u][:, :block], entry(tab, labels + 1 - side)))
        high, low = split(values[u][:, block:])
        label = entry(tab, labels + side)
        place = slice(u * block, (u + 1) * block)
        ap_high[place] = two_columns(high, label)
        ap_low[place] = two_columns(low, label)
    return here


def same_kernel(
    tab, a_high, a_low, trans_high, trans_low, far_0, group,
    own_part, ap_high, ap_low, out_1,
    p_high, p_low,
):
    half = trans_high.shape[0]
    block = half // 2
    side = pair_side()
    out_1[:, :half] = group[...]
    for j in range(far_0.shape[0]):
        p_high[j, :, :block], p_low[j, :, :block] = split(far_0[j, 1 - side])
        p_high[j, :, block:], p_low[j, :, block:] = split(far_0[j, side])
    here = far_columns(tab, side, a_high, a_low, p_high, p_low, ap_high, ap_low)
    for u, value in enumerate(here):
        own_part[u] = value
    out_1[:, half:] = coarse_group(trans_high, trans_low, ap_high, ap_low)


def own_part_kernel(tab, a01_high, a01_low, own, t, so_far, own_part, back_high, back_low, own_high, own_low):
    rows = own.shape[0]
    side = 1 - pair_side()
    for j in range(rows // 2):
        back_high[j], back_low[j] = split(t[entry(tab, BACK + (rows // 2) * side + j)])
    for u in range(rows):
        own_high[u], own_low[u] = split(own[u])
    for u in range(rows):
        near = entry(tab, NEAR + u)
        own_part[u] = so_far[u] + dot3(a01_high[u], a01_low[u], wide(own_high, u, near), wide(own_low, u, near))


def second_kernel(
    tab, a_high, a_low, own_part, back_high, back_low, trans_high, trans_low, far_1,
    own_high, own_low, ap_high, ap_low, out_1,
    p_high, p_low,
):
    rows, block = own_part.shape[0], own_part.shape[1]
    half = 2 * block
    side = 1 - pair_side()
    towards = [dot3k(*split(far_1[j, 1 - side]), back_high[j], back_low[j]) for j in range(rows // 2)]
    for j in range(rows // 2):
        p_high[j, :, :block], p_low[j, :, :block] = split(towards[j])
        p_high[j, :, block:], p_low[j, :, block:] = split(far_1[j, side])
    here = far_columns(tab, side, a_high, a_low, p_high, p_low, ap_high, ap_low)
    for u in range(rows):
        place = slice(u * block, (u + 1) * block)
        own_high[place], own_low[place] = split(own_part[u] + here[u])
    out_1[:, :half] = coarse_group(trans_high, trans_low, own_high, own_low)
    out_1[:, half:] = coarse_group(trans_high, trans_low, ap_high, ap_low)


def every_group(trans_high, trans_low, aps, out):
    half = trans_high.shape[0]
    for i in range(len(aps) // 2):
        out[:, i * half : (i + 1) * half] = coarse_group(trans_high, trans_low, aps[2 * i], aps[2 * i + 1])


def other_kernel(tab, far, *refs):
    aps, (out_0, trans_high, trans_low) = refs[:10], refs[10:]
    turn(tab, far, pair_side(), trans_high, trans_low)
    every_group(trans_high, trans_low, aps, out_0)


def own_kernel(own, *refs):
    aps, (out, trans_high, trans_low) = refs[:10], refs[10:]
    rows, block = own.shape[0], own.shape[1]
    for u in range(rows):
        place = slice(u * block, (u + 1) * block)
        high, low = split(own[u])
        trans_high[:, place] = high.T
        trans_low[:, place] = low.T
    every_group(trans_high, trans_low, aps, out)


def write_slots(inverse, totals, results, out, sems):
    block = inverse.shape[1]
    inv = [split(inverse[agg]) for agg in range(2)]
    values = [dot3k(*inv[agg], *split(total)) for agg, _, total in totals]
    copies = []
    for n, ((agg, d, _), value) in enumerate(zip(totals, values)):
        results[n, 0] = value[:, :block]
        results[n, 1] = value[:, block:]
        copies.append(pltpu.make_async_copy(results.at[n], out.at[agg, pl.ds(2 * (d + 3), 2)], sems.at[n]))
        copies[-1].start()
    for copy in copies:
        copy.wait()


OWN_AT, SAME_AT = (1, -1, 2, 0, -2), (0, 2, -1, 1, 3)
PARTS_AT = (-2, -3), (-1, 1), (0,)


def finish_kernel(offsets, part_at, inverse, own, *refs):
    refs, (out, results, sems) = refs[:-3], refs[-3:]
    others = ((refs[0], SAME_AT), (refs[1], part_at)) if len(refs) > 1 else ((refs[0], part_at),)
    block = inverse.shape[1]
    half = 2 * block
    side = pair_side()

    def run(way):
        done = []
        for agg in range(2):
            line = slice(agg * block, (agg + 1) * block)
            for d in offsets:
                places = [(ref, at.index(d)) for ref, at in ((own, OWN_AT), *others) if d in at]
                shares = [ref[line, i * half : (i + 1) * half] for ref, i in places]
                done.append((agg, way * d, sum(shares[1:], shares[0])))
        write_slots(inverse, done, results, out, sems)

    pl.when(side == ABOVE)(lambda: run(1))
    pl.when(side == BELOW)(lambda: run(-1))


VMEM = pl.BlockSpec(memory_space=pltpu.VMEM)
HBM = pl.BlockSpec(memory_space=pltpu.HBM)


def call(body, outs, ins, scratch=(), micros=1.0, in_hbm=(), out_hbm=(), aliases={}):
    def specs(values, in_place):
        return [HBM if i in in_place else VMEM for i, x in enumerate(values)]

    return pl.pallas_call(
        body,
        out_shape=outs,
        in_specs=specs(ins, in_hbm),
        out_specs=specs(outs, out_hbm),
        scratch_shapes=[pltpu.VMEM(*x) if isinstance(x, tuple) else x for x in scratch],
        input_output_aliases=aliases,
        compiler_params=pltpu.CompilerParams(vmem_limit_bytes=24 * 2**20),
        cost_estimate=pl.CostEstimate(flops=int(micros * 1e9), bytes_accessed=2**20, transcendentals=0),
    )(*ins)


def shards(a, a_cols, t_blocks, t_agg, dinv, coarse_inv):
    devices = lax.axis_size(AXES)
    rows, block = t_blocks.shape[:2]
    width, half, deep = rows // 2, 2 * block, rows * block
    shape = jax.ShapeDtypeStruct
    full = lambda *dims: shape(dims, F32)
    pair = lambda *dims: [shape(dims, BF16), shape(dims, BF16)]
    two = lambda *dims: [(dims, BF16)] * 2
    tile = full(width, block, half)
    cols = a_cols.reshape(-1, ROW_CHUNK, 4).transpose(0, 2, 1).reshape(-1)

    tab, t_0, t_1, t = call(
        functools.partial(load_kernel, devices),
        [shape((TAB, LANES), jnp.int32)] + [full(width, block, block)] * 2 + [full(*t_blocks.shape)],
        [pltpu.with_memory_space_constraint(x, pltpu.HBM) for x in (cols, t_agg, t_blocks)],
        [
            pltpu.SMEM((3 * 4 * ROW_CHUNK,), jnp.int32),
            pltpu.SMEM(t_agg.shape, jnp.int32),
            pltpu.SMEM((8 * rows,), jnp.int32),
            pltpu.SemaphoreType.DMA((5,)),
        ],
        micros=3,
        in_hbm=(0, 1, 2),
    )
    t_1 = exchanged(t_1, 1)
    t_0 = exchanged(t_0, 0)
    near_0, near_1, own, a23_high, a23_low, a01_high, a01_low = call(
        near_kernel,
        [tile, tile, full(rows, block, half)] + pair(2, rows, block, block) + pair(rows, block, half),
        [tab, a, t, dinv],
        micros=2,
    )
    near_0 = exchanged(near_0, 0)
    sent = full(width, 2, block, block)
    far_1, t0_high, t0_low = call(
        far_sent_kernel, [sent] + pair(width, block, block), [tab, a23_high, a23_low, dinv, t_0], micros=2
    )
    got_far_1 = exchanged(far_1, 1)
    near_1 = exchanged(near_1, 1)
    far_0, far = call(
        far_kernel,
        [sent, full(rows, 2, block, block)],
        [tab, a23_high, a23_low, dinv, t0_high, t0_low, t_1, far_1],
        two(2, width, block, block),
        micros=1,
    )
    far_0, far_1 = exchanged(far_0, 0), got_far_1
    out_high, out_low, part, ap_e1_high, ap_e1_low, group = call(
        mid_kernel,
        pair(half, deep) + [full(rows, block, half)] + pair(deep, half) + [full(half, half)],
        [tab, a01_high, a01_low, a23_high, a23_low, far, near_0],
        two(2, rows, block, half) + two(width, block, half),
        micros=2,
    )
    part_own, ap_e2_high, ap_e2_low, part_1 = call(
        same_kernel,
        [full(rows, block, half)] + pair(deep, half) + [full(half, 2 * half)],
        [tab, a23_high, a23_low, out_high, out_low, far_0, group],
        two(width, block, half),
        micros=1,
    )
    part_1 = exchanged(part_1, 1)
    part_own, back_high, back_low = call(
        own_part_kernel,
        [full(rows, block, half)] + pair(width, block, block),
        [tab, a01_high, a01_low, own, t, part_own],
        two(rows, block, half),
        micros=1,
    )
    ap_own_high, ap_own_low, ap_o2_high, ap_o2_low, part_2 = call(
        second_kernel,
        pair(deep, half) * 2 + [full(half, 2 * half)],
        [tab, a23_high, a23_low, part_own, back_high, back_low, out_high, out_low, far_1],
        two(width, block, half),
        micros=2,
    )
    part_2 = exchanged(part_2, 1)
    ap_o1_high, ap_o1_low, part_3 = call(
        first_kernel,
        pair(deep, half) + [full(half, half)],
        [tab, a23_high, a23_low, part, out_high, out_low, near_1],
        two(width, block, half),
        micros=2,
    )
    part_3 = exchanged(part_3, 1)
    aps = [
        ap_e1_high, ap_e1_low, ap_o1_high, ap_o1_low, ap_e2_high, ap_e2_low,
        ap_own_high, ap_own_low, ap_o2_high, ap_o2_low,
    ]
    (both_0,) = call(other_kernel, [full(half, 5 * half)], [tab, far] + aps, two(half, deep), micros=2)
    both_0 = exchanged(both_0, 0)
    (total,) = call(own_kernel, [full(half, 5 * half)], [own] + aps, two(half, deep), micros=2)
    out = []
    for i, (offsets, got) in enumerate((((-3, -2), part_1), ((-1, 1, 2, 3), part_2), ((0,), part_3))):
        n = 2 * len(offsets)
        out = call(
            functools.partial(finish_kernel, offsets, PARTS_AT[i]),
            [full(2, 14, block, block)],
            [coarse_inv, total] + ([both_0] if i else []) + [got, *out],
            [((n, 2, block, block), F32), pltpu.SemaphoreType.DMA((n,))],
            micros=1,
            in_hbm=(4,),
            out_hbm=(0,),
            aliases={4: 0} if i else {},
        )
    return out[0]


def solution(mesh):
    placed = (
        P(AXES, None, None, None),
        P(),
        P(AXES, None, None),
        P(),
        P(AXES, None, None),
        P(AXES, None, None),
    )
    return jax.shard_map(
        shards,
        mesh=mesh,
        in_specs=placed,
        out_specs=P(AXES, None, None, None),
        check_vma=False,
    )
```

```python
import functools

import jax
import jax.numpy as jnp
from jax import lax
from jax.experimental import pallas as pl
from jax.experimental.pallas import tpu as pltpu
from jax.sharding import PartitionSpec as P


OMEGA = 0.6
AXES = ("gx", "gy")
F32 = jnp.float32
BF16 = jnp.bfloat16
ROW, NEAR, POS2, POS3, LIST_0, OWN_LAB, SIDE_LAB, BACK, TAB = 0, 8, 16, 24, 32, 40, 72, 88, 96
LANES = 128
BELOW, ABOVE = 0, 1
ROW_CHUNK = 128


def exchanged(value, first):
    count = lax.axis_size(AXES)
    pairs = []
    for low in range(first, count + first, 2):
        high = (low + 1) % count
        pairs += [(low, high), (high, low)]
    return lax.ppermute(value, AXES, pairs)


def pair_side():
    return 1 - lax.rem(lax.axis_index("gy"), 2)


def split(x):
    high = x.astype(BF16)
    return high, (x - high.astype(F32)).astype(BF16)


def dot(a, b):
    return jnp.dot(a, b, preferred_element_type=F32)


def dot3(a_high, a_low, b_high, b_low):
    return dot(a_high, b_high) + dot(a_low, b_high) + dot(a_high, b_low)


def dot3k(a_high, a_low, b_high, b_low):
    both = jnp.concatenate([a_high, a_low], axis=1)
    return dot(both, jnp.concatenate([b_high, b_high], axis=0)) + dot(a_high, b_low)


def note(tab, i, value):
    tab[pl.ds(i, 1), :] = jnp.full((1, tab.shape[1]), value, jnp.int32)


def entry(tab, i):
    return tab[pl.ds(i, 1), :][0, 0]


def far_partner():
    return lax.axis_index("gy") == 0


def load_kernel(
    devices, cols_hbm, agg_hbm, t_hbm, dinv_hbm, a_hbm,
    tab, t_0, t_1, t, near_0, near_1, own, a_high, a_low, a01_high, a01_low,
    cols, agg, rank, dinv, a, sem,
):
    early = [
        pltpu.make_async_copy(dinv_hbm, dinv, sem.at[5]),
        pltpu.make_async_copy(a_hbm, a, sem.at[6]),
    ]

    rows, width = t.shape[0], t.shape[0] // 2
    device = lax.axis_index("gx") * lax.axis_size("gy") + lax.axis_index("gy")
    previous = lax.rem(device + devices - 1, devices)
    following = lax.rem(device + 1, devices)
    slabs = previous, following, device
    side = pair_side()
    shift = ROW_CHUNK.bit_length() - 1
    chunk = 4 * ROW_CHUNK
    copies = [
        pltpu.make_async_copy(
            cols_hbm.at[pl.ds(pl.multiple_of(((slab * rows) >> shift) * chunk, chunk), chunk)],
            cols.at[pl.ds(i * chunk, chunk)],
            sem.at[i],
        )
        for i, slab in enumerate(slabs)
    ]
    copies += [pltpu.make_async_copy(t_hbm, t, sem.at[3]), pltpu.make_async_copy(agg_hbm, agg, sem.at[4])]
    for copy in copies:
        copy.start()

    def col(i, r, k):
        return cols[i * chunk + k * ROW_CHUNK + ((slabs[i] * rows) & (ROW_CHUNK - 1)) + r]

    def rank_rows(i, k, where):
        mask = jnp.int32(0)
        for r in range(rows):
            mask = mask | (jnp.int32(1) << (col(i, r, k) & (rows - 1)))
        named, other = jnp.int32(0), jnp.int32(width)
        for r in range(rows):
            hit = (mask >> r) & 1
            place = jnp.where(hit == 1, named, other)
            rank[where * rows + r] = place
            rank[(where + 1) * rows + place] = r
            named = named + hit
            other = other + 1 - hit

    def ranked(where, r):
        return rank[where * rows + r]

    copies[0].wait()
    copies[1].wait()
    rank_rows(0, 3, 0)
    rank_rows(1, 2, 2)
    sent_1, sent_0 = jnp.where(side == ABOVE, 0, 2), jnp.where(side == ABOVE, 2, 0)
    copies[3].wait()
    for j in range(width):
        t_1[j] = t[ranked(sent_1 + 1, j)]
        t_0[j] = t[ranked(sent_0 + 1, j)]
    copies[2].wait()
    copies[4].wait()
    rank_rows(2, 2, 4)
    rank_rows(2, 3, 6)
    for j in range(width):
        note(tab, LIST_0 + j, ranked(sent_1, ranked(sent_0 + 1, j)))
        for which in (BELOW, ABOVE):
            note(tab, BACK + width * which + j, col(which, ranked(5 + 2 * which, j), 3 - which) & (rows - 1))
            for k in range(2):
                note(tab, SIDE_LAB + 8 * which + 2 * j + k, agg[col(which, ranked(5 + 2 * which, j), 2 + k)])
    for u in range(rows):
        row = ranked(sent_1 + 1, u)
        note(tab, ROW + u, row)
        note(tab, NEAR + u, ranked(sent_1, col(2, row, 1) & (rows - 1)))
        note(tab, POS2 + u, ranked(4, col(2, row, 2) & (rows - 1)))
        note(tab, POS3 + u, ranked(6, col(2, row, 3) & (rows - 1)))
        for k in range(4):
            note(tab, OWN_LAB + 4 * u + k, agg[col(2, row, k)])

    @pl.when(far_partner())
    def _():
        for copy in early:
            copy.start()
        for copy in early:
            copy.wait()
        near_blocks(tab, a, t, dinv, near_0, near_1, own, a_high, a_low, a01_high, a01_low)


def put(value, label, column):
    return jnp.where(label == column, value, jnp.zeros_like(value))


def two_columns(value, label):
    return jnp.concatenate([put(value, label, 0), put(value, label, 1)], axis=1)


def near_tiles(tab, a, t, dinv, order):
    block = t.shape[1]
    rows = [entry(tab, ROW + u) for u in order]
    prods = []
    for u, row in zip(order, rows):
        near = entry(tab, ROW + entry(tab, NEAR + u))
        prods.append(
            jnp.concatenate(
                [dot3k(*split(a[row, 0]), *split(t[row])), dot3k(*split(a[row, 1]), *split(t[near]))], axis=1
            )
        )
    tiles = []
    for u, row, prod in zip(order, rows, prods):
        smoothed = dot3k(*split(dinv[row]), *split(prod))
        p0 = t[row] - OMEGA * smoothed[:, :block]
        p1 = -OMEGA * smoothed[:, block:]
        tiles.append(two_columns(p0, entry(tab, OWN_LAB + 4 * u)) + two_columns(p1, entry(tab, OWN_LAB + 4 * u + 1)))
    return tiles


def wide(ref, *places):
    return jnp.concatenate([ref[place] for place in places], axis=0)


def near_blocks(tab, a, t, dinv, near_0, near_1, own, a_high, a_low, a01_high, a01_low):
    rows, width = own.shape[0], near_1.shape[0]
    for u, value in enumerate(near_tiles(tab, a, t, dinv, range(rows))):
        own[u] = value
        if u < width:
            near_1[u] = value
    for j in range(width):
        near_0[j] = own[entry(tab, LIST_0 + j)]
    for u in range(rows):
        row = entry(tab, ROW + u)
        a01_high[u], a01_low[u] = split(jnp.concatenate([a[row, 0], a[row, 1]], axis=1))
        for which in (BELOW, ABOVE):
            a_high[which, u], a_low[which, u] = split(a[row, 2 + which])


def near_kernel(tab, a, t, dinv, *refs):
    pl.when(jnp.logical_not(far_partner()))(lambda: near_blocks(tab, a, t, dinv, *refs[7:]))


def far_blocks(tab, a_high, a_low, dinv, t_high, t_low, order):
    prods = [
        jnp.concatenate(
            [
                dot3k(a_high[which, u], a_low[which, u], t_high[which, pos], t_low[which, pos])
                for which, pos in ((BELOW, entry(tab, POS2 + u)), (ABOVE, entry(tab, POS3 + u)))
            ],
            axis=1,
        )
        for u in order
    ]
    return [-OMEGA * dot3k(*split(dinv[entry(tab, ROW + u)]), *split(prod)) for u, prod in zip(order, prods)]


def split_rows(value, high, low):
    for j in range(value.shape[0]):
        high[j], low[j] = split(value[j])


def far_sent_kernel(tab, a_high, a_low, dinv, t_0, far_1, t_high, t_low):
    side = pair_side()
    block = dinv.shape[1]
    split_rows(t_0, t_high, t_low)
    order = range(far_1.shape[0])
    prods = []
    for u in order:
        pos = entry(tab, POS2 + 8 * side + u)
        high, low = split(dot3k(a_high[side, u], a_low[side, u], t_high[pos], t_low[pos]))
        prods.append(
            (jnp.concatenate([high, a_high[1 - side, u]], axis=1), jnp.concatenate([low, a_low[1 - side, u]], axis=1))
        )
    for u in order:
        both = -OMEGA * dot3k(*split(dinv[entry(tab, ROW + u)]), *prods[u])
        far_1[u, side] = both[:, :block]
        far_1[u, 1 - side] = both[:, block:]


def store_turned(trans, label, place, value):
    block = value.shape[0]
    trans[pl.ds(pl.multiple_of(label * block, block), block), place] = value.T
    trans[pl.ds(pl.multiple_of((1 - label) * block, block), block), place] = jnp.zeros_like(value)


def turn(tab, far, side, trans_high, trans_low):
    for u in range(far.shape[0]):
        block = far.shape[2]
        label = entry(tab, OWN_LAB + 4 * u + 2 + side)
        high, low = split(far[u, side])
        place = slice(u * block, (u + 1) * block)
        store_turned(trans_high, label, place, high)
        store_turned(trans_low, label, place, low)


def coarse_group(trans_high, trans_low, ap_high, ap_low):
    return dot3(trans_high[...], trans_low[...], ap_high[...], ap_low[...])


def far_kernel(tab, a_high, a_low, dinv, t0_high, t0_low, t_1, far_1, far_0, far, t_high, t_low):
    rows, block = far.shape[0], far.shape[2]
    width = rows // 2
    side = pair_side()
    for j in range(width):
        t_high[side, j], t_low[side, j] = t0_high[j], t0_low[j]
        t_high[1 - side, j], t_low[1 - side, j] = split(t_1[j])
    for u in range(width):
        pos = entry(tab, POS2 + 8 * (1 - side) + u)
        far[u, side] = far_1[u, side]
        far[u, 1 - side] = dot3k(*split(far_1[u, 1 - side]), t_high[1 - side, pos], t_low[1 - side, pos])
    for u, both in enumerate(far_blocks(tab, a_high, a_low, dinv, t_high, t_low, range(width, rows))):
        far[width + u, BELOW] = both[:, :block]
        far[width + u, ABOVE] = both[:, block:]
    for j in range(width):
        far_0[j] = far[entry(tab, LIST_0 + j)]


def mid_kernel(
    tab, a01_high, a01_low, a_high, a_low, far, near_0,
    trans_high, trans_low, part, ap_high, ap_low, group,
    far_high, far_low, p_high, p_low,
):
    rows, block = far.shape[0], far.shape[2]
    side = pair_side()
    split_rows(near_0, p_high, p_low)
    for u in range(rows):
        for which in (BELOW, ABOVE):
            label = entry(tab, OWN_LAB + 4 * u + 2 + which)
            high, low = split(far[u, which])
            far_high[which, u] = two_columns(high, label)
            far_low[which, u] = two_columns(low, label)

    def mine(u, which):
        near = entry(tab, NEAR + u)
        return dot3(a01_high[u], a01_low[u], wide(far_high.at[which], u, near), wide(far_low.at[which], u, near))

    totals = []
    for u in range(rows):
        pos = entry(tab, POS2 + 8 * side + u)
        totals.append(mine(u, side) + dot3k(a_high[side, u], a_low[side, u], p_high[pos], p_low[pos]))
    for u in range(rows):
        place = slice(u * block, (u + 1) * block)
        ap_high[place], ap_low[place] = split(totals[u])
    turn(tab, far, 1 - side, trans_high, trans_low)
    for u in range(rows):
        part[u] = mine(u, 1 - side)
    group[...] = coarse_group(trans_high, trans_low, ap_high, ap_low)


def first_kernel(
    tab, a_high, a_low, part, trans_high, trans_low, near_1,
    ap_high, ap_low, out_1,
    p_high, p_low,
):
    rows, block = part.shape[0], part.shape[1]
    side = 1 - pair_side()
    split_rows(near_1, p_high, p_low)
    totals = []
    for u in range(rows):
        pos = entry(tab, POS2 + 8 * side + u)
        totals.append(part[u] + dot3k(a_high[side, u], a_low[side, u], p_high[pos], p_low[pos]))
    for u in range(rows):
        place = slice(u * block, (u + 1) * block)
        ap_high[place], ap_low[place] = split(totals[u])
    out_1[...] = coarse_group(trans_high, trans_low, ap_high, ap_low)


def far_columns(tab, side, a_high, a_low, p_high, p_low, ap_high, ap_low):
    rows, block = a_high.shape[1], a_high.shape[3]
    values, here = [], []
    for u in range(rows):
        pos = entry(tab, POS2 + 8 * side + u)
        values.append(dot3k(a_high[side, u], a_low[side, u], p_high[pos], p_low[pos]))
    for u in range(rows):
        labels = SIDE_LAB + 8 * side + 2 * entry(tab, POS2 + 8 * side + u)
        here.append(two_columns(values[u][:, :block], entry(tab, labels + 1 - side)))
        high, low = split(values[u][:, block:])
        label = entry(tab, labels + side)
        place = slice(u * block, (u + 1) * block)
        ap_high[place] = two_columns(high, label)
        ap_low[place] = two_columns(low, label)
    return here


def same_kernel(
    tab, a_high, a_low, trans_high, trans_low, far_0, group,
    own_part, ap_high, ap_low, out_1,
    p_high, p_low,
):
    half = trans_high.shape[0]
    block = half // 2
    side = pair_side()
    out_1[:, :half] = group[...]
    for j in range(far_0.shape[0]):
        p_high[j, :, :block], p_low[j, :, :block] = split(far_0[j, 1 - side])
        p_high[j, :, block:], p_low[j, :, block:] = split(far_0[j, side])
    here = far_columns(tab, side, a_high, a_low, p_high, p_low, ap_high, ap_low)
    for u, value in enumerate(here):
        own_part[u] = value
    out_1[:, half:] = coarse_group(trans_high, trans_low, ap_high, ap_low)


def own_part_kernel(tab, a01_high, a01_low, own, t, so_far, own_part, back_high, back_low, own_high, own_low):
    rows = own.shape[0]
    side = 1 - pair_side()
    for j in range(rows // 2):
        back_high[j], back_low[j] = split(t[entry(tab, BACK + (rows // 2) * side + j)])
    for u in range(rows):
        own_high[u], own_low[u] = split(own[u])
    for u in range(rows):
        near = entry(tab, NEAR + u)
        own_part[u] = so_far[u] + dot3(a01_high[u], a01_low[u], wide(own_high, u, near), wide(own_low, u, near))


def second_kernel(
    tab, a_high, a_low, own_part, back_high, back_low, trans_high, trans_low, far_1,
    own_high, own_low, ap_high, ap_low, out_1,
    p_high, p_low,
):
    rows, block = own_part.shape[0], own_part.shape[1]
    half = 2 * block
    side = 1 - pair_side()
    towards = [dot3k(*split(far_1[j, 1 - side]), back_high[j], back_low[j]) for j in range(rows // 2)]
    for j in range(rows // 2):
        p_high[j, :, :block], p_low[j, :, :block] = split(towards[j])
        p_high[j, :, block:], p_low[j, :, block:] = split(far_1[j, side])
    here = far_columns(tab, side, a_high, a_low, p_high, p_low, ap_high, ap_low)
    for u in range(rows):
        place = slice(u * block, (u + 1) * block)
        own_high[place], own_low[place] = split(own_part[u] + here[u])
    out_1[:, :half] = coarse_group(trans_high, trans_low, own_high, own_low)
    out_1[:, half:] = coarse_group(trans_high, trans_low, ap_high, ap_low)


def every_group(trans_high, trans_low, aps, out):
    half = trans_high.shape[0]
    for i in range(len(aps) // 2):
        out[:, i * half : (i + 1) * half] = coarse_group(trans_high, trans_low, aps[2 * i], aps[2 * i + 1])


def other_kernel(tab, far, *refs):
    aps, (out_0, trans_high, trans_low) = refs[:10], refs[10:]
    turn(tab, far, pair_side(), trans_high, trans_low)
    every_group(trans_high, trans_low, aps, out_0)


def own_kernel(own, *refs):
    aps, (out, trans_high, trans_low) = refs[:10], refs[10:]
    rows, block = own.shape[0], own.shape[1]
    for u in range(rows):
        place = slice(u * block, (u + 1) * block)
        high, low = split(own[u])
        trans_high[:, place] = high.T
        trans_low[:, place] = low.T
    every_group(trans_high, trans_low, aps, out)


def write_slots(inverse, totals, results, out, sems):
    block = inverse.shape[1]
    inv = [split(inverse[agg]) for agg in range(2)]
    values = [dot3k(*inv[agg], *split(total)) for agg, _, total in totals]
    copies = []
    for n, ((agg, d, _), value) in enumerate(zip(totals, values)):
        results[n, 0] = value[:, :block]
        results[n, 1] = value[:, block:]
        copies.append(pltpu.make_async_copy(results.at[n], out.at[agg, pl.ds(2 * (d + 3), 2)], sems.at[n]))
        copies[-1].start()
    for copy in copies:
        copy.wait()


OWN_AT, SAME_AT = (1, -1, 2, 0, -2), (0, 2, -1, 1, 3)
PARTS_AT = (-2, -3), (-1, 1), (0,)


def finish_kernel(offsets, part_at, inverse, own, *refs):
    refs, (out, results, sems) = refs[:-3], refs[-3:]
    others = ((refs[0], SAME_AT), (refs[1], part_at)) if len(refs) > 1 else ((refs[0], part_at),)
    block = inverse.shape[1]
    half = 2 * block
    side = pair_side()

    def run(way):
        done = []
        for agg in range(2):
            line = slice(agg * block, (agg + 1) * block)
            for d in offsets:
                places = [(ref, at.index(d)) for ref, at in ((own, OWN_AT), *others) if d in at]
                shares = [ref[line, i * half : (i + 1) * half] for ref, i in places]
                done.append((agg, way * d, sum(shares[1:], shares[0])))
        write_slots(inverse, done, results, out, sems)

    pl.when(side == ABOVE)(lambda: run(1))
    pl.when(side == BELOW)(lambda: run(-1))


VMEM = pl.BlockSpec(memory_space=pltpu.VMEM)
HBM = pl.BlockSpec(memory_space=pltpu.HBM)


def call(body, outs, ins, scratch=(), micros=1.0, in_hbm=(), out_hbm=(), aliases={}):
    def specs(values, in_place):
        return [HBM if i in in_place else VMEM for i, x in enumerate(values)]

    return pl.pallas_call(
        body,
        out_shape=outs,
        in_specs=specs(ins, in_hbm),
        out_specs=specs(outs, out_hbm),
        scratch_shapes=[pltpu.VMEM(*x) if isinstance(x, tuple) else x for x in scratch],
        input_output_aliases=aliases,
        compiler_params=pltpu.CompilerParams(vmem_limit_bytes=24 * 2**20),
        cost_estimate=pl.CostEstimate(flops=int(micros * 1e9), bytes_accessed=2**20, transcendentals=0),
    )(*ins)


def shards(a, a_cols, t_blocks, t_agg, dinv, coarse_inv):
    devices = lax.axis_size(AXES)
    rows, block = t_blocks.shape[:2]
    width, half, deep = rows // 2, 2 * block, rows * block
    shape = jax.ShapeDtypeStruct
    full = lambda *dims: shape(dims, F32)
    pair = lambda *dims: [shape(dims, BF16), shape(dims, BF16)]
    two = lambda *dims: [(dims, BF16)] * 2
    tile = full(width, block, half)
    cols = a_cols.reshape(-1, ROW_CHUNK, 4).transpose(0, 2, 1).reshape(-1)

    near_shapes = [tile, tile, full(rows, block, half)] + pair(2, rows, block, block) + pair(rows, block, half)
    tab, t_0, t_1, t, *near = call(
        functools.partial(load_kernel, devices),
        [shape((TAB, LANES), jnp.int32)] + [full(width, block, block)] * 2 + [full(*t_blocks.shape)] + near_shapes,
        [pltpu.with_memory_space_constraint(x, pltpu.HBM) for x in (cols, t_agg, t_blocks, dinv, a)],
        [
            pltpu.SMEM((3 * 4 * ROW_CHUNK,), jnp.int32),
            pltpu.SMEM(t_agg.shape, jnp.int32),
            pltpu.SMEM((8 * rows,), jnp.int32),
            (dinv.shape, F32),
            (a.shape, F32),
            pltpu.SemaphoreType.DMA((7,)),
        ],
        micros=3,
        in_hbm=(0, 1, 2, 3, 4),
    )
    t_0 = exchanged(t_0, 0)
    t_1 = exchanged(t_1, 1)
    near_0, near_1, own, a23_high, a23_low, a01_high, a01_low = call(
        near_kernel, near_shapes, [tab, a, t, dinv, *near], micros=2, aliases={4 + i: i for i in range(7)}
    )
    near_0 = exchanged(near_0, 0)
    sent = full(width, 2, block, block)
    far_1, t0_high, t0_low = call(
        far_sent_kernel, [sent] + pair(width, block, block), [tab, a23_high, a23_low, dinv, t_0], micros=2
    )
    got_far_1 = exchanged(far_1, 1)
    near_1 = exchanged(near_1, 1)
    far_0, far = call(
        far_kernel,
        [sent, full(rows, 2, block, block)],
        [tab, a23_high, a23_low, dinv, t0_high, t0_low, t_1, far_1],
        two(2, width, block, block),
        micros=1,
    )
    far_0, far_1 = exchanged(far_0, 0), got_far_1
    out_high, out_low, part, ap_e1_high, ap_e1_low, group = call(
        mid_kernel,
        pair(half, deep) + [full(rows, block, half)] + pair(deep, half) + [full(half, half)],
        [tab, a01_high, a01_low, a23_high, a23_low, far, near_0],
        two(2, rows, block, half) + two(width, block, half),
        micros=2,
    )
    part_own, ap_e2_high, ap_e2_low, part_1 = call(
        same_kernel,
        [full(rows, block, half)] + pair(deep, half) + [full(half, 2 * half)],
        [tab, a23_high, a23_low, out_high, out_low, far_0, group],
        two(width, block, half),
        micros=1,
    )
    part_1 = exchanged(part_1, 1)
    part_own, back_high, back_low = call(
        own_part_kernel,
        [full(rows, block, half)] + pair(width, block, block),
        [tab, a01_high, a01_low, own, t, part_own],
        two(rows, block, half),
        micros=1,
    )
    ap_own_high, ap_own_low, ap_o2_high, ap_o2_low, part_2 = call(
        second_kernel,
        pair(deep, half) * 2 + [full(half, 2 * half)],
        [tab, a23_high, a23_low, part_own, back_high, back_low, out_high, out_low, far_1],
        two(width, block, half),
        micros=2,
    )
    part_2 = exchanged(part_2, 1)
    ap_o1_high, ap_o1_low, part_3 = call(
        first_kernel,
        pair(deep, half) + [full(half, half)],
        [tab, a23_high, a23_low, part, out_high, out_low, near_1],
        two(width, block, half),
        micros=2,
    )
    part_3 = exchanged(part_3, 1)
    aps = [
        ap_e1_high, ap_e1_low, ap_o1_high, ap_o1_low, ap_e2_high, ap_e2_low,
        ap_own_high, ap_own_low, ap_o2_high, ap_o2_low,
    ]
    (both_0,) = call(other_kernel, [full(half, 5 * half)], [tab, far] + aps, two(half, deep), micros=2)
    both_0 = exchanged(both_0, 0)
    (total,) = call(own_kernel, [full(half, 5 * half)], [own] + aps, two(half, deep), micros=2)
    out = []
    for i, (offsets, got) in enumerate((((-3, -2), part_1), ((-1, 1, 2, 3), part_2), ((0,), part_3))):
        n = 2 * len(offsets)
        out = call(
            functools.partial(finish_kernel, offsets, PARTS_AT[i]),
            [full(2, 14, block, block)],
            [coarse_inv, total] + ([both_0] if i else []) + [got, *out],
            [((n, 2, block, block), F32), pltpu.SemaphoreType.DMA((n,))],
            micros=1,
            in_hbm=(4,),
            out_hbm=(0,),
            aliases={4: 0} if i else {},
        )
    return out[0]


def solution(mesh):
    placed = (
        P(AXES, None, None, None),
        P(),
        P(AXES, None, None),
        P(),
        P(AXES, None, None),
        P(AXES, None, None),
    )
    return jax.shard_map(
        shards,
        mesh=mesh,
        in_specs=placed,
        out_specs=P(AXES, None, None, None),
        check_vma=False,
    )
```

```python
import functools

import jax
import jax.numpy as jnp
from jax import lax
from jax.experimental import pallas as pl
from jax.experimental.pallas import tpu as pltpu
from jax.sharding import PartitionSpec as P


OMEGA = 0.6
AXES = ("gx", "gy")
F32 = jnp.float32
BF16 = jnp.bfloat16
ROW, NEAR, POS2, POS3, LIST_0, OWN_LAB, SIDE_LAB, BACK, TAB = 0, 8, 16, 24, 32, 40, 72, 88, 96
LANES = 128
BELOW, ABOVE = 0, 1
ROW_CHUNK = 128


def exchanged(value, first):
    count = lax.axis_size(AXES)
    pairs = []
    for low in range(first, count + first, 2):
        high = (low + 1) % count
        pairs += [(low, high), (high, low)]
    return lax.ppermute(value, AXES, pairs)


def pair_side():
    return 1 - lax.rem(lax.axis_index("gy"), 2)


def split(x):
    high = x.astype(BF16)
    return high, (x - high.astype(F32)).astype(BF16)


def dot(a, b):
    return jnp.dot(a, b, preferred_element_type=F32)


def dot3(a_high, a_low, b_high, b_low):
    return dot(a_high, b_high) + dot(a_low, b_high) + dot(a_high, b_low)


def dot3k(a_high, a_low, b_high, b_low):
    both = jnp.concatenate([a_high, a_low], axis=1)
    return dot(both, jnp.concatenate([b_high, b_high], axis=0)) + dot(a_high, b_low)


def note(tab, i, value):
    tab[pl.ds(i, 1), :] = jnp.full((1, tab.shape[1]), value, jnp.int32)


def entry(tab, i):
    return tab[pl.ds(i, 1), :][0, 0]


def far_partner():
    return lax.axis_index("gy") == 0


def load_kernel(
    devices, cols_hbm, agg_hbm, t_hbm, dinv_hbm, a_hbm,
    tab, t_0, t_1, t, near_0, near_1, own, a_high, a_low, a01_high, a01_low,
    cols, agg, rank, dinv, a, sem,
):
    early = [
        pltpu.make_async_copy(dinv_hbm, dinv, sem.at[5]),
        pltpu.make_async_copy(a_hbm, a, sem.at[6]),
    ]

    rows, width = t.shape[0], t.shape[0] // 2
    device = lax.axis_index("gx") * lax.axis_size("gy") + lax.axis_index("gy")
    previous = lax.rem(device + devices - 1, devices)
    following = lax.rem(device + 1, devices)
    slabs = previous, following, device
    side = pair_side()
    shift = ROW_CHUNK.bit_length() - 1
    chunk = 4 * ROW_CHUNK
    copies = [
        pltpu.make_async_copy(
            cols_hbm.at[pl.ds(pl.multiple_of(((slab * rows) >> shift) * chunk, chunk), chunk)],
            cols.at[pl.ds(i * chunk, chunk)],
            sem.at[i],
        )
        for i, slab in enumerate(slabs)
    ]
    copies += [pltpu.make_async_copy(t_hbm, t, sem.at[3]), pltpu.make_async_copy(agg_hbm, agg, sem.at[4])]
    for i, copy in enumerate(copies):
        copy.start(priority=1 if i == 3 else 0)

    def col(i, r, k):
        return cols[i * chunk + k * ROW_CHUNK + ((slabs[i] * rows) & (ROW_CHUNK - 1)) + r]

    def rank_rows(i, k, where):
        mask = jnp.int32(0)
        for r in range(rows):
            mask = mask | (jnp.int32(1) << (col(i, r, k) & (rows - 1)))
        named, other = jnp.int32(0), jnp.int32(width)
        for r in range(rows):
            hit = (mask >> r) & 1
            place = jnp.where(hit == 1, named, other)
            rank[where * rows + r] = place
            rank[(where + 1) * rows + place] = r
            named = named + hit
            other = other + 1 - hit

    def ranked(where, r):
        return rank[where * rows + r]

    copies[0].wait()
    copies[1].wait()
    rank_rows(0, 3, 0)
    rank_rows(1, 2, 2)
    sent_1, sent_0 = jnp.where(side == ABOVE, 0, 2), jnp.where(side == ABOVE, 2, 0)
    copies[3].wait()
    for j in range(width):
        t_1[j] = t[ranked(sent_1 + 1, j)]
        t_0[j] = t[ranked(sent_0 + 1, j)]
    copies[2].wait()
    copies[4].wait()
    rank_rows(2, 2, 4)
    rank_rows(2, 3, 6)
    for j in range(width):
        note(tab, LIST_0 + j, ranked(sent_1, ranked(sent_0 + 1, j)))
        for which in (BELOW, ABOVE):
            note(tab, BACK + width * which + j, col(which, ranked(5 + 2 * which, j), 3 - which) & (rows - 1))
            for k in range(2):
                note(tab, SIDE_LAB + 8 * which + 2 * j + k, agg[col(which, ranked(5 + 2 * which, j), 2 + k)])
    for u in range(rows):
        row = ranked(sent_1 + 1, u)
        note(tab, ROW + u, row)
        note(tab, NEAR + u, ranked(sent_1, col(2, row, 1) & (rows - 1)))
        note(tab, POS2 + u, ranked(4, col(2, row, 2) & (rows - 1)))
        note(tab, POS3 + u, ranked(6, col(2, row, 3) & (rows - 1)))
        for k in range(4):
            note(tab, OWN_LAB + 4 * u + k, agg[col(2, row, k)])

    @pl.when(far_partner())
    def _():
        for copy in early:
            copy.start()
        for copy in early:
            copy.wait()
        near_blocks(tab, a, t, dinv, near_0, near_1, own, a_high, a_low, a01_high, a01_low)


def put(value, label, column):
    return jnp.where(label == column, value, jnp.zeros_like(value))


def two_columns(value, label):
    return jnp.concatenate([put(value, label, 0), put(value, label, 1)], axis=1)


def near_tiles(tab, a, t, dinv, order):
    block = t.shape[1]
    rows = [entry(tab, ROW + u) for u in order]
    prods = []
    for u, row in zip(order, rows):
        near = entry(tab, ROW + entry(tab, NEAR + u))
        prods.append(
            jnp.concatenate(
                [dot3k(*split(a[row, 0]), *split(t[row])), dot3k(*split(a[row, 1]), *split(t[near]))], axis=1
            )
        )
    tiles = []
    for u, row, prod in zip(order, rows, prods):
        smoothed = dot3k(*split(dinv[row]), *split(prod))
        p0 = t[row] - OMEGA * smoothed[:, :block]
        p1 = -OMEGA * smoothed[:, block:]
        tiles.append(two_columns(p0, entry(tab, OWN_LAB + 4 * u)) + two_columns(p1, entry(tab, OWN_LAB + 4 * u + 1)))
    return tiles


def wide(ref, *places):
    return jnp.concatenate([ref[place] for place in places], axis=0)


def near_blocks(tab, a, t, dinv, near_0, near_1, own, a_high, a_low, a01_high, a01_low):
    rows, width = own.shape[0], near_1.shape[0]
    for u, value in enumerate(near_tiles(tab, a, t, dinv, range(rows))):
        own[u] = value
        if u < width:
            near_1[u] = value
    for j in range(width):
        near_0[j] = own[entry(tab, LIST_0 + j)]
    for u in range(rows):
        row = entry(tab, ROW + u)
        a01_high[u], a01_low[u] = split(jnp.concatenate([a[row, 0], a[row, 1]], axis=1))
        for which in (BELOW, ABOVE):
            a_high[which, u], a_low[which, u] = split(a[row, 2 + which])


def near_kernel(tab, a, t, dinv, *refs):
    pl.when(jnp.logical_not(far_partner()))(lambda: near_blocks(tab, a, t, dinv, *refs[7:]))


def far_blocks(tab, a_high, a_low, dinv, t_high, t_low, order):
    prods = [
        jnp.concatenate(
            [
                dot3k(a_high[which, u], a_low[which, u], t_high[which, pos], t_low[which, pos])
                for which, pos in ((BELOW, entry(tab, POS2 + u)), (ABOVE, entry(tab, POS3 + u)))
            ],
            axis=1,
        )
        for u in order
    ]
    return [-OMEGA * dot3k(*split(dinv[entry(tab, ROW + u)]), *split(prod)) for u, prod in zip(order, prods)]


def split_rows(value, high, low):
    for j in range(value.shape[0]):
        high[j], low[j] = split(value[j])


def far_sent_kernel(tab, a_high, a_low, dinv, t_0, far_1, t_high, t_low):
    side = pair_side()
    block = dinv.shape[1]
    split_rows(t_0, t_high, t_low)
    order = range(far_1.shape[0])
    prods = []
    for u in order:
        pos = entry(tab, POS2 + 8 * side + u)
        high, low = split(dot3k(a_high[side, u], a_low[side, u], t_high[pos], t_low[pos]))
        prods.append(
            (jnp.concatenate([high, a_high[1 - side, u]], axis=1), jnp.concatenate([low, a_low[1 - side, u]], axis=1))
        )
    for u in order:
        both = -OMEGA * dot3k(*split(dinv[entry(tab, ROW + u)]), *prods[u])
        far_1[u, side] = both[:, :block]
        far_1[u, 1 - side] = both[:, block:]


def store_turned(trans, label, place, value):
    block = value.shape[0]
    trans[pl.ds(pl.multiple_of(label * block, block), block), place] = value.T
    trans[pl.ds(pl.multiple_of((1 - label) * block, block), block), place] = jnp.zeros_like(value)


def turn(tab, far, side, trans_high, trans_low):
    for u in range(far.shape[0]):
        block = far.shape[2]
        label = entry(tab, OWN_LAB + 4 * u + 2 + side)
        high, low = split(far[u, side])
        place = slice(u * block, (u + 1) * block)
        store_turned(trans_high, label, place, high)
        store_turned(trans_low, label, place, low)


def coarse_group(trans_high, trans_low, ap_high, ap_low):
    return dot3(trans_high[...], trans_low[...], ap_high[...], ap_low[...])


def far_kernel(tab, a_high, a_low, dinv, t0_high, t0_low, t_1, far_1, far_0, far, t_high, t_low):
    rows, block = far.shape[0], far.shape[2]
    width = rows // 2
    side = pair_side()
    for j in range(width):
        t_high[side, j], t_low[side, j] = t0_high[j], t0_low[j]
        t_high[1 - side, j], t_low[1 - side, j] = split(t_1[j])
    for u in range(width):
        pos = entry(tab, POS2 + 8 * (1 - side) + u)
        far[u, side] = far_1[u, side]
        far[u, 1 - side] = dot3k(*split(far_1[u, 1 - side]), t_high[1 - side, pos], t_low[1 - side, pos])
    for u, both in enumerate(far_blocks(tab, a_high, a_low, dinv, t_high, t_low, range(width, rows))):
        far[width + u, BELOW] = both[:, :block]
        far[width + u, ABOVE] = both[:, block:]
    for j in range(width):
        far_0[j] = far[entry(tab, LIST_0 + j)]


def mid_kernel(
    tab, a01_high, a01_low, a_high, a_low, far, near_0,
    trans_high, trans_low, part, ap_high, ap_low, group,
    far_high, far_low, p_high, p_low,
):
    rows, block = far.shape[0], far.shape[2]
    side = pair_side()
    split_rows(near_0, p_high, p_low)
    for u in range(rows):
        for which in (BELOW, ABOVE):
            label = entry(tab, OWN_LAB + 4 * u + 2 + which)
            high, low = split(far[u, which])
            far_high[which, u] = two_columns(high, label)
            far_low[which, u] = two_columns(low, label)

    def mine(u, which):
        near = entry(tab, NEAR + u)
        return dot3(a01_high[u], a01_low[u], wide(far_high.at[which], u, near), wide(far_low.at[which], u, near))

    totals = []
    for u in range(rows):
        pos = entry(tab, POS2 + 8 * side + u)
        totals.append(mine(u, side) + dot3k(a_high[side, u], a_low[side, u], p_high[pos], p_low[pos]))
    for u in range(rows):
        place = slice(u * block, (u + 1) * block)
        ap_high[place], ap_low[place] = split(totals[u])
    turn(tab, far, 1 - side, trans_high, trans_low)
    for u in range(rows):
        part[u] = mine(u, 1 - side)
    group[...] = coarse_group(trans_high, trans_low, ap_high, ap_low)


def first_kernel(
    tab, a_high, a_low, part, trans_high, trans_low, near_1,
    ap_high, ap_low, out_1,
    p_high, p_low,
):
    rows, block = part.shape[0], part.shape[1]
    side = 1 - pair_side()
    split_rows(near_1, p_high, p_low)
    totals = []
    for u in range(rows):
        pos = entry(tab, POS2 + 8 * side + u)
        totals.append(part[u] + dot3k(a_high[side, u], a_low[side, u], p_high[pos], p_low[pos]))
    for u in range(rows):
        place = slice(u * block, (u + 1) * block)
        ap_high[place], ap_low[place] = split(totals[u])
    out_1[...] = coarse_group(trans_high, trans_low, ap_high, ap_low)


def far_columns(tab, side, a_high, a_low, p_high, p_low, ap_high, ap_low):
    rows, block = a_high.shape[1], a_high.shape[3]
    values, here = [], []
    for u in range(rows):
        pos = entry(tab, POS2 + 8 * side + u)
        values.append(dot3k(a_high[side, u], a_low[side, u], p_high[pos], p_low[pos]))
    for u in range(rows):
        labels = SIDE_LAB + 8 * side + 2 * entry(tab, POS2 + 8 * side + u)
        here.append(two_columns(values[u][:, :block], entry(tab, labels + 1 - side)))
        high, low = split(values[u][:, block:])
        label = entry(tab, labels + side)
        place = slice(u * block, (u + 1) * block)
        ap_high[place] = two_columns(high, label)
        ap_low[place] = two_columns(low, label)
    return here


def same_kernel(
    tab, a_high, a_low, trans_high, trans_low, far_0, group,
    own_part, ap_high, ap_low, out_1,
    p_high, p_low,
):
    half = trans_high.shape[0]
    block = half // 2
    side = pair_side()
    out_1[:, :half] = group[...]
    for j in range(far_0.shape[0]):
        p_high[j, :, :block], p_low[j, :, :block] = split(far_0[j, 1 - side])
        p_high[j, :, block:], p_low[j, :, block:] = split(far_0[j, side])
    here = far_columns(tab, side, a_high, a_low, p_high, p_low, ap_high, ap_low)
    for u, value in enumerate(here):
        own_part[u] = value
    out_1[:, half:] = coarse_group(trans_high, trans_low, ap_high, ap_low)


def own_part_kernel(early, tab, a01_high, a01_low, own, t, *refs):
    own_part, back_high, back_low, own_high, own_low = refs[-5:]
    rows = own.shape[0]
    side = 1 - pair_side()

    @pl.when(far_partner() == early)
    def _():
        for j in range(rows // 2):
            back_high[j], back_low[j] = split(t[entry(tab, BACK + (rows // 2) * side + j)])
        for u in range(rows):
            own_high[u], own_low[u] = split(own[u])
        for u in range(rows):
            near = entry(tab, NEAR + u)
            own_part[u] = dot3(a01_high[u], a01_low[u], wide(own_high, u, near), wide(own_low, u, near))


def second_kernel(
    tab, a_high, a_low, own_part, so_far, back_high, back_low, trans_high, trans_low, far_1,
    own_high, own_low, ap_high, ap_low, out_1,
    p_high, p_low,
):
    rows, block = own_part.shape[0], own_part.shape[1]
    half = 2 * block
    side = 1 - pair_side()
    towards = [dot3k(*split(far_1[j, 1 - side]), back_high[j], back_low[j]) for j in range(rows // 2)]
    for j in range(rows // 2):
        p_high[j, :, :block], p_low[j, :, :block] = split(towards[j])
        p_high[j, :, block:], p_low[j, :, block:] = split(far_1[j, side])
    here = far_columns(tab, side, a_high, a_low, p_high, p_low, ap_high, ap_low)
    for u in range(rows):
        place = slice(u * block, (u + 1) * block)
        own_high[place], own_low[place] = split(own_part[u] + so_far[u] + here[u])
    out_1[:, :half] = coarse_group(trans_high, trans_low, own_high, own_low)
    out_1[:, half:] = coarse_group(trans_high, trans_low, ap_high, ap_low)


def every_group(trans_high, trans_low, aps, out):
    half = trans_high.shape[0]
    for i in range(len(aps) // 2):
        out[:, i * half : (i + 1) * half] = coarse_group(trans_high, trans_low, aps[2 * i], aps[2 * i + 1])


def other_kernel(tab, far, *refs):
    aps, (out_0, trans_high, trans_low) = refs[:10], refs[10:]
    turn(tab, far, pair_side(), trans_high, trans_low)
    every_group(trans_high, trans_low, aps, out_0)


def own_kernel(early, own, *refs):
    aps, (out, trans_high, trans_low) = refs[:10], refs[-3:]
    rows, block = own.shape[0], own.shape[1]

    @pl.when(far_partner() != early)
    def _():
        for u in range(rows):
            place = slice(u * block, (u + 1) * block)
            high, low = split(own[u])
            trans_high[:, place] = high.T
            trans_low[:, place] = low.T
        every_group(trans_high, trans_low, aps, out)


def write_slots(inverse, totals, results, out, sems):
    block = inverse.shape[1]
    inv = [split(inverse[agg]) for agg in range(2)]
    values = [dot3k(*inv[agg], *split(total)) for agg, _, total in totals]
    copies = []
    for n, ((agg, d, _), value) in enumerate(zip(totals, values)):
        results[n, 0] = value[:, :block]
        results[n, 1] = value[:, block:]
        copies.append(pltpu.make_async_copy(results.at[n], out.at[agg, pl.ds(2 * (d + 3), 2)], sems.at[n]))
        copies[-1].start()
    for copy in copies:
        copy.wait()


OWN_AT, SAME_AT = (1, -1, 2, 0, -2), (0, 2, -1, 1, 3)
PARTS_AT = (-2, -3), (-1, 1), (0,)


def finish_kernel(offsets, part_at, inverse, own, *refs):
    refs, (out, results, sems) = refs[:-3], refs[-3:]
    others = ((refs[0], SAME_AT), (refs[1], part_at)) if len(refs) > 1 else ((refs[0], part_at),)
    block = inverse.shape[1]
    half = 2 * block
    side = pair_side()

    def run(way):
        done = []
        for agg in range(2):
            line = slice(agg * block, (agg + 1) * block)
            for d in offsets:
                places = [(ref, at.index(d)) for ref, at in ((own, OWN_AT), *others) if d in at]
                shares = [ref[line, i * half : (i + 1) * half] for ref, i in places]
                done.append((agg, way * d, sum(shares[1:], shares[0])))
        write_slots(inverse, done, results, out, sems)

    pl.when(side == ABOVE)(lambda: run(1))
    pl.when(side == BELOW)(lambda: run(-1))


VMEM = pl.BlockSpec(memory_space=pltpu.VMEM)
HBM = pl.BlockSpec(memory_space=pltpu.HBM)


def call(body, outs, ins, scratch=(), micros=1.0, in_hbm=(), out_hbm=(), aliases={}):
    def specs(values, in_place):
        return [HBM if i in in_place else VMEM for i, x in enumerate(values)]

    return pl.pallas_call(
        body,
        out_shape=outs,
        in_specs=specs(ins, in_hbm),
        out_specs=specs(outs, out_hbm),
        scratch_shapes=[pltpu.VMEM(*x) if isinstance(x, tuple) else x for x in scratch],
        input_output_aliases=aliases,
        compiler_params=pltpu.CompilerParams(vmem_limit_bytes=24 * 2**20),
        cost_estimate=pl.CostEstimate(flops=int(micros * 1e9), bytes_accessed=2**20, transcendentals=0),
    )(*ins)


def shards(a, a_cols, t_blocks, t_agg, dinv, coarse_inv):
    devices = lax.axis_size(AXES)
    rows, block = t_blocks.shape[:2]
    width, half, deep = rows // 2, 2 * block, rows * block
    shape = jax.ShapeDtypeStruct
    full = lambda *dims: shape(dims, F32)
    pair = lambda *dims: [shape(dims, BF16), shape(dims, BF16)]
    two = lambda *dims: [(dims, BF16)] * 2
    tile = full(width, block, half)
    cols = a_cols.reshape(-1, ROW_CHUNK, 4).transpose(0, 2, 1).reshape(-1)

    near_shapes = [tile, tile, full(rows, block, half)] + pair(2, rows, block, block) + pair(rows, block, half)
    tab, t_0, t_1, t, *near = call(
        functools.partial(load_kernel, devices),
        [shape((TAB, LANES), jnp.int32)] + [full(width, block, block)] * 2 + [full(*t_blocks.shape)] + near_shapes,
        [pltpu.with_memory_space_constraint(x, pltpu.HBM) for x in (cols, t_agg, t_blocks, dinv, a)],
        [
            pltpu.SMEM((3 * 4 * ROW_CHUNK,), jnp.int32),
            pltpu.SMEM(t_agg.shape, jnp.int32),
            pltpu.SMEM((8 * rows,), jnp.int32),
            (dinv.shape, F32),
            (a.shape, F32),
            pltpu.SemaphoreType.DMA((7,)),
        ],
        micros=3,
        in_hbm=(0, 1, 2, 3, 4),
    )
    t_0 = exchanged(t_0, 0)
    t_1 = exchanged(t_1, 1)
    near_0, near_1, own, a23_high, a23_low, a01_high, a01_low = call(
        near_kernel, near_shapes, [tab, a, t, dinv, *near], micros=2, aliases={4 + i: i for i in range(7)}
    )
    near_0 = exchanged(near_0, 0)
    sent = full(width, 2, block, block)
    far_1, t0_high, t0_low = call(
        far_sent_kernel, [sent] + pair(width, block, block), [tab, a23_high, a23_low, dinv, t_0], micros=2
    )
    got_far_1 = exchanged(far_1, 1)

    def own_share(early, done):
        return call(
            functools.partial(own_part_kernel, early),
            [full(rows, block, half)] + pair(width, block, block),
            [tab, a01_high, a01_low, own, t, *done],
            two(rows, block, half),
            micros=1,
            aliases={5 + i: i for i in range(len(done))},
        )

    share = own_share(True, [])
    near_1 = exchanged(near_1, 1)
    far_0, far = call(
        far_kernel,
        [sent, full(rows, 2, block, block)],
        [tab, a23_high, a23_low, dinv, t0_high, t0_low, t_1, far_1],
        two(2, width, block, block),
        micros=1,
    )
    far_0, far_1 = exchanged(far_0, 0), got_far_1
    out_high, out_low, part, ap_e1_high, ap_e1_low, group = call(
        mid_kernel,
        pair(half, deep) + [full(rows, block, half)] + pair(deep, half) + [full(half, half)],
        [tab, a01_high, a01_low, a23_high, a23_low, far, near_0],
        two(2, rows, block, half) + two(width, block, half),
        micros=2,
    )
    part_own, ap_e2_high, ap_e2_low, part_1 = call(
        same_kernel,
        [full(rows, block, half)] + pair(deep, half) + [full(half, 2 * half)],
        [tab, a23_high, a23_low, out_high, out_low, far_0, group],
        two(width, block, half),
        micros=1,
    )
    part_1 = exchanged(part_1, 1)
    share_own, back_high, back_low = own_share(False, share)
    ap_own_high, ap_own_low, ap_o2_high, ap_o2_low, part_2 = call(
        second_kernel,
        pair(deep, half) * 2 + [full(half, 2 * half)],
        [tab, a23_high, a23_low, share_own, part_own, back_high, back_low, out_high, out_low, far_1],
        two(width, block, half),
        micros=2,
    )
    part_2 = exchanged(part_2, 1)
    ap_o1_high, ap_o1_low, part_3 = call(
        first_kernel,
        pair(deep, half) + [full(half, half)],
        [tab, a23_high, a23_low, part, out_high, out_low, near_1],
        two(width, block, half),
        micros=2,
    )
    part_3 = exchanged(part_3, 1)
    aps = [
        ap_e1_high, ap_e1_low, ap_o1_high, ap_o1_low, ap_e2_high, ap_e2_low,
        ap_own_high, ap_own_low, ap_o2_high, ap_o2_low,
    ]
    (both_0,) = call(other_kernel, [full(half, 5 * half)], [tab, far] + aps, two(half, deep), micros=2)
    total = []
    for early in (True, False):
        total = call(
            functools.partial(own_kernel, early),
            [full(half, 5 * half)],
            [own] + aps + total,
            two(half, deep),
            micros=2,
            aliases={11: 0} if total else {},
        )
        total = list(total)
        if early:
            both_0 = exchanged(both_0, 0)
    (total,) = total
    out = []
    for i, (offsets, got) in enumerate((((-3, -2), part_1), ((-1, 1, 2, 3), part_2), ((0,), part_3))):
        n = 2 * len(offsets)
        out = call(
            functools.partial(finish_kernel, offsets, PARTS_AT[i]),
            [full(2, 14, block, block)],
            [coarse_inv, total] + ([both_0] if i else []) + [got, *out],
            [((n, 2, block, block), F32), pltpu.SemaphoreType.DMA((n,))],
            micros=1,
            in_hbm=(4,),
            out_hbm=(0,),
            aliases={4: 0} if i else {},
        )
    return out[0]


def solution(mesh):
    placed = (
        P(AXES, None, None, None),
        P(),
        P(AXES, None, None),
        P(),
        P(AXES, None, None),
        P(AXES, None, None),
    )
    return jax.shard_map(
        shards,
        mesh=mesh,
        in_specs=placed,
        out_specs=P(AXES, None, None, None),
        check_vma=False,
    )
```

```python
import functools

import jax
import jax.numpy as jnp
from jax import lax
from jax.experimental import pallas as pl
from jax.experimental.pallas import tpu as pltpu
from jax.sharding import PartitionSpec as P


OMEGA = 0.6
AXES = ("gx", "gy")
F32 = jnp.float32
BF16 = jnp.bfloat16
ROW, NEAR, POS2, POS3, LIST_0, OWN_LAB, SIDE_LAB, BACK, TAB = 0, 8, 16, 24, 32, 40, 72, 88, 96
LANES = 128
BELOW, ABOVE = 0, 1
ROW_CHUNK = 128


def exchanged(value, first):
    count = lax.axis_size(AXES)
    pairs = []
    for low in range(first, count + first, 2):
        high = (low + 1) % count
        pairs += [(low, high), (high, low)]
    return lax.ppermute(value, AXES, pairs)


def pair_side():
    return 1 - lax.rem(lax.axis_index("gy"), 2)


def split(x):
    high = x.astype(BF16)
    return high, (x - high.astype(F32)).astype(BF16)


def dot(a, b):
    return jnp.dot(a, b, preferred_element_type=F32)


def dot3(a_high, a_low, b_high, b_low):
    return dot(a_high, b_high) + dot(a_low, b_high) + dot(a_high, b_low)


def dot3k(a_high, a_low, b_high, b_low):
    both = jnp.concatenate([a_high, a_low], axis=1)
    return dot(both, jnp.concatenate([b_high, b_high], axis=0)) + dot(a_high, b_low)


def note(tab, i, value):
    tab[pl.ds(i, 1), :] = jnp.full((1, tab.shape[1]), value, jnp.int32)


def entry(tab, i):
    return tab[pl.ds(i, 1), :][0, 0]


def far_partner():
    return lax.axis_index("gy") == 0


def load_kernel(
    devices, cols_hbm, agg_hbm, t_hbm, dinv_hbm, a_hbm,
    tab, t_0, t_1, t, near_0, near_1, own, a_high, a_low, a01_high, a01_low,
    cols, agg, rank, dinv, a, sem,
):
    early = [
        pltpu.make_async_copy(dinv_hbm, dinv, sem.at[5]),
        pltpu.make_async_copy(a_hbm, a, sem.at[6]),
    ]

    rows, width = t.shape[0], t.shape[0] // 2
    device = lax.axis_index("gx") * lax.axis_size("gy") + lax.axis_index("gy")
    previous = lax.rem(device + devices - 1, devices)
    following = lax.rem(device + 1, devices)
    slabs = previous, following, device
    side = pair_side()
    shift = ROW_CHUNK.bit_length() - 1
    chunk = 4 * ROW_CHUNK
    at_1 = [(slab * rows) >> shift for slab in slabs[:2]]
    at_2 = [(lax.rem(device + step, devices) * rows) >> shift for step in (devices - 2, 2)]
    copies = [
        pltpu.make_async_copy(
            cols_hbm.at[pl.ds(pl.multiple_of(at_1[i] * chunk, chunk), chunk)], cols.at[pl.ds(i * chunk, chunk)], sem.at[i]
        )
        for i in range(2)
    ]
    copies += [pltpu.make_async_copy(t_hbm, t, sem.at[2])]
    copies += [
        pltpu.make_async_copy(
            agg_hbm.at[pl.ds(pl.multiple_of(at_2[i] * ROW_CHUNK, ROW_CHUNK), ROW_CHUNK)],
            agg.at[pl.ds(i * ROW_CHUNK, ROW_CHUNK)],
            sem.at[3 + i],
        )
        for i in range(2)
    ]
    for copy in copies:
        copy.start()
    own_at = jnp.where((device * rows) >> shift == at_1[0], 0, 1)
    starts = [
        held * chunk + ((slab * rows) & (ROW_CHUNK - 1)) for held, slab in zip((0, 1, own_at), slabs)
    ]

    def col(i, r, k):
        return cols[starts[i] + k * ROW_CHUNK + r]

    def label_of(row):
        held = jnp.where(row >> shift == at_2[0], 0, ROW_CHUNK)
        return agg[held + (row & (ROW_CHUNK - 1))]

    def rank_rows(i, k, where):
        mask = jnp.int32(0)
        for r in range(rows):
            mask = mask | (jnp.int32(1) << (col(i, r, k) & (rows - 1)))
        named, other = jnp.int32(0), jnp.int32(width)
        for r in range(rows):
            hit = (mask >> r) & 1
            place = jnp.where(hit == 1, named, other)
            rank[where * rows + r] = place
            rank[(where + 1) * rows + place] = r
            named = named + hit
            other = other + 1 - hit

    def ranked(where, r):
        return rank[where * rows + r]

    copies[0].wait()
    copies[1].wait()
    rank_rows(0, 3, 0)
    rank_rows(1, 2, 2)
    sent_1, sent_0 = jnp.where(side == ABOVE, 0, 2), jnp.where(side == ABOVE, 2, 0)
    copies[2].wait()
    for j in range(width):
        t_1[j] = t[ranked(sent_1 + 1, j)]
        t_0[j] = t[ranked(sent_0 + 1, j)]
    copies[3].wait()
    copies[4].wait()
    rank_rows(2, 2, 4)
    rank_rows(2, 3, 6)
    for j in range(width):
        note(tab, LIST_0 + j, ranked(sent_1, ranked(sent_0 + 1, j)))
        for which in (BELOW, ABOVE):
            note(tab, BACK + width * which + j, col(which, ranked(5 + 2 * which, j), 3 - which) & (rows - 1))
            for k in range(2):
                note(tab, SIDE_LAB + 8 * which + 2 * j + k, label_of(col(which, ranked(5 + 2 * which, j), 2 + k)))
    for u in range(rows):
        row = ranked(sent_1 + 1, u)
        note(tab, ROW + u, row)
        note(tab, NEAR + u, ranked(sent_1, col(2, row, 1) & (rows - 1)))
        note(tab, POS2 + u, ranked(4, col(2, row, 2) & (rows - 1)))
        note(tab, POS3 + u, ranked(6, col(2, row, 3) & (rows - 1)))
        for k in range(4):
            note(tab, OWN_LAB + 4 * u + k, label_of(col(2, row, k)))

    @pl.when(far_partner())
    def _():
        for copy in early:
            copy.start()
        for copy in early:
            copy.wait()
        near_blocks(tab, a, t, dinv, near_0, near_1, own, a_high, a_low, a01_high, a01_low)


def put(value, label, column):
    return jnp.where(label == column, value, jnp.zeros_like(value))


def two_columns(value, label):
    return jnp.concatenate([put(value, label, 0), put(value, label, 1)], axis=1)


def near_tiles(tab, a, t, dinv, order):
    block = t.shape[1]
    rows = [entry(tab, ROW + u) for u in order]
    prods = []
    for u, row in zip(order, rows):
        near = entry(tab, ROW + entry(tab, NEAR + u))
        prods.append(
            jnp.concatenate(
                [dot3k(*split(a[row, 0]), *split(t[row])), dot3k(*split(a[row, 1]), *split(t[near]))], axis=1
            )
        )
    tiles = []
    for u, row, prod in zip(order, rows, prods):
        smoothed = dot3k(*split(dinv[row]), *split(prod))
        p0 = t[row] - OMEGA * smoothed[:, :block]
        p1 = -OMEGA * smoothed[:, block:]
        tiles.append(two_columns(p0, entry(tab, OWN_LAB + 4 * u)) + two_columns(p1, entry(tab, OWN_LAB + 4 * u + 1)))
    return tiles


def wide(ref, *places):
    return jnp.concatenate([ref[place] for place in places], axis=0)


def near_blocks(tab, a, t, dinv, near_0, near_1, own, a_high, a_low, a01_high, a01_low):
    rows, width = own.shape[0], near_1.shape[0]
    for u, value in enumerate(near_tiles(tab, a, t, dinv, range(rows))):
        own[u] = value
        if u < width:
            near_1[u] = value
    for j in range(width):
        near_0[j] = own[entry(tab, LIST_0 + j)]
    for u in range(rows):
        row = entry(tab, ROW + u)
        a01_high[u], a01_low[u] = split(jnp.concatenate([a[row, 0], a[row, 1]], axis=1))
        for which in (BELOW, ABOVE):
            a_high[which, u], a_low[which, u] = split(a[row, 2 + which])


def near_kernel(tab, a, t, dinv, *refs):
    pl.when(jnp.logical_not(far_partner()))(lambda: near_blocks(tab, a, t, dinv, *refs[7:]))


def far_blocks(tab, a_high, a_low, dinv, t_high, t_low, order):
    prods = [
        jnp.concatenate(
            [
                dot3k(a_high[which, u], a_low[which, u], t_high[which, pos], t_low[which, pos])
                for which, pos in ((BELOW, entry(tab, POS2 + u)), (ABOVE, entry(tab, POS3 + u)))
            ],
            axis=1,
        )
        for u in order
    ]
    return [-OMEGA * dot3k(*split(dinv[entry(tab, ROW + u)]), *split(prod)) for u, prod in zip(order, prods)]


def split_rows(value, high, low):
    for j in range(value.shape[0]):
        high[j], low[j] = split(value[j])


def far_sent_kernel(tab, a_high, a_low, dinv, t_0, far_1, t_high, t_low):
    side = pair_side()
    block = dinv.shape[1]
    split_rows(t_0, t_high, t_low)
    order = range(far_1.shape[0])
    prods = []
    for u in order:
        pos = entry(tab, POS2 + 8 * side + u)
        high, low = split(dot3k(a_high[side, u], a_low[side, u], t_high[pos], t_low[pos]))
        prods.append(
            (jnp.concatenate([high, a_high[1 - side, u]], axis=1), jnp.concatenate([low, a_low[1 - side, u]], axis=1))
        )
    for u in order:
        both = -OMEGA * dot3k(*split(dinv[entry(tab, ROW + u)]), *prods[u])
        far_1[u, side] = both[:, :block]
        far_1[u, 1 - side] = both[:, block:]


def store_turned(trans, label, place, value):
    block = value.shape[0]
    trans[pl.ds(pl.multiple_of(label * block, block), block), place] = value.T
    trans[pl.ds(pl.multiple_of((1 - label) * block, block), block), place] = jnp.zeros_like(value)


def turn(tab, far, side, trans_high, trans_low):
    for u in range(far.shape[0]):
        block = far.shape[2]
        label = entry(tab, OWN_LAB + 4 * u + 2 + side)
        high, low = split(far[u, side])
        place = slice(u * block, (u + 1) * block)
        store_turned(trans_high, label, place, high)
        store_turned(trans_low, label, place, low)


def coarse_group(trans_high, trans_low, ap_high, ap_low):
    return dot3(trans_high[...], trans_low[...], ap_high[...], ap_low[...])


def far_kernel(tab, a_high, a_low, dinv, t0_high, t0_low, t_1, far_1, far_0, far, t_high, t_low):
    rows, block = far.shape[0], far.shape[2]
    width = rows // 2
    side = pair_side()
    for j in range(width):
        t_high[side, j], t_low[side, j] = t0_high[j], t0_low[j]
        t_high[1 - side, j], t_low[1 - side, j] = split(t_1[j])
    for u in range(width):
        pos = entry(tab, POS2 + 8 * (1 - side) + u)
        far[u, side] = far_1[u, side]
        far[u, 1 - side] = dot3k(*split(far_1[u, 1 - side]), t_high[1 - side, pos], t_low[1 - side, pos])
    for u, both in enumerate(far_blocks(tab, a_high, a_low, dinv, t_high, t_low, range(width, rows))):
        far[width + u, BELOW] = both[:, :block]
        far[width + u, ABOVE] = both[:, block:]
    for j in range(width):
        far_0[j] = far[entry(tab, LIST_0 + j)]


def mid_kernel(
    tab, a01_high, a01_low, a_high, a_low, far, near_0,
    trans_high, trans_low, part, ap_high, ap_low, group,
    far_high, far_low, p_high, p_low,
):
    rows, block = far.shape[0], far.shape[2]
    side = pair_side()
    split_rows(near_0, p_high, p_low)
    for u in range(rows):
        for which in (BELOW, ABOVE):
            label = entry(tab, OWN_LAB + 4 * u + 2 + which)
            high, low = split(far[u, which])
            far_high[which, u] = two_columns(high, label)
            far_low[which, u] = two_columns(low, label)

    def mine(u, which):
        near = entry(tab, NEAR + u)
        return dot3(a01_high[u], a01_low[u], wide(far_high.at[which], u, near), wide(far_low.at[which], u, near))

    totals = []
    for u in range(rows):
        pos = entry(tab, POS2 + 8 * side + u)
        totals.append(mine(u, side) + dot3k(a_high[side, u], a_low[side, u], p_high[pos], p_low[pos]))
    for u in range(rows):
        place = slice(u * block, (u + 1) * block)
        ap_high[place], ap_low[place] = split(totals[u])
    turn(tab, far, 1 - side, trans_high, trans_low)
    for u in range(rows):
        part[u] = mine(u, 1 - side)
    group[...] = coarse_group(trans_high, trans_low, ap_high, ap_low)


def first_kernel(
    tab, a_high, a_low, part, trans_high, trans_low, near_1,
    ap_high, ap_low, out_1,
    p_high, p_low,
):
    rows, block = part.shape[0], part.shape[1]
    side = 1 - pair_side()
    split_rows(near_1, p_high, p_low)
    totals = []
    for u in range(rows):
        pos = entry(tab, POS2 + 8 * side + u)
        totals.append(part[u] + dot3k(a_high[side, u], a_low[side, u], p_high[pos], p_low[pos]))
    for u in range(rows):
        place = slice(u * block, (u + 1) * block)
        ap_high[place], ap_low[place] = split(totals[u])
    out_1[...] = coarse_group(trans_high, trans_low, ap_high, ap_low)


def far_columns(tab, side, a_high, a_low, p_high, p_low, ap_high, ap_low):
    rows, block = a_high.shape[1], a_high.shape[3]
    values, here = [], []
    for u in range(rows):
        pos = entry(tab, POS2 + 8 * side + u)
        values.append(dot3k(a_high[side, u], a_low[side, u], p_high[pos], p_low[pos]))
    for u in range(rows):
        labels = SIDE_LAB + 8 * side + 2 * entry(tab, POS2 + 8 * side + u)
        here.append(two_columns(values[u][:, :block], entry(tab, labels + 1 - side)))
        high, low = split(values[u][:, block:])
        label = entry(tab, labels + side)
        place = slice(u * block, (u + 1) * block)
        ap_high[place] = two_columns(high, label)
        ap_low[place] = two_columns(low, label)
    return here


def same_kernel(
    tab, a_high, a_low, trans_high, trans_low, far_0, group,
    own_part, ap_high, ap_low, out_1,
    p_high, p_low,
):
    half = trans_high.shape[0]
    block = half // 2
    side = pair_side()
    out_1[:, :half] = group[...]
    for j in range(far_0.shape[0]):
        p_high[j, :, :block], p_low[j, :, :block] = split(far_0[j, 1 - side])
        p_high[j, :, block:], p_low[j, :, block:] = split(far_0[j, side])
    here = far_columns(tab, side, a_high, a_low, p_high, p_low, ap_high, ap_low)
    for u, value in enumerate(here):
        own_part[u] = value
    out_1[:, half:] = coarse_group(trans_high, trans_low, ap_high, ap_low)


def own_part_kernel(early, tab, a01_high, a01_low, own, t, *refs):
    own_part, back_high, back_low, own_high, own_low = refs[-5:]
    rows = own.shape[0]
    side = 1 - pair_side()

    @pl.when(far_partner() == early)
    def _():
        for j in range(rows // 2):
            back_high[j], back_low[j] = split(t[entry(tab, BACK + (rows // 2) * side + j)])
        for u in range(rows):
            own_high[u], own_low[u] = split(own[u])
        for u in range(rows):
            near = entry(tab, NEAR + u)
            own_part[u] = dot3(a01_high[u], a01_low[u], wide(own_high, u, near), wide(own_low, u, near))


def second_kernel(
    tab, a_high, a_low, own_part, so_far, back_high, back_low, trans_high, trans_low, far_1,
    own_high, own_low, ap_high, ap_low, out_1,
    p_high, p_low,
):
    rows, block = own_part.shape[0], own_part.shape[1]
    half = 2 * block
    side = 1 - pair_side()
    towards = [dot3k(*split(far_1[j, 1 - side]), back_high[j], back_low[j]) for j in range(rows // 2)]
    for j in range(rows // 2):
        p_high[j, :, :block], p_low[j, :, :block] = split(towards[j])
        p_high[j, :, block:], p_low[j, :, block:] = split(far_1[j, side])
    here = far_columns(tab, side, a_high, a_low, p_high, p_low, ap_high, ap_low)
    for u in range(rows):
        place = slice(u * block, (u + 1) * block)
        own_high[place], own_low[place] = split(own_part[u] + so_far[u] + here[u])
    out_1[:, :half] = coarse_group(trans_high, trans_low, own_high, own_low)
    out_1[:, half:] = coarse_group(trans_high, trans_low, ap_high, ap_low)


def every_group(trans_high, trans_low, aps, out):
    half = trans_high.shape[0]
    for i in range(len(aps) // 2):
        out[:, i * half : (i + 1) * half] = coarse_group(trans_high, trans_low, aps[2 * i], aps[2 * i + 1])


def other_kernel(tab, far, *refs):
    aps, (out_0, trans_high, trans_low) = refs[:10], refs[10:]
    turn(tab, far, pair_side(), trans_high, trans_low)
    every_group(trans_high, trans_low, aps, out_0)


def own_kernel(early, own, *refs):
    aps, (out, trans_high, trans_low) = refs[:10], refs[-3:]
    rows, block = own.shape[0], own.shape[1]

    @pl.when(far_partner() != early)
    def _():
        for u in range(rows):
            place = slice(u * block, (u + 1) * block)
            high, low = split(own[u])
            trans_high[:, place] = high.T
            trans_low[:, place] = low.T
        every_group(trans_high, trans_low, aps, out)


def write_slots(inverse, totals, results, out, sems):
    block = inverse.shape[1]
    inv = [split(inverse[agg]) for agg in range(2)]
    values = [dot3k(*inv[agg], *split(total)) for agg, _, total in totals]
    copies = []
    for n, ((agg, d, _), value) in enumerate(zip(totals, values)):
        results[n, 0] = value[:, :block]
        results[n, 1] = value[:, block:]
        copies.append(pltpu.make_async_copy(results.at[n], out.at[agg, pl.ds(2 * (d + 3), 2)], sems.at[n]))
        copies[-1].start()
    for copy in copies:
        copy.wait()


OWN_AT, SAME_AT = (1, -1, 2, 0, -2), (0, 2, -1, 1, 3)
PARTS_AT = (-2, -3), (-1, 1), (0,)


def finish_kernel(offsets, part_at, inverse, own, *refs):
    refs, (out, results, sems) = refs[:-3], refs[-3:]
    others = ((refs[0], SAME_AT), (refs[1], part_at)) if len(refs) > 1 else ((refs[0], part_at),)
    block = inverse.shape[1]
    half = 2 * block
    side = pair_side()

    def run(way):
        done = []
        for agg in range(2):
            line = slice(agg * block, (agg + 1) * block)
            for d in offsets:
                places = [(ref, at.index(d)) for ref, at in ((own, OWN_AT), *others) if d in at]
                shares = [ref[line, i * half : (i + 1) * half] for ref, i in places]
                done.append((agg, way * d, sum(shares[1:], shares[0])))
        write_slots(inverse, done, results, out, sems)

    pl.when(side == ABOVE)(lambda: run(1))
    pl.when(side == BELOW)(lambda: run(-1))


VMEM = pl.BlockSpec(memory_space=pltpu.VMEM)
HBM = pl.BlockSpec(memory_space=pltpu.HBM)


def call(body, outs, ins, scratch=(), micros=1.0, in_hbm=(), out_hbm=(), aliases={}):
    def specs(values, in_place):
        return [HBM if i in in_place else VMEM for i, x in enumerate(values)]

    return pl.pallas_call(
        body,
        out_shape=outs,
        in_specs=specs(ins, in_hbm),
        out_specs=specs(outs, out_hbm),
        scratch_shapes=[pltpu.VMEM(*x) if isinstance(x, tuple) else x for x in scratch],
        input_output_aliases=aliases,
        compiler_params=pltpu.CompilerParams(vmem_limit_bytes=24 * 2**20),
        cost_estimate=pl.CostEstimate(flops=int(micros * 1e9), bytes_accessed=2**20, transcendentals=0),
    )(*ins)


def shards(a, a_cols, t_blocks, t_agg, dinv, coarse_inv):
    devices = lax.axis_size(AXES)
    rows, block = t_blocks.shape[:2]
    width, half, deep = rows // 2, 2 * block, rows * block
    shape = jax.ShapeDtypeStruct
    full = lambda *dims: shape(dims, F32)
    pair = lambda *dims: [shape(dims, BF16), shape(dims, BF16)]
    two = lambda *dims: [(dims, BF16)] * 2
    tile = full(width, block, half)
    cols = a_cols.reshape(-1, ROW_CHUNK, 4).transpose(0, 2, 1).reshape(-1)

    near_shapes = [tile, tile, full(rows, block, half)] + pair(2, rows, block, block) + pair(rows, block, half)
    tab, t_0, t_1, t, *near = call(
        functools.partial(load_kernel, devices),
        [shape((TAB, LANES), jnp.int32)] + [full(width, block, block)] * 2 + [full(*t_blocks.shape)] + near_shapes,
        [pltpu.with_memory_space_constraint(x, pltpu.HBM) for x in (cols, t_agg, t_blocks, dinv, a)],
        [
            pltpu.SMEM((2 * 4 * ROW_CHUNK,), jnp.int32),
            pltpu.SMEM((2 * ROW_CHUNK,), jnp.int32),
            pltpu.SMEM((8 * rows,), jnp.int32),
            (dinv.shape, F32),
            (a.shape, F32),
            pltpu.SemaphoreType.DMA((7,)),
        ],
        micros=3,
        in_hbm=(0, 1, 2, 3, 4),
    )
    t_0 = exchanged(t_0, 0)
    t_1 = exchanged(t_1, 1)
    near_0, near_1, own, a23_high, a23_low, a01_high, a01_low = call(
        near_kernel, near_shapes, [tab, a, t, dinv, *near], micros=2, aliases={4 + i: i for i in range(7)}
    )
    near_0 = exchanged(near_0, 0)
    sent = full(width, 2, block, block)
    far_1, t0_high, t0_low = call(
        far_sent_kernel, [sent] + pair(width, block, block), [tab, a23_high, a23_low, dinv, t_0], micros=2
    )
    got_far_1 = exchanged(far_1, 1)

    def own_share(early, done):
        return call(
            functools.partial(own_part_kernel, early),
            [full(rows, block, half)] + pair(width, block, block),
            [tab, a01_high, a01_low, own, t, *done],
            two(rows, block, half),
            micros=1,
            aliases={5 + i: i for i in range(len(done))},
        )

    share = own_share(True, [])
    near_1 = exchanged(near_1, 1)
    far_0, far = call(
        far_kernel,
        [sent, full(rows, 2, block, block)],
        [tab, a23_high, a23_low, dinv, t0_high, t0_low, t_1, far_1],
        two(2, width, block, block),
        micros=1,
    )
    far_0, far_1 = exchanged(far_0, 0), got_far_1
    out_high, out_low, part, ap_e1_high, ap_e1_low, group = call(
        mid_kernel,
        pair(half, deep) + [full(rows, block, half)] + pair(deep, half) + [full(half, half)],
        [tab, a01_high, a01_low, a23_high, a23_low, far, near_0],
        two(2, rows, block, half) + two(width, block, half),
        micros=2,
    )
    part_own, ap_e2_high, ap_e2_low, part_1 = call(
        same_kernel,
        [full(rows, block, half)] + pair(deep, half) + [full(half, 2 * half)],
        [tab, a23_high, a23_low, out_high, out_low, far_0, group],
        two(width, block, half),
        micros=1,
    )
    part_1 = exchanged(part_1, 1)
    share_own, back_high, back_low = own_share(False, share)
    ap_own_high, ap_own_low, ap_o2_high, ap_o2_low, part_2 = call(
        second_kernel,
        pair(deep, half) * 2 + [full(half, 2 * half)],
        [tab, a23_high, a23_low, share_own, part_own, back_high, back_low, out_high, out_low, far_1],
        two(width, block, half),
        micros=2,
    )
    part_2 = exchanged(part_2, 1)
    ap_o1_high, ap_o1_low, part_3 = call(
        first_kernel,
        pair(deep, half) + [full(half, half)],
        [tab, a23_high, a23_low, part, out_high, out_low, near_1],
        two(width, block, half),
        micros=2,
    )
    part_3 = exchanged(part_3, 1)
    aps = [
        ap_e1_high, ap_e1_low, ap_o1_high, ap_o1_low, ap_e2_high, ap_e2_low,
        ap_own_high, ap_own_low, ap_o2_high, ap_o2_low,
    ]
    (both_0,) = call(other_kernel, [full(half, 5 * half)], [tab, far] + aps, two(half, deep), micros=2)
    total = []
    for early in (True, False):
        total = call(
            functools.partial(own_kernel, early),
            [full(half, 5 * half)],
            [own] + aps + total,
            two(half, deep),
            micros=2,
            aliases={11: 0} if total else {},
        )
        total = list(total)
        if early:
            both_0 = exchanged(both_0, 0)
    (total,) = total
    out = []
    for i, (offsets, got) in enumerate((((-3, -2), part_1), ((-1, 1, 2, 3), part_2), ((0,), part_3))):
        n = 2 * len(offsets)
        out = call(
            functools.partial(finish_kernel, offsets, PARTS_AT[i]),
            [full(2, 14, block, block)],
            [coarse_inv, total] + ([both_0] if i else []) + [got, *out],
            [((n, 2, block, block), F32), pltpu.SemaphoreType.DMA((n,))],
            micros=1,
            in_hbm=(4,),
            out_hbm=(0,),
            aliases={4: 0} if i else {},
        )
    return out[0]


def solution(mesh):
    placed = (
        P(AXES, None, None, None),
        P(),
        P(AXES, None, None),
        P(),
        P(AXES, None, None),
        P(AXES, None, None),
    )
    return jax.shard_map(
        shards,
        mesh=mesh,
        in_specs=placed,
        out_specs=P(AXES, None, None, None),
        check_vma=False,
    )
```

```python
import functools

import jax
import jax.numpy as jnp
from jax import lax
from jax.experimental import pallas as pl
from jax.experimental.pallas import tpu as pltpu
from jax.sharding import PartitionSpec as P


OMEGA = 0.6
AXES = ("gx", "gy")
F32 = jnp.float32
BF16 = jnp.bfloat16
ROW, NEAR, POS2, POS3, LIST_0, OWN_LAB, SIDE_LAB, BACK, TAB = 0, 8, 16, 24, 32, 40, 72, 88, 96
LANES = 128
BELOW, ABOVE = 0, 1
ROW_CHUNK = 128


def exchanged(value, first):
    count = lax.axis_size(AXES)
    pairs = []
    for low in range(first, count + first, 2):
        high = (low + 1) % count
        pairs += [(low, high), (high, low)]
    return lax.ppermute(value, AXES, pairs)


def pair_side():
    return 1 - lax.rem(lax.axis_index("gy"), 2)


def split(x):
    high = x.astype(BF16)
    return high, (x - high.astype(F32)).astype(BF16)


def dot(a, b):
    return jnp.dot(a, b, preferred_element_type=F32)


def dot3(a_high, a_low, b_high, b_low):
    return dot(a_high, b_high) + dot(a_low, b_high) + dot(a_high, b_low)


def dot3k(a_high, a_low, b_high, b_low):
    both = jnp.concatenate([a_high, a_low], axis=1)
    return dot(both, jnp.concatenate([b_high, b_high], axis=0)) + dot(a_high, b_low)


def note(tab, i, value):
    tab[pl.ds(i, 1), :] = jnp.full((1, tab.shape[1]), value, jnp.int32)


def entry(tab, i):
    return tab[pl.ds(i, 1), :][0, 0]


def far_partner():
    return lax.axis_index("gy") == 0


def load_kernel(
    devices, cols_hbm, agg_hbm, t_hbm, dinv_hbm, a_hbm,
    tab, t_0, t_1, t, near_0, near_1, own, a_high, a_low, a01_high, a01_low,
    cols, agg, rank, dinv, a, sem,
):
    early = [
        pltpu.make_async_copy(dinv_hbm, dinv, sem.at[4]),
        pltpu.make_async_copy(a_hbm, a, sem.at[5]),
    ]

    rows, width = t.shape[0], t.shape[0] // 2
    device = lax.axis_index("gx") * lax.axis_size("gy") + lax.axis_index("gy")
    previous = lax.rem(device + devices - 1, devices)
    following = lax.rem(device + 1, devices)
    slabs = previous, following, device
    side = pair_side()
    shift = ROW_CHUNK.bit_length() - 1
    chunk = 4 * ROW_CHUNK
    copies = [
        pltpu.make_async_copy(
            cols_hbm.at[pl.ds(pl.multiple_of(((slab * rows) >> shift) * chunk, chunk), chunk)],
            cols.at[pl.ds(i * chunk, chunk)],
            sem.at[i],
        )
        for i, slab in enumerate(slabs)
    ]
    t_rows = [pltpu.make_async_copy(t_hbm.at[r], t.at[r], sem.at[6 + r]) for r in range(rows)]
    copies.append(pltpu.make_async_copy(agg_hbm, agg, sem.at[3]))
    for copy in copies[:2] + t_rows + copies[2:]:
        copy.start()

    def col(i, r, k):
        return cols[i * chunk + k * ROW_CHUNK + ((slabs[i] * rows) & (ROW_CHUNK - 1)) + r]

    def rank_rows(i, k, where):
        mask = jnp.int32(0)
        for r in range(rows):
            mask = mask | (jnp.int32(1) << (col(i, r, k) & (rows - 1)))
        named, other = jnp.int32(0), jnp.int32(width)
        for r in range(rows):
            hit = (mask >> r) & 1
            place = jnp.where(hit == 1, named, other)
            rank[where * rows + r] = place
            rank[(where + 1) * rows + place] = r
            named = named + hit
            other = other + 1 - hit

    def ranked(where, r):
        return rank[where * rows + r]

    copies[0].wait()
    copies[1].wait()
    rank_rows(0, 3, 0)
    rank_rows(1, 2, 2)
    sent_1, sent_0 = jnp.where(side == ABOVE, 0, 2), jnp.where(side == ABOVE, 2, 0)
    for copy in t_rows:
        copy.wait()
    for j in range(width):
        t_1[j] = t[ranked(sent_1 + 1, j)]
        t_0[j] = t[ranked(sent_0 + 1, j)]
    copies[2].wait()
    copies[3].wait()
    rank_rows(2, 2, 4)
    rank_rows(2, 3, 6)
    for j in range(width):
        note(tab, LIST_0 + j, ranked(sent_1, ranked(sent_0 + 1, j)))
        for which in (BELOW, ABOVE):
            note(tab, BACK + width * which + j, col(which, ranked(5 + 2 * which, j), 3 - which) & (rows - 1))
            for k in range(2):
                note(tab, SIDE_LAB + 8 * which + 2 * j + k, agg[col(which, ranked(5 + 2 * which, j), 2 + k)])
    for u in range(rows):
        row = ranked(sent_1 + 1, u)
        note(tab, ROW + u, row)
        note(tab, NEAR + u, ranked(sent_1, col(2, row, 1) & (rows - 1)))
        note(tab, POS2 + u, ranked(4, col(2, row, 2) & (rows - 1)))
        note(tab, POS3 + u, ranked(6, col(2, row, 3) & (rows - 1)))
        for k in range(4):
            note(tab, OWN_LAB + 4 * u + k, agg[col(2, row, k)])

    @pl.when(far_partner())
    def _():
        for copy in early:
            copy.start()
        for copy in early:
            copy.wait()
        near_blocks(tab, a, t, dinv, near_0, near_1, own, a_high, a_low, a01_high, a01_low)


def put(value, label, column):
    return jnp.where(label == column, value, jnp.zeros_like(value))


def two_columns(value, label):
    return jnp.concatenate([put(value, label, 0), put(value, label, 1)], axis=1)


def near_tiles(tab, a, t, dinv, order):
    block = t.shape[1]
    rows = [entry(tab, ROW + u) for u in order]
    prods = []
    for u, row in zip(order, rows):
        near = entry(tab, ROW + entry(tab, NEAR + u))
        prods.append(
            jnp.concatenate(
                [dot3k(*split(a[row, 0]), *split(t[row])), dot3k(*split(a[row, 1]), *split(t[near]))], axis=1
            )
        )
    tiles = []
    for u, row, prod in zip(order, rows, prods):
        smoothed = dot3k(*split(dinv[row]), *split(prod))
        p0 = t[row] - OMEGA * smoothed[:, :block]
        p1 = -OMEGA * smoothed[:, block:]
        tiles.append(two_columns(p0, entry(tab, OWN_LAB + 4 * u)) + two_columns(p1, entry(tab, OWN_LAB + 4 * u + 1)))
    return tiles


def wide(ref, *places):
    return jnp.concatenate([ref[place] for place in places], axis=0)


def near_blocks(tab, a, t, dinv, near_0, near_1, own, a_high, a_low, a01_high, a01_low):
    rows, width = own.shape[0], near_1.shape[0]
    for u, value in enumerate(near_tiles(tab, a, t, dinv, range(rows))):
        own[u] = value
        if u < width:
            near_1[u] = value
    for j in range(width):
        near_0[j] = own[entry(tab, LIST_0 + j)]
    for u in range(rows):
        row = entry(tab, ROW + u)
        a01_high[u], a01_low[u] = split(jnp.concatenate([a[row, 0], a[row, 1]], axis=1))
        for which in (BELOW, ABOVE):
            a_high[which, u], a_low[which, u] = split(a[row, 2 + which])


def near_kernel(tab, a, t, dinv, *refs):
    pl.when(jnp.logical_not(far_partner()))(lambda: near_blocks(tab, a, t, dinv, *refs[7:]))


def far_blocks(tab, a_high, a_low, dinv, t_high, t_low, order):
    prods = [
        jnp.concatenate(
            [
                dot3k(a_high[which, u], a_low[which, u], t_high[which, pos], t_low[which, pos])
                for which, pos in ((BELOW, entry(tab, POS2 + u)), (ABOVE, entry(tab, POS3 + u)))
            ],
            axis=1,
        )
        for u in order
    ]
    return [-OMEGA * dot3k(*split(dinv[entry(tab, ROW + u)]), *split(prod)) for u, prod in zip(order, prods)]


def split_rows(value, high, low):
    for j in range(value.shape[0]):
        high[j], low[j] = split(value[j])


def far_sent_kernel(tab, a_high, a_low, dinv, t_0, far_1, t_high, t_low):
    side = pair_side()
    block = dinv.shape[1]
    split_rows(t_0, t_high, t_low)
    order = range(far_1.shape[0])
    prods = []
    for u in order:
        pos = entry(tab, POS2 + 8 * side + u)
        high, low = split(dot3k(a_high[side, u], a_low[side, u], t_high[pos], t_low[pos]))
        prods.append(
            (jnp.concatenate([high, a_high[1 - side, u]], axis=1), jnp.concatenate([low, a_low[1 - side, u]], axis=1))
        )
    for u in order:
        both = -OMEGA * dot3k(*split(dinv[entry(tab, ROW + u)]), *prods[u])
        far_1[u, side] = both[:, :block]
        far_1[u, 1 - side] = both[:, block:]


def store_turned(trans, label, place, value):
    block = value.shape[0]
    trans[pl.ds(pl.multiple_of(label * block, block), block), place] = value.T
    trans[pl.ds(pl.multiple_of((1 - label) * block, block), block), place] = jnp.zeros_like(value)


def turn(tab, far, side, trans_high, trans_low):
    for u in range(far.shape[0]):
        block = far.shape[2]
        label = entry(tab, OWN_LAB + 4 * u + 2 + side)
        high, low = split(far[u, side])
        place = slice(u * block, (u + 1) * block)
        store_turned(trans_high, label, place, high)
        store_turned(trans_low, label, place, low)


def coarse_group(trans_high, trans_low, ap_high, ap_low):
    return dot3(trans_high[...], trans_low[...], ap_high[...], ap_low[...])


def far_kernel(tab, a_high, a_low, dinv, t0_high, t0_low, t_1, far_1, far_0, far, t_high, t_low):
    rows, block = far.shape[0], far.shape[2]
    width = rows // 2
    side = pair_side()
    for j in range(width):
        t_high[side, j], t_low[side, j] = t0_high[j], t0_low[j]
        t_high[1 - side, j], t_low[1 - side, j] = split(t_1[j])
    for u in range(width):
        pos = entry(tab, POS2 + 8 * (1 - side) + u)
        far[u, side] = far_1[u, side]
        far[u, 1 - side] = dot3k(*split(far_1[u, 1 - side]), t_high[1 - side, pos], t_low[1 - side, pos])
    for u, both in enumerate(far_blocks(tab, a_high, a_low, dinv, t_high, t_low, range(width, rows))):
        far[width + u, BELOW] = both[:, :block]
        far[width + u, ABOVE] = both[:, block:]
    for j in range(width):
        far_0[j] = far[entry(tab, LIST_0 + j)]


def mid_kernel(
    tab, a01_high, a01_low, a_high, a_low, far, near_0,
    trans_high, trans_low, part, ap_high, ap_low, group,
    far_high, far_low, p_high, p_low,
):
    rows, block = far.shape[0], far.shape[2]
    side = pair_side()
    split_rows(near_0, p_high, p_low)
    for u in range(rows):
        for which in (BELOW, ABOVE):
            label = entry(tab, OWN_LAB + 4 * u + 2 + which)
            high, low = split(far[u, which])
            far_high[which, u] = two_columns(high, label)
            far_low[which, u] = two_columns(low, label)

    def mine(u, which):
        near = entry(tab, NEAR + u)
        return dot3(a01_high[u], a01_low[u], wide(far_high.at[which], u, near), wide(far_low.at[which], u, near))

    totals = []
    for u in range(rows):
        pos = entry(tab, POS2 + 8 * side + u)
        totals.append(mine(u, side) + dot3k(a_high[side, u], a_low[side, u], p_high[pos], p_low[pos]))
    for u in range(rows):
        place = slice(u * block, (u + 1) * block)
        ap_high[place], ap_low[place] = split(totals[u])
    turn(tab, far, 1 - side, trans_high, trans_low)
    for u in range(rows):
        part[u] = mine(u, 1 - side)
    group[...] = coarse_group(trans_high, trans_low, ap_high, ap_low)


def first_kernel(
    tab, a_high, a_low, part, trans_high, trans_low, near_1,
    ap_high, ap_low, out_1,
    p_high, p_low,
):
    rows, block = part.shape[0], part.shape[1]
    side = 1 - pair_side()
    split_rows(near_1, p_high, p_low)
    totals = []
    for u in range(rows):
        pos = entry(tab, POS2 + 8 * side + u)
        totals.append(part[u] + dot3k(a_high[side, u], a_low[side, u], p_high[pos], p_low[pos]))
    for u in range(rows):
        place = slice(u * block, (u + 1) * block)
        ap_high[place], ap_low[place] = split(totals[u])
    out_1[...] = coarse_group(trans_high, trans_low, ap_high, ap_low)


def far_columns(tab, side, a_high, a_low, p_high, p_low, ap_high, ap_low):
    rows, block = a_high.shape[1], a_high.shape[3]
    values, here = [], []
    for u in range(rows):
        pos = entry(tab, POS2 + 8 * side + u)
        values.append(dot3k(a_high[side, u], a_low[side, u], p_high[pos], p_low[pos]))
    for u in range(rows):
        labels = SIDE_LAB + 8 * side + 2 * entry(tab, POS2 + 8 * side + u)
        here.append(two_columns(values[u][:, :block], entry(tab, labels + 1 - side)))
        high, low = split(values[u][:, block:])
        label = entry(tab, labels + side)
        place = slice(u * block, (u + 1) * block)
        ap_high[place] = two_columns(high, label)
        ap_low[place] = two_columns(low, label)
    return here


def same_kernel(
    tab, a_high, a_low, trans_high, trans_low, far_0, group,
    own_part, ap_high, ap_low, out_1,
    p_high, p_low,
):
    half = trans_high.shape[0]
    block = half // 2
    side = pair_side()
    out_1[:, :half] = group[...]
    for j in range(far_0.shape[0]):
        p_high[j, :, :block], p_low[j, :, :block] = split(far_0[j, 1 - side])
        p_high[j, :, block:], p_low[j, :, block:] = split(far_0[j, side])
    here = far_columns(tab, side, a_high, a_low, p_high, p_low, ap_high, ap_low)
    for u, value in enumerate(here):
        own_part[u] = value
    out_1[:, half:] = coarse_group(trans_high, trans_low, ap_high, ap_low)


def own_part_kernel(early, tab, a01_high, a01_low, own, t, *refs):
    own_part, back_high, back_low, own_high, own_low = refs[-5:]
    rows = own.shape[0]
    side = 1 - pair_side()

    @pl.when(far_partner() == early)
    def _():
        for j in range(rows // 2):
            back_high[j], back_low[j] = split(t[entry(tab, BACK + (rows // 2) * side + j)])
        for u in range(rows):
            own_high[u], own_low[u] = split(own[u])
        for u in range(rows):
            near = entry(tab, NEAR + u)
            own_part[u] = dot3(a01_high[u], a01_low[u], wide(own_high, u, near), wide(own_low, u, near))


def second_kernel(
    tab, a_high, a_low, own_part, so_far, back_high, back_low, trans_high, trans_low, far_1,
    own_high, own_low, ap_high, ap_low, out_1,
    p_high, p_low,
):
    rows, block = own_part.shape[0], own_part.shape[1]
    half = 2 * block
    side = 1 - pair_side()
    towards = [dot3k(*split(far_1[j, 1 - side]), back_high[j], back_low[j]) for j in range(rows // 2)]
    for j in range(rows // 2):
        p_high[j, :, :block], p_low[j, :, :block] = split(towards[j])
        p_high[j, :, block:], p_low[j, :, block:] = split(far_1[j, side])
    here = far_columns(tab, side, a_high, a_low, p_high, p_low, ap_high, ap_low)
    for u in range(rows):
        place = slice(u * block, (u + 1) * block)
        own_high[place], own_low[place] = split(own_part[u] + so_far[u] + here[u])
    out_1[:, :half] = coarse_group(trans_high, trans_low, own_high, own_low)
    out_1[:, half:] = coarse_group(trans_high, trans_low, ap_high, ap_low)


def every_group(trans_high, trans_low, aps, out):
    half = trans_high.shape[0]
    for i in range(len(aps) // 2):
        out[:, i * half : (i + 1) * half] = coarse_group(trans_high, trans_low, aps[2 * i], aps[2 * i + 1])


def other_kernel(tab, far, *refs):
    aps, (out_0, trans_high, trans_low) = refs[:10], refs[10:]
    turn(tab, far, pair_side(), trans_high, trans_low)
    every_group(trans_high, trans_low, aps, out_0)


def own_kernel(early, own, *refs):
    aps, (out, trans_high, trans_low) = refs[:10], refs[-3:]
    rows, block = own.shape[0], own.shape[1]

    @pl.when(far_partner() != early)
    def _():
        for u in range(rows):
            place = slice(u * block, (u + 1) * block)
            high, low = split(own[u])
            trans_high[:, place] = high.T
            trans_low[:, place] = low.T
        every_group(trans_high, trans_low, aps, out)


def write_slots(inverse, totals, results, out, sems):
    block = inverse.shape[1]
    inv = [split(inverse[agg]) for agg in range(2)]
    values = [dot3k(*inv[agg], *split(total)) for agg, _, total in totals]
    copies = []
    for n, ((agg, d, _), value) in enumerate(zip(totals, values)):
        results[n, 0] = value[:, :block]
        results[n, 1] = value[:, block:]
        copies.append(pltpu.make_async_copy(results.at[n], out.at[agg, pl.ds(2 * (d + 3), 2)], sems.at[n]))
        copies[-1].start()
    for copy in copies:
        copy.wait()


OWN_AT, SAME_AT = (1, -1, 2, 0, -2), (0, 2, -1, 1, 3)
PARTS_AT = (-2, -3), (-1, 1), (0,)


def finish_kernel(offsets, part_at, inverse, own, *refs):
    refs, (out, results, sems) = refs[:-3], refs[-3:]
    others = ((refs[0], SAME_AT), (refs[1], part_at)) if len(refs) > 1 else ((refs[0], part_at),)
    block = inverse.shape[1]
    half = 2 * block
    side = pair_side()

    def run(way):
        done = []
        for agg in range(2):
            line = slice(agg * block, (agg + 1) * block)
            for d in offsets:
                places = [(ref, at.index(d)) for ref, at in ((own, OWN_AT), *others) if d in at]
                shares = [ref[line, i * half : (i + 1) * half] for ref, i in places]
                done.append((agg, way * d, sum(shares[1:], shares[0])))
        write_slots(inverse, done, results, out, sems)

    pl.when(side == ABOVE)(lambda: run(1))
    pl.when(side == BELOW)(lambda: run(-1))


VMEM = pl.BlockSpec(memory_space=pltpu.VMEM)
HBM = pl.BlockSpec(memory_space=pltpu.HBM)


def call(body, outs, ins, scratch=(), micros=1.0, in_hbm=(), out_hbm=(), aliases={}):
    def specs(values, in_place):
        return [HBM if i in in_place else VMEM for i, x in enumerate(values)]

    return pl.pallas_call(
        body,
        out_shape=outs,
        in_specs=specs(ins, in_hbm),
        out_specs=specs(outs, out_hbm),
        scratch_shapes=[pltpu.VMEM(*x) if isinstance(x, tuple) else x for x in scratch],
        input_output_aliases=aliases,
        compiler_params=pltpu.CompilerParams(vmem_limit_bytes=24 * 2**20),
        cost_estimate=pl.CostEstimate(flops=int(micros * 1e9), bytes_accessed=2**20, transcendentals=0),
    )(*ins)


def shards(a, a_cols, t_blocks, t_agg, dinv, coarse_inv):
    devices = lax.axis_size(AXES)
    rows, block = t_blocks.shape[:2]
    width, half, deep = rows // 2, 2 * block, rows * block
    shape = jax.ShapeDtypeStruct
    full = lambda *dims: shape(dims, F32)
    pair = lambda *dims: [shape(dims, BF16), shape(dims, BF16)]
    two = lambda *dims: [(dims, BF16)] * 2
    tile = full(width, block, half)
    cols = a_cols.reshape(-1, ROW_CHUNK, 4).transpose(0, 2, 1).reshape(-1)

    near_shapes = [tile, tile, full(rows, block, half)] + pair(2, rows, block, block) + pair(rows, block, half)
    tab, t_0, t_1, t, *near = call(
        functools.partial(load_kernel, devices),
        [shape((TAB, LANES), jnp.int32)] + [full(width, block, block)] * 2 + [full(*t_blocks.shape)] + near_shapes,
        [pltpu.with_memory_space_constraint(x, pltpu.HBM) for x in (cols, t_agg, t_blocks, dinv, a)],
        [
            pltpu.SMEM((3 * 4 * ROW_CHUNK,), jnp.int32),
            pltpu.SMEM(t_agg.shape, jnp.int32),
            pltpu.SMEM((8 * rows,), jnp.int32),
            (dinv.shape, F32),
            (a.shape, F32),
            pltpu.SemaphoreType.DMA((6 + rows,)),
        ],
        micros=3,
        in_hbm=(0, 1, 2, 3, 4),
    )
    t_0 = exchanged(t_0, 0)
    t_1 = exchanged(t_1, 1)
    near_0, near_1, own, a23_high, a23_low, a01_high, a01_low = call(
        near_kernel, near_shapes, [tab, a, t, dinv, *near], micros=2, aliases={4 + i: i for i in range(7)}
    )
    near_0 = exchanged(near_0, 0)
    sent = full(width, 2, block, block)
    far_1, t0_high, t0_low = call(
        far_sent_kernel, [sent] + pair(width, block, block), [tab, a23_high, a23_low, dinv, t_0], micros=2
    )
    got_far_1 = exchanged(far_1, 1)

    def own_share(early, done):
        return call(
            functools.partial(own_part_kernel, early),
            [full(rows, block, half)] + pair(width, block, block),
            [tab, a01_high, a01_low, own, t, *done],
            two(rows, block, half),
            micros=1,
            aliases={5 + i: i for i in range(len(done))},
        )

    share = own_share(True, [])
    near_1 = exchanged(near_1, 1)
    far_0, far = call(
        far_kernel,
        [sent, full(rows, 2, block, block)],
        [tab, a23_high, a23_low, dinv, t0_high, t0_low, t_1, far_1],
        two(2, width, block, block),
        micros=1,
    )
    far_0, far_1 = exchanged(far_0, 0), got_far_1
    out_high, out_low, part, ap_e1_high, ap_e1_low, group = call(
        mid_kernel,
        pair(half, deep) + [full(rows, block, half)] + pair(deep, half) + [full(half, half)],
        [tab, a01_high, a01_low, a23_high, a23_low, far, near_0],
        two(2, rows, block, half) + two(width, block, half),
        micros=2,
    )
    part_own, ap_e2_high, ap_e2_low, part_1 = call(
        same_kernel,
        [full(rows, block, half)] + pair(deep, half) + [full(half, 2 * half)],
        [tab, a23_high, a23_low, out_high, out_low, far_0, group],
        two(width, block, half),
        micros=1,
    )
    part_1 = exchanged(part_1, 1)
    share_own, back_high, back_low = own_share(False, share)
    ap_own_high, ap_own_low, ap_o2_high, ap_o2_low, part_2 = call(
        second_kernel,
        pair(deep, half) * 2 + [full(half, 2 * half)],
        [tab, a23_high, a23_low, share_own, part_own, back_high, back_low, out_high, out_low, far_1],
        two(width, block, half),
        micros=2,
    )
    part_2 = exchanged(part_2, 1)
    ap_o1_high, ap_o1_low, part_3 = call(
        first_kernel,
        pair(deep, half) + [full(half, half)],
        [tab, a23_high, a23_low, part, out_high, out_low, near_1],
        two(width, block, half),
        micros=2,
    )
    part_3 = exchanged(part_3, 1)
    aps = [
        ap_e1_high, ap_e1_low, ap_o1_high, ap_o1_low, ap_e2_high, ap_e2_low,
        ap_own_high, ap_own_low, ap_o2_high, ap_o2_low,
    ]
    (both_0,) = call(other_kernel, [full(half, 5 * half)], [tab, far] + aps, two(half, deep), micros=2)
    total = []
    for early in (True, False):
        total = call(
            functools.partial(own_kernel, early),
            [full(half, 5 * half)],
            [own] + aps + total,
            two(half, deep),
            micros=2,
            aliases={11: 0} if total else {},
        )
        total = list(total)
        if early:
            both_0 = exchanged(both_0, 0)
    (total,) = total
    out = []
    for i, (offsets, got) in enumerate((((-3, -2), part_1), ((-1, 1, 2, 3), part_2), ((0,), part_3))):
        n = 2 * len(offsets)
        out = call(
            functools.partial(finish_kernel, offsets, PARTS_AT[i]),
            [full(2, 14, block, block)],
            [coarse_inv, total] + ([both_0] if i else []) + [got, *out],
            [((n, 2, block, block), F32), pltpu.SemaphoreType.DMA((n,))],
            micros=1,
            in_hbm=(4,),
            out_hbm=(0,),
            aliases={4: 0} if i else {},
        )
    return out[0]


def solution(mesh):
    placed = (
        P(AXES, None, None, None),
        P(),
        P(AXES, None, None),
        P(),
        P(AXES, None, None),
        P(AXES, None, None),
    )
    return jax.shard_map(
        shards,
        mesh=mesh,
        in_specs=placed,
        out_specs=P(AXES, None, None, None),
        check_vma=False,
    )
```

```python
import functools

import jax
import jax.numpy as jnp
from jax import lax
from jax.experimental import pallas as pl
from jax.experimental.pallas import tpu as pltpu
from jax.sharding import PartitionSpec as P


OMEGA = 0.6
AXES = ("gx", "gy")
F32 = jnp.float32
BF16 = jnp.bfloat16
ROW, NEAR, POS2, POS3, LIST_0, OWN_LAB, SIDE_LAB, BACK, TAB = 0, 8, 16, 24, 32, 40, 72, 88, 96
LANES = 128
BELOW, ABOVE = 0, 1
ROW_CHUNK = 128


def exchanged(value, first):
    count = lax.axis_size(AXES)
    pairs = []
    for low in range(first, count + first, 2):
        high = (low + 1) % count
        pairs += [(low, high), (high, low)]
    return lax.ppermute(value, AXES, pairs)


def pair_side():
    return 1 - lax.rem(lax.axis_index("gy"), 2)


def split(x):
    high = x.astype(BF16)
    return high, (x - high.astype(F32)).astype(BF16)


def dot(a, b):
    return jnp.dot(a, b, preferred_element_type=F32)


def dot3(a_high, a_low, b_high, b_low):
    return dot(a_high, b_high) + dot(a_low, b_high) + dot(a_high, b_low)


def dot3k(a_high, a_low, b_high, b_low):
    both = jnp.concatenate([a_high, a_low], axis=1)
    return dot(both, jnp.concatenate([b_high, b_high], axis=0)) + dot(a_high, b_low)


def note(tab, i, value):
    tab[pl.ds(i, 1), :] = jnp.full((1, tab.shape[1]), value, jnp.int32)


def entry(tab, i):
    return tab[pl.ds(i, 1), :][0, 0]


def far_partner():
    return lax.axis_index("gy") == 0


def load_kernel(
    devices, cols_hbm, agg_hbm, t_hbm, dinv_hbm, a_hbm,
    tab, t_0, t_1, t, near_0, near_1, own, a_high, a_low, a01_high, a01_low, m_high, m_low,
    cols, agg, rank, dinv, a, sem,
):
    early = [
        pltpu.make_async_copy(dinv_hbm, dinv, sem.at[5]),
        pltpu.make_async_copy(a_hbm, a, sem.at[6]),
    ]

    rows, width = t.shape[0], t.shape[0] // 2
    device = lax.axis_index("gx") * lax.axis_size("gy") + lax.axis_index("gy")
    previous = lax.rem(device + devices - 1, devices)
    following = lax.rem(device + 1, devices)
    slabs = previous, following, device
    side = pair_side()
    shift = ROW_CHUNK.bit_length() - 1
    chunk = 4 * ROW_CHUNK
    copies = [
        pltpu.make_async_copy(
            cols_hbm.at[pl.ds(pl.multiple_of(((slab * rows) >> shift) * chunk, chunk), chunk)],
            cols.at[pl.ds(i * chunk, chunk)],
            sem.at[i],
        )
        for i, slab in enumerate(slabs)
    ]
    copies += [pltpu.make_async_copy(t_hbm, t, sem.at[3]), pltpu.make_async_copy(agg_hbm, agg, sem.at[4])]
    for copy in copies:
        copy.start()

    @pl.when(far_partner())
    def _():
        for copy in early:
            copy.start()

    def col(i, r, k):
        return cols[i * chunk + k * ROW_CHUNK + ((slabs[i] * rows) & (ROW_CHUNK - 1)) + r]

    def rank_rows(i, k, where):
        mask = jnp.int32(0)
        for r in range(rows):
            mask = mask | (jnp.int32(1) << (col(i, r, k) & (rows - 1)))
        named, other = jnp.int32(0), jnp.int32(width)
        for r in range(rows):
            hit = (mask >> r) & 1
            place = jnp.where(hit == 1, named, other)
            rank[where * rows + r] = place
            rank[(where + 1) * rows + place] = r
            named = named + hit
            other = other + 1 - hit

    def ranked(where, r):
        return rank[where * rows + r]

    copies[0].wait()
    copies[1].wait()
    rank_rows(0, 3, 0)
    rank_rows(1, 2, 2)
    sent_1, sent_0 = jnp.where(side == ABOVE, 0, 2), jnp.where(side == ABOVE, 2, 0)
    copies[3].wait()
    for j in range(width):
        t_1[j] = t[ranked(sent_1 + 1, j)]
        t_0[j] = t[ranked(sent_0 + 1, j)]
    copies[2].wait()
    copies[4].wait()
    rank_rows(2, 2, 4)
    rank_rows(2, 3, 6)
    for j in range(width):
        note(tab, LIST_0 + j, ranked(sent_1, ranked(sent_0 + 1, j)))
        for which in (BELOW, ABOVE):
            note(tab, BACK + width * which + j, col(which, ranked(5 + 2 * which, j), 3 - which) & (rows - 1))
            for k in range(2):
                note(tab, SIDE_LAB + 8 * which + 2 * j + k, agg[col(which, ranked(5 + 2 * which, j), 2 + k)])
    for u in range(rows):
        row = ranked(sent_1 + 1, u)
        note(tab, ROW + u, row)
        note(tab, NEAR + u, ranked(sent_1, col(2, row, 1) & (rows - 1)))
        note(tab, POS2 + u, ranked(4, col(2, row, 2) & (rows - 1)))
        note(tab, POS3 + u, ranked(6, col(2, row, 3) & (rows - 1)))
        for k in range(4):
            note(tab, OWN_LAB + 4 * u + k, agg[col(2, row, k)])

    @pl.when(far_partner())
    def _():
        for copy in early:
            copy.wait()
        near_blocks(tab, a, t, dinv, near_0, near_1, own, a_high, a_low, a01_high, a01_low, m_high, m_low)


def put(value, label, column):
    return jnp.where(label == column, value, jnp.zeros_like(value))


def two_columns(value, label):
    return jnp.concatenate([put(value, label, 0), put(value, label, 1)], axis=1)


def near_tiles(tab, a, t, dinv, order):
    block = t.shape[1]
    rows = [entry(tab, ROW + u) for u in order]
    prods = []
    for u, row in zip(order, rows):
        near = entry(tab, ROW + entry(tab, NEAR + u))
        prods.append(
            jnp.concatenate(
                [dot3k(*split(a[row, 0]), *split(t[row])), dot3k(*split(a[row, 1]), *split(t[near]))], axis=1
            )
        )
    tiles = []
    for u, row, prod in zip(order, rows, prods):
        smoothed = dot3k(*split(dinv[row]), *split(prod))
        p0 = t[row] - OMEGA * smoothed[:, :block]
        p1 = -OMEGA * smoothed[:, block:]
        tiles.append(two_columns(p0, entry(tab, OWN_LAB + 4 * u)) + two_columns(p1, entry(tab, OWN_LAB + 4 * u + 1)))
    return tiles


def wide(ref, *places):
    return jnp.concatenate([ref[place] for place in places], axis=0)


def near_blocks(tab, a, t, dinv, near_0, near_1, own, a_high, a_low, a01_high, a01_low, m_high, m_low):
    rows, width = own.shape[0], near_1.shape[0]
    for u, value in enumerate(near_tiles(tab, a, t, dinv, range(rows))):
        own[u] = value
        if u < width:
            near_1[u] = value
    for j in range(width):
        near_0[j] = own[entry(tab, LIST_0 + j)]
    for u in range(rows):
        row = entry(tab, ROW + u)
        a01_high[u], a01_low[u] = split(jnp.concatenate([a[row, 0], a[row, 1]], axis=1))
        for which in (BELOW, ABOVE):
            a_high[which, u], a_low[which, u] = split(a[row, 2 + which])
    makers = []
    for u in range(width):
        wide_high, wide_low = (jnp.concatenate([x[BELOW, u], x[ABOVE, u]], axis=1) for x in (a_high, a_low))
        makers.append(-OMEGA * dot3k(*split(dinv[entry(tab, ROW + u)]), wide_high, wide_low))
    block = t.shape[1]
    for u in range(width):
        for which in (BELOW, ABOVE):
            m_high[which, u], m_low[which, u] = split(makers[u][:, which * block : (which + 1) * block])


def near_kernel(tab, a, t, dinv, *refs):
    pl.when(jnp.logical_not(far_partner()))(lambda: near_blocks(tab, a, t, dinv, *refs[9:]))


def far_blocks(tab, a_high, a_low, dinv, t_high, t_low, order):
    prods = [
        jnp.concatenate(
            [
                dot3k(a_high[which, u], a_low[which, u], t_high[which, pos], t_low[which, pos])
                for which, pos in ((BELOW, entry(tab, POS2 + u)), (ABOVE, entry(tab, POS3 + u)))
            ],
            axis=1,
        )
        for u in order
    ]
    return [-OMEGA * dot3k(*split(dinv[entry(tab, ROW + u)]), *split(prod)) for u, prod in zip(order, prods)]


def split_rows(value, high, low):
    for j in range(value.shape[0]):
        high[j], low[j] = split(value[j])


def far_sent_kernel(tab, m_high, m_low, t_0, far_1, t_high, t_low):
    side = pair_side()
    split_rows(t_0, t_high, t_low)
    for u in range(far_1.shape[0]):
        pos = entry(tab, POS2 + 8 * side + u)
        far_1[u, side] = dot3k(m_high[side, u], m_low[side, u], t_high[pos], t_low[pos])
        far_1[u, 1 - side] = m_high[1 - side, u].astype(F32) + m_low[1 - side, u].astype(F32)


def store_turned(trans, label, place, value):
    block = value.shape[0]
    trans[pl.ds(pl.multiple_of(label * block, block), block), place] = value.T
    trans[pl.ds(pl.multiple_of((1 - label) * block, block), block), place] = jnp.zeros_like(value)


def turn(tab, far, side, trans_high, trans_low):
    for u in range(far.shape[0]):
        block = far.shape[2]
        label = entry(tab, OWN_LAB + 4 * u + 2 + side)
        high, low = split(far[u, side])
        place = slice(u * block, (u + 1) * block)
        store_turned(trans_high, label, place, high)
        store_turned(trans_low, label, place, low)


def coarse_group(trans_high, trans_low, ap_high, ap_low):
    return dot3(trans_high[...], trans_low[...], ap_high[...], ap_low[...])


def far_kernel(tab, a_high, a_low, dinv, t0_high, t0_low, t_1, far_1, far_0, far, t_high, t_low):
    rows, block = far.shape[0], far.shape[2]
    width = rows // 2
    side = pair_side()
    for j in range(width):
        t_high[side, j], t_low[side, j] = t0_high[j], t0_low[j]
        t_high[1 - side, j], t_low[1 - side, j] = split(t_1[j])
    for u in range(width):
        pos = entry(tab, POS2 + 8 * (1 - side) + u)
        far[u, side] = far_1[u, side]
        far[u, 1 - side] = dot3k(*split(far_1[u, 1 - side]), t_high[1 - side, pos], t_low[1 - side, pos])
    for u, both in enumerate(far_blocks(tab, a_high, a_low, dinv, t_high, t_low, range(width, rows))):
        far[width + u, BELOW] = both[:, :block]
        far[width + u, ABOVE] = both[:, block:]
    for j in range(width):
        far_0[j] = far[entry(tab, LIST_0 + j)]


def mid_kernel(
    tab, a01_high, a01_low, a_high, a_low, far, near_0,
    trans_high, trans_low, part, ap_high, ap_low, group,
    far_high, far_low, p_high, p_low,
):
    rows, block = far.shape[0], far.shape[2]
    side = pair_side()
    split_rows(near_0, p_high, p_low)
    for u in range(rows):
        for which in (BELOW, ABOVE):
            label = entry(tab, OWN_LAB + 4 * u + 2 + which)
            high, low = split(far[u, which])
            far_high[which, u] = two_columns(high, label)
            far_low[which, u] = two_columns(low, label)

    def mine(u, which):
        near = entry(tab, NEAR + u)
        return dot3(a01_high[u], a01_low[u], wide(far_high.at[which], u, near), wide(far_low.at[which], u, near))

    totals = []
    for u in range(rows):
        pos = entry(tab, POS2 + 8 * side + u)
        totals.append(mine(u, side) + dot3k(a_high[side, u], a_low[side, u], p_high[pos], p_low[pos]))
    for u in range(rows):
        place = slice(u * block, (u + 1) * block)
        ap_high[place], ap_low[place] = split(totals[u])
    turn(tab, far, 1 - side, trans_high, trans_low)
    for u in range(rows):
        part[u] = mine(u, 1 - side)
    group[...] = coarse_group(trans_high, trans_low, ap_high, ap_low)


def first_kernel(
    tab, a_high, a_low, part, trans_high, trans_low, near_1,
    ap_high, ap_low, out_1,
    p_high, p_low,
):
    rows, block = part.shape[0], part.shape[1]
    side = 1 - pair_side()
    split_rows(near_1, p_high, p_low)
    totals = []
    for u in range(rows):
        pos = entry(tab, POS2 + 8 * side + u)
        totals.append(part[u] + dot3k(a_high[side, u], a_low[side, u], p_high[pos], p_low[pos]))
    for u in range(rows):
        place = slice(u * block, (u + 1) * block)
        ap_high[place], ap_low[place] = split(totals[u])
    out_1[...] = coarse_group(trans_high, trans_low, ap_high, ap_low)


def far_columns(tab, side, a_high, a_low, p_high, p_low, ap_high, ap_low):
    rows, block = a_high.shape[1], a_high.shape[3]
    values, here = [], []
    for u in range(rows):
        pos = entry(tab, POS2 + 8 * side + u)
        values.append(dot3k(a_high[side, u], a_low[side, u], p_high[pos], p_low[pos]))
    for u in range(rows):
        labels = SIDE_LAB + 8 * side + 2 * entry(tab, POS2 + 8 * side + u)
        here.append(two_columns(values[u][:, :block], entry(tab, labels + 1 - side)))
        high, low = split(values[u][:, block:])
        label = entry(tab, labels + side)
        place = slice(u * block, (u + 1) * block)
        ap_high[place] = two_columns(high, label)
        ap_low[place] = two_columns(low, label)
    return here


def same_kernel(
    tab, a_high, a_low, trans_high, trans_low, far_0, group,
    own_part, ap_high, ap_low, out_1,
    p_high, p_low,
):
    half = trans_high.shape[0]
    block = half // 2
    side = pair_side()
    out_1[:, :half] = group[...]
    for j in range(far_0.shape[0]):
        p_high[j, :, :block], p_low[j, :, :block] = split(far_0[j, 1 - side])
        p_high[j, :, block:], p_low[j, :, block:] = split(far_0[j, side])
    here = far_columns(tab, side, a_high, a_low, p_high, p_low, ap_high, ap_low)
    for u, value in enumerate(here):
        own_part[u] = value
    out_1[:, half:] = coarse_group(trans_high, trans_low, ap_high, ap_low)


def own_part_kernel(early, tab, a01_high, a01_low, own, t, *refs):
    own_part, back_high, back_low, own_high, own_low = refs[-5:]
    rows = own.shape[0]
    side = 1 - pair_side()

    @pl.when(far_partner() == early)
    def _():
        for j in range(rows // 2):
            back_high[j], back_low[j] = split(t[entry(tab, BACK + (rows // 2) * side + j)])
        for u in range(rows):
            own_high[u], own_low[u] = split(own[u])
        for u in range(rows):
            near = entry(tab, NEAR + u)
            own_part[u] = dot3(a01_high[u], a01_low[u], wide(own_high, u, near), wide(own_low, u, near))


def second_kernel(
    tab, a_high, a_low, own_part, so_far, back_high, back_low, trans_high, trans_low, far_1,
    own_high, own_low, ap_high, ap_low, out_1,
    p_high, p_low,
):
    rows, block = own_part.shape[0], own_part.shape[1]
    half = 2 * block
    side = 1 - pair_side()
    towards = [dot3k(*split(far_1[j, 1 - side]), back_high[j], back_low[j]) for j in range(rows // 2)]
    for j in range(rows // 2):
        p_high[j, :, :block], p_low[j, :, :block] = split(towards[j])
        p_high[j, :, block:], p_low[j, :, block:] = split(far_1[j, side])
    here = far_columns(tab, side, a_high, a_low, p_high, p_low, ap_high, ap_low)
    for u in range(rows):
        place = slice(u * block, (u + 1) * block)
        own_high[place], own_low[place] = split(own_part[u] + so_far[u] + here[u])
    out_1[:, :half] = coarse_group(trans_high, trans_low, own_high, own_low)
    out_1[:, half:] = coarse_group(trans_high, trans_low, ap_high, ap_low)


def every_group(trans_high, trans_low, aps, out):
    half = trans_high.shape[0]
    for i in range(len(aps) // 2):
        out[:, i * half : (i + 1) * half] = coarse_group(trans_high, trans_low, aps[2 * i], aps[2 * i + 1])


def other_kernel(tab, far, *refs):
    aps, (out_0, trans_high, trans_low) = refs[:10], refs[10:]
    turn(tab, far, pair_side(), trans_high, trans_low)
    every_group(trans_high, trans_low, aps, out_0)


def own_kernel(early, own, *refs):
    aps, (out, trans_high, trans_low) = refs[:10], refs[-3:]
    rows, block = own.shape[0], own.shape[1]

    @pl.when(far_partner() != early)
    def _():
        for u in range(rows):
            place = slice(u * block, (u + 1) * block)
            high, low = split(own[u])
            trans_high[:, place] = high.T
            trans_low[:, place] = low.T
        every_group(trans_high, trans_low, aps, out)


def write_slots(inverse, totals, results, out, sems):
    block = inverse.shape[1]
    inv = [split(inverse[agg]) for agg in range(2)]
    values = [dot3k(*inv[agg], *split(total)) for agg, _, total in totals]
    copies = []
    for n, ((agg, d, _), value) in enumerate(zip(totals, values)):
        results[n, 0] = value[:, :block]
        results[n, 1] = value[:, block:]
        copies.append(pltpu.make_async_copy(results.at[n], out.at[agg, pl.ds(2 * (d + 3), 2)], sems.at[n]))
        copies[-1].start()
    for copy in copies:
        copy.wait()


OWN_AT, SAME_AT = (1, -1, 2, 0, -2), (0, 2, -1, 1, 3)
PARTS_AT = (-2, -3), (-1, 1), (0,)


def finish_kernel(offsets, part_at, inverse, own, *refs):
    refs, (out, results, sems) = refs[:-3], refs[-3:]
    others = ((refs[0], SAME_AT), (refs[1], part_at)) if len(refs) > 1 else ((refs[0], part_at),)
    block = inverse.shape[1]
    half = 2 * block
    side = pair_side()

    def run(way):
        done = []
        for agg in range(2):
            line = slice(agg * block, (agg + 1) * block)
            for d in offsets:
                places = [(ref, at.index(d)) for ref, at in ((own, OWN_AT), *others) if d in at]
                shares = [ref[line, i * half : (i + 1) * half] for ref, i in places]
                done.append((agg, way * d, sum(shares[1:], shares[0])))
        write_slots(inverse, done, results, out, sems)

    pl.when(side == ABOVE)(lambda: run(1))
    pl.when(side == BELOW)(lambda: run(-1))


VMEM = pl.BlockSpec(memory_space=pltpu.VMEM)
HBM = pl.BlockSpec(memory_space=pltpu.HBM)


def call(body, outs, ins, scratch=(), micros=1.0, in_hbm=(), out_hbm=(), aliases={}):
    def specs(values, in_place):
        return [HBM if i in in_place else VMEM for i, x in enumerate(values)]

    return pl.pallas_call(
        body,
        out_shape=outs,
        in_specs=specs(ins, in_hbm),
        out_specs=specs(outs, out_hbm),
        scratch_shapes=[pltpu.VMEM(*x) if isinstance(x, tuple) else x for x in scratch],
        input_output_aliases=aliases,
        compiler_params=pltpu.CompilerParams(vmem_limit_bytes=24 * 2**20),
        cost_estimate=pl.CostEstimate(flops=int(micros * 1e9), bytes_accessed=2**20, transcendentals=0),
    )(*ins)


def shards(a, a_cols, t_blocks, t_agg, dinv, coarse_inv):
    devices = lax.axis_size(AXES)
    rows, block = t_blocks.shape[:2]
    width, half, deep = rows // 2, 2 * block, rows * block
    shape = jax.ShapeDtypeStruct
    full = lambda *dims: shape(dims, F32)
    pair = lambda *dims: [shape(dims, BF16), shape(dims, BF16)]
    two = lambda *dims: [(dims, BF16)] * 2
    tile = full(width, block, half)
    cols = a_cols.reshape(-1, ROW_CHUNK, 4).transpose(0, 2, 1).reshape(-1)

    near_shapes = [tile, tile, full(rows, block, half)] + pair(2, rows, block, block) + pair(rows, block, half)
    near_shapes += pair(2, width, block, block)
    tab, t_0, t_1, t, *near = call(
        functools.partial(load_kernel, devices),
        [shape((TAB, LANES), jnp.int32)] + [full(width, block, block)] * 2 + [full(*t_blocks.shape)] + near_shapes,
        [pltpu.with_memory_space_constraint(x, pltpu.HBM) for x in (cols, t_agg, t_blocks, dinv, a)],
        [
            pltpu.SMEM((3 * 4 * ROW_CHUNK,), jnp.int32),
            pltpu.SMEM(t_agg.shape, jnp.int32),
            pltpu.SMEM((8 * rows,), jnp.int32),
            (dinv.shape, F32),
            (a.shape, F32),
            pltpu.SemaphoreType.DMA((7,)),
        ],
        micros=3,
        in_hbm=(0, 1, 2, 3, 4),
    )
    t_0 = exchanged(t_0, 0)
    t_1 = exchanged(t_1, 1)
    near_0, near_1, own, a23_high, a23_low, a01_high, a01_low, m_high, m_low = call(
        near_kernel, near_shapes, [tab, a, t, dinv, *near], micros=2, aliases={4 + i: i for i in range(9)}
    )
    near_0 = exchanged(near_0, 0)
    sent = full(width, 2, block, block)
    far_1, t0_high, t0_low = call(
        far_sent_kernel, [sent] + pair(width, block, block), [tab, m_high, m_low, t_0], micros=2
    )
    got_far_1 = exchanged(far_1, 1)

    def own_share(early, done):
        return call(
            functools.partial(own_part_kernel, early),
            [full(rows, block, half)] + pair(width, block, block),
            [tab, a01_high, a01_low, own, t, *done],
            two(rows, block, half),
            micros=1,
            aliases={5 + i: i for i in range(len(done))},
        )

    share = own_share(True, [])
    near_1 = exchanged(near_1, 1)
    far_0, far = call(
        far_kernel,
        [sent, full(rows, 2, block, block)],
        [tab, a23_high, a23_low, dinv, t0_high, t0_low, t_1, far_1],
        two(2, width, block, block),
        micros=1,
    )
    far_0, far_1 = exchanged(far_0, 0), got_far_1
    out_high, out_low, part, ap_e1_high, ap_e1_low, group = call(
        mid_kernel,
        pair(half, deep) + [full(rows, block, half)] + pair(deep, half) + [full(half, half)],
        [tab, a01_high, a01_low, a23_high, a23_low, far, near_0],
        two(2, rows, block, half) + two(width, block, half),
        micros=2,
    )
    part_own, ap_e2_high, ap_e2_low, part_1 = call(
        same_kernel,
        [full(rows, block, half)] + pair(deep, half) + [full(half, 2 * half)],
        [tab, a23_high, a23_low, out_high, out_low, far_0, group],
        two(width, block, half),
        micros=1,
    )
    part_1 = exchanged(part_1, 1)
    share_own, back_high, back_low = own_share(False, share)
    ap_own_high, ap_own_low, ap_o2_high, ap_o2_low, part_2 = call(
        second_kernel,
        pair(deep, half) * 2 + [full(half, 2 * half)],
        [tab, a23_high, a23_low, share_own, part_own, back_high, back_low, out_high, out_low, far_1],
        two(width, block, half),
        micros=2,
    )
    part_2 = exchanged(part_2, 1)
    ap_o1_high, ap_o1_low, part_3 = call(
        first_kernel,
        pair(deep, half) + [full(half, half)],
        [tab, a23_high, a23_low, part, out_high, out_low, near_1],
        two(width, block, half),
        micros=2,
    )
    part_3 = exchanged(part_3, 1)
    aps = [
        ap_e1_high, ap_e1_low, ap_o1_high, ap_o1_low, ap_e2_high, ap_e2_low,
        ap_own_high, ap_own_low, ap_o2_high, ap_o2_low,
    ]
    (both_0,) = call(other_kernel, [full(half, 5 * half)], [tab, far] + aps, two(half, deep), micros=2)
    total = []
    for early in (True, False):
        total = call(
            functools.partial(own_kernel, early),
            [full(half, 5 * half)],
            [own] + aps + total,
            two(half, deep),
            micros=2,
            aliases={11: 0} if total else {},
        )
        total = list(total)
        if early:
            both_0 = exchanged(both_0, 0)
    (total,) = total
    out = []
    for i, (offsets, got) in enumerate((((-3, -2), part_1), ((-1, 1, 2, 3), part_2), ((0,), part_3))):
        n = 2 * len(offsets)
        out = call(
            functools.partial(finish_kernel, offsets, PARTS_AT[i]),
            [full(2, 14, block, block)],
            [coarse_inv, total] + ([both_0] if i else []) + [got, *out],
            [((n, 2, block, block), F32), pltpu.SemaphoreType.DMA((n,))],
            micros=1,
            in_hbm=(4,),
            out_hbm=(0,),
            aliases={4: 0} if i else {},
        )
    return out[0]


def solution(mesh):
    placed = (
        P(AXES, None, None, None),
        P(),
        P(AXES, None, None),
        P(),
        P(AXES, None, None),
        P(AXES, None, None),
    )
    return jax.shard_map(
        shards,
        mesh=mesh,
        in_specs=placed,
        out_specs=P(AXES, None, None, None),
        check_vma=False,
    )
```

```python
import functools

import jax
import jax.numpy as jnp
from jax import lax
from jax.experimental import pallas as pl
from jax.experimental.pallas import tpu as pltpu
from jax.sharding import PartitionSpec as P


OMEGA = 0.6
AXES = ("gx", "gy")
F32 = jnp.float32
BF16 = jnp.bfloat16
ROW, NEAR, POS2, POS3, LIST_0, OWN_LAB, SIDE_LAB, BACK, TAB = 0, 8, 16, 24, 32, 40, 72, 88, 96
LANES = 128
BELOW, ABOVE = 0, 1
ROW_CHUNK = 128


def exchanged(value, first):
    count = lax.axis_size(AXES)
    pairs = []
    for low in range(first, count + first, 2):
        high = (low + 1) % count
        pairs += [(low, high), (high, low)]
    return lax.ppermute(value, AXES, pairs)


def pair_side():
    return 1 - lax.rem(lax.axis_index("gy"), 2)


def split(x):
    high = x.astype(BF16)
    return high, (x - high.astype(F32)).astype(BF16)


def dot(a, b):
    return jnp.dot(a, b, preferred_element_type=F32)


def dot3(a_high, a_low, b_high, b_low):
    return dot(a_high, b_high) + dot(a_low, b_high) + dot(a_high, b_low)


def dot3k(a_high, a_low, b_high, b_low):
    both = jnp.concatenate([a_high, a_low], axis=1)
    return dot(both, jnp.concatenate([b_high, b_high], axis=0)) + dot(a_high, b_low)


def note(tab, i, value):
    tab[pl.ds(i, 1), :] = jnp.full((1, tab.shape[1]), value, jnp.int32)


def entry(tab, i):
    return tab[pl.ds(i, 1), :][0, 0]


def far_partner():
    return lax.axis_index("gy") == 0


def load_kernel(
    devices, cols_hbm, agg_hbm, t_hbm, dinv_hbm, a_hbm,
    tab, t_0, t_1, t, near_0, near_1, own, a_high, a_low, a01_high, a01_low, m_high, m_low,
    cols, agg, rank, dinv, a, sem,
):
    early = [
        pltpu.make_async_copy(dinv_hbm, dinv, sem.at[5]),
        pltpu.make_async_copy(a_hbm, a, sem.at[6]),
    ]

    rows, width = t.shape[0], t.shape[0] // 2
    device = lax.axis_index("gx") * lax.axis_size("gy") + lax.axis_index("gy")
    previous = lax.rem(device + devices - 1, devices)
    following = lax.rem(device + 1, devices)
    slabs = previous, following, device
    side = pair_side()
    shift = ROW_CHUNK.bit_length() - 1
    chunk = 4 * ROW_CHUNK
    copies = [
        pltpu.make_async_copy(
            cols_hbm.at[pl.ds(pl.multiple_of(((slab * rows) >> shift) * chunk, chunk), chunk)],
            cols.at[pl.ds(i * chunk, chunk)],
            sem.at[i],
        )
        for i, slab in enumerate(slabs)
    ]
    copies += [pltpu.make_async_copy(t_hbm, t, sem.at[3]), pltpu.make_async_copy(agg_hbm, agg, sem.at[4])]
    for copy in copies:
        copy.start()

    @pl.when(far_partner())
    def _():
        for copy in early:
            copy.start()

    def col(i, r, k):
        return cols[i * chunk + k * ROW_CHUNK + ((slabs[i] * rows) & (ROW_CHUNK - 1)) + r]

    def rank_rows(i, k, where):
        mask = jnp.int32(0)
        for r in range(rows):
            mask = mask | (jnp.int32(1) << (col(i, r, k) & (rows - 1)))
        named, other = jnp.int32(0), jnp.int32(width)
        for r in range(rows):
            hit = (mask >> r) & 1
            place = jnp.where(hit == 1, named, other)
            rank[where * rows + r] = place
            rank[(where + 1) * rows + place] = r
            named = named + hit
            other = other + 1 - hit

    def ranked(where, r):
        return rank[where * rows + r]

    copies[0].wait()
    copies[1].wait()
    rank_rows(0, 3, 0)
    rank_rows(1, 2, 2)
    sent_1, sent_0 = jnp.where(side == ABOVE, 0, 2), jnp.where(side == ABOVE, 2, 0)
    copies[3].wait()
    for j in range(width):
        t_1[j] = t[ranked(sent_1 + 1, j)]
        t_0[j] = t[ranked(sent_0 + 1, j)]
    copies[2].wait()
    copies[4].wait()
    rank_rows(2, 2, 4)
    rank_rows(2, 3, 6)
    for j in range(width):
        note(tab, LIST_0 + j, ranked(sent_1, ranked(sent_0 + 1, j)))
        for which in (BELOW, ABOVE):
            note(tab, BACK + width * which + j, col(which, ranked(5 + 2 * which, j), 3 - which) & (rows - 1))
            for k in range(2):
                note(tab, SIDE_LAB + 8 * which + 2 * j + k, agg[col(which, ranked(5 + 2 * which, j), 2 + k)])
    for u in range(rows):
        row = ranked(sent_1 + 1, u)
        note(tab, ROW + u, row)
        note(tab, NEAR + u, ranked(sent_1, col(2, row, 1) & (rows - 1)))
        note(tab, POS2 + u, ranked(4, col(2, row, 2) & (rows - 1)))
        note(tab, POS3 + u, ranked(6, col(2, row, 3) & (rows - 1)))
        for k in range(4):
            note(tab, OWN_LAB + 4 * u + k, agg[col(2, row, k)])

    @pl.when(far_partner())
    def _():
        for copy in early:
            copy.wait()
        near_blocks(tab, a, t, dinv, near_0, near_1, own, a_high, a_low, a01_high, a01_low, m_high, m_low)


def put(value, label, column):
    return jnp.where(label == column, value, jnp.zeros_like(value))


def two_columns(value, label):
    return jnp.concatenate([put(value, label, 0), put(value, label, 1)], axis=1)


def near_tiles(tab, a, t, dinv, order):
    block = t.shape[1]
    rows = [entry(tab, ROW + u) for u in order]
    prods = []
    for u, row in zip(order, rows):
        near = entry(tab, ROW + entry(tab, NEAR + u))
        prods.append(
            jnp.concatenate(
                [dot3k(*split(a[row, 0]), *split(t[row])), dot3k(*split(a[row, 1]), *split(t[near]))], axis=1
            )
        )
    tiles = []
    for u, row, prod in zip(order, rows, prods):
        smoothed = dot3k(*split(dinv[row]), *split(prod))
        p0 = t[row] - OMEGA * smoothed[:, :block]
        p1 = -OMEGA * smoothed[:, block:]
        tiles.append(two_columns(p0, entry(tab, OWN_LAB + 4 * u)) + two_columns(p1, entry(tab, OWN_LAB + 4 * u + 1)))
    return tiles


def wide(ref, *places):
    return jnp.concatenate([ref[place] for place in places], axis=0)


def near_blocks(tab, a, t, dinv, near_0, near_1, own, a_high, a_low, a01_high, a01_low, m_high, m_low):
    rows, width = own.shape[0], near_1.shape[0]
    for u, value in enumerate(near_tiles(tab, a, t, dinv, range(rows))):
        own[u] = value
        if u < width:
            near_1[u] = value
    for j in range(width):
        near_0[j] = own[entry(tab, LIST_0 + j)]
    for u in range(rows):
        row = entry(tab, ROW + u)
        a01_high[u], a01_low[u] = split(jnp.concatenate([a[row, 0], a[row, 1]], axis=1))
        for which in (BELOW, ABOVE):
            a_high[which, u], a_low[which, u] = split(a[row, 2 + which])
    makers = []
    for u in range(width):
        wide_high, wide_low = (jnp.concatenate([x[BELOW, u], x[ABOVE, u]], axis=1) for x in (a_high, a_low))
        makers.append(-OMEGA * dot3k(*split(dinv[entry(tab, ROW + u)]), wide_high, wide_low))
    block = t.shape[1]
    for u in range(width):
        for which in (BELOW, ABOVE):
            m_high[which, u], m_low[which, u] = split(makers[u][:, which * block : (which + 1) * block])


def near_kernel(tab, a, t, dinv, *refs):
    pl.when(jnp.logical_not(far_partner()))(lambda: near_blocks(tab, a, t, dinv, *refs[9:]))


def far_blocks(tab, a_high, a_low, dinv, t_high, t_low, order):
    prods = [
        jnp.concatenate(
            [
                dot3k(a_high[which, u], a_low[which, u], t_high[which, pos], t_low[which, pos])
                for which, pos in ((BELOW, entry(tab, POS2 + u)), (ABOVE, entry(tab, POS3 + u)))
            ],
            axis=1,
        )
        for u in order
    ]
    return [-OMEGA * dot3k(*split(dinv[entry(tab, ROW + u)]), *split(prod)) for u, prod in zip(order, prods)]


def split_rows(value, high, low):
    for j in range(value.shape[0]):
        high[j], low[j] = split(value[j])


def far_sent_kernel(tab, m_high, m_low, t_0, far_1, t_high, t_low):
    side = pair_side()
    split_rows(t_0, t_high, t_low)
    for u in range(far_1.shape[0]):
        pos = entry(tab, POS2 + 8 * side + u)
        far_1[u, side] = dot3k(m_high[side, u], m_low[side, u], t_high[pos], t_low[pos])
        far_1[u, 1 - side] = m_high[1 - side, u].astype(F32) + m_low[1 - side, u].astype(F32)


def store_turned(trans, label, place, value):
    block = value.shape[0]
    trans[pl.ds(pl.multiple_of(label * block, block), block), place] = value.T
    trans[pl.ds(pl.multiple_of((1 - label) * block, block), block), place] = jnp.zeros_like(value)


def turn(tab, far, side, trans_high, trans_low):
    for u in range(far.shape[0]):
        block = far.shape[2]
        label = entry(tab, OWN_LAB + 4 * u + 2 + side)
        high, low = split(far[u, side])
        place = slice(u * block, (u + 1) * block)
        store_turned(trans_high, label, place, high)
        store_turned(trans_low, label, place, low)


def coarse_group(trans_high, trans_low, ap_high, ap_low):
    return dot3(trans_high[...], trans_low[...], ap_high[...], ap_low[...])


def far_kernel(tab, a_high, a_low, dinv, t0_high, t0_low, t_1, far_1, far_0, far, t_high, t_low):
    rows, block = far.shape[0], far.shape[2]
    width = rows // 2
    side = pair_side()
    for j in range(width):
        t_high[side, j], t_low[side, j] = t0_high[j], t0_low[j]
        t_high[1 - side, j], t_low[1 - side, j] = split(t_1[j])
    for u in range(width):
        pos = entry(tab, POS2 + 8 * (1 - side) + u)
        far[u, side] = far_1[u, side]
        far[u, 1 - side] = dot3k(*split(far_1[u, 1 - side]), t_high[1 - side, pos], t_low[1 - side, pos])
    for u, both in enumerate(far_blocks(tab, a_high, a_low, dinv, t_high, t_low, range(width, rows))):
        far[width + u, BELOW] = both[:, :block]
        far[width + u, ABOVE] = both[:, block:]
    for j in range(width):
        far_0[j] = far[entry(tab, LIST_0 + j)]


def mid_kernel(
    tab, a01_high, a01_low, a_high, a_low, far, near_0,
    trans_high, trans_low, away_high, away_low, ap_high, ap_low, group,
    far_high, far_low, p_high, p_low,
):
    rows, block = far.shape[0], far.shape[2]
    side = pair_side()
    split_rows(near_0, p_high, p_low)
    for u in range(rows):
        for which, high_ref, low_ref in ((side, far_high, far_low), (1 - side, away_high, away_low)):
            label = entry(tab, OWN_LAB + 4 * u + 2 + which)
            high, low = split(far[u, which])
            high_ref[u] = two_columns(high, label)
            low_ref[u] = two_columns(low, label)

    def mine(u):
        near = entry(tab, NEAR + u)
        return dot3(a01_high[u], a01_low[u], wide(far_high, u, near), wide(far_low, u, near))

    totals = []
    for u in range(rows):
        pos = entry(tab, POS2 + 8 * side + u)
        totals.append(mine(u) + dot3k(a_high[side, u], a_low[side, u], p_high[pos], p_low[pos]))
    for u in range(rows):
        place = slice(u * block, (u + 1) * block)
        ap_high[place], ap_low[place] = split(totals[u])
    turn(tab, far, 1 - side, trans_high, trans_low)
    group[...] = coarse_group(trans_high, trans_low, ap_high, ap_low)


def first_kernel(
    tab, a01_high, a01_low, a_high, a_low, away_high, away_low, trans_high, trans_low, near_1,
    ap_high, ap_low, out_1,
    p_high, p_low,
):
    rows, block = away_high.shape[0], away_high.shape[1]
    side = 1 - pair_side()
    split_rows(near_1, p_high, p_low)
    totals = []
    for u in range(rows):
        pos = entry(tab, POS2 + 8 * side + u)
        near = entry(tab, NEAR + u)
        mine = dot3(a01_high[u], a01_low[u], wide(away_high, u, near), wide(away_low, u, near))
        totals.append(mine + dot3k(a_high[side, u], a_low[side, u], p_high[pos], p_low[pos]))
    for u in range(rows):
        place = slice(u * block, (u + 1) * block)
        ap_high[place], ap_low[place] = split(totals[u])
    out_1[...] = coarse_group(trans_high, trans_low, ap_high, ap_low)


def far_columns(tab, side, a_high, a_low, p_high, p_low, ap_high, ap_low):
    rows, block = a_high.shape[1], a_high.shape[3]
    values, here = [], []
    for u in range(rows):
        pos = entry(tab, POS2 + 8 * side + u)
        values.append(dot3k(a_high[side, u], a_low[side, u], p_high[pos], p_low[pos]))
    for u in range(rows):
        labels = SIDE_LAB + 8 * side + 2 * entry(tab, POS2 + 8 * side + u)
        here.append(two_columns(values[u][:, :block], entry(tab, labels + 1 - side)))
        high, low = split(values[u][:, block:])
        label = entry(tab, labels + side)
        place = slice(u * block, (u + 1) * block)
        ap_high[place] = two_columns(high, label)
        ap_low[place] = two_columns(low, label)
    return here


def same_kernel(
    tab, a_high, a_low, trans_high, trans_low, far_0, group,
    own_part, ap_high, ap_low, out_1,
    p_high, p_low,
):
    half = trans_high.shape[0]
    block = half // 2
    side = pair_side()
    out_1[:, :half] = group[...]
    for j in range(far_0.shape[0]):
        p_high[j, :, :block], p_low[j, :, :block] = split(far_0[j, 1 - side])
        p_high[j, :, block:], p_low[j, :, block:] = split(far_0[j, side])
    here = far_columns(tab, side, a_high, a_low, p_high, p_low, ap_high, ap_low)
    for u, value in enumerate(here):
        own_part[u] = value
    out_1[:, half:] = coarse_group(trans_high, trans_low, ap_high, ap_low)


def own_part_kernel(early, tab, a01_high, a01_low, own, t, *refs):
    own_part, back_high, back_low, own_high, own_low = refs[-5:]
    rows = own.shape[0]
    side = 1 - pair_side()

    @pl.when(far_partner() == early)
    def _():
        for j in range(rows // 2):
            back_high[j], back_low[j] = split(t[entry(tab, BACK + (rows // 2) * side + j)])
        for u in range(rows):
            own_high[u], own_low[u] = split(own[u])
        for u in range(rows):
            near = entry(tab, NEAR + u)
            own_part[u] = dot3(a01_high[u], a01_low[u], wide(own_high, u, near), wide(own_low, u, near))


def second_kernel(
    tab, a_high, a_low, own_part, so_far, back_high, back_low, trans_high, trans_low, far_1,
    own_high, own_low, ap_high, ap_low, out_1,
    p_high, p_low,
):
    rows, block = own_part.shape[0], own_part.shape[1]
    half = 2 * block
    side = 1 - pair_side()
    towards = [dot3k(*split(far_1[j, 1 - side]), back_high[j], back_low[j]) for j in range(rows // 2)]
    for j in range(rows // 2):
        p_high[j, :, :block], p_low[j, :, :block] = split(towards[j])
        p_high[j, :, block:], p_low[j, :, block:] = split(far_1[j, side])
    here = far_columns(tab, side, a_high, a_low, p_high, p_low, ap_high, ap_low)
    for u in range(rows):
        place = slice(u * block, (u + 1) * block)
        own_high[place], own_low[place] = split(own_part[u] + so_far[u] + here[u])
    out_1[:, :half] = coarse_group(trans_high, trans_low, own_high, own_low)
    out_1[:, half:] = coarse_group(trans_high, trans_low, ap_high, ap_low)


def every_group(trans_high, trans_low, aps, out):
    half = trans_high.shape[0]
    for i in range(len(aps) // 2):
        out[:, i * half : (i + 1) * half] = coarse_group(trans_high, trans_low, aps[2 * i], aps[2 * i + 1])


def other_kernel(tab, far, *refs):
    aps, (out_0, trans_high, trans_low) = refs[:10], refs[10:]
    turn(tab, far, pair_side(), trans_high, trans_low)
    every_group(trans_high, trans_low, aps, out_0)


def own_kernel(early, own, *refs):
    aps, (out, trans_high, trans_low) = refs[:10], refs[-3:]
    rows, block = own.shape[0], own.shape[1]

    @pl.when(far_partner() != early)
    def _():
        for u in range(rows):
            place = slice(u * block, (u + 1) * block)
            high, low = split(own[u])
            trans_high[:, place] = high.T
            trans_low[:, place] = low.T
        every_group(trans_high, trans_low, aps, out)


def write_slots(inverse, totals, results, out, sems):
    block = inverse.shape[1]
    inv = [split(inverse[agg]) for agg in range(2)]
    values = [dot3k(*inv[agg], *split(total)) for agg, _, total in totals]
    copies = []
    for n, ((agg, d, _), value) in enumerate(zip(totals, values)):
        results[n, 0] = value[:, :block]
        results[n, 1] = value[:, block:]
        copies.append(pltpu.make_async_copy(results.at[n], out.at[agg, pl.ds(2 * (d + 3), 2)], sems.at[n]))
        copies[-1].start()
    for copy in copies:
        copy.wait()


OWN_AT, SAME_AT = (1, -1, 2, 0, -2), (0, 2, -1, 1, 3)
PARTS_AT = (-2, -3), (-1, 1), (0,)


def finish_kernel(offsets, part_at, inverse, own, *refs):
    refs, (out, results, sems) = refs[:-3], refs[-3:]
    others = ((refs[0], SAME_AT), (refs[1], part_at)) if len(refs) > 1 else ((refs[0], part_at),)
    block = inverse.shape[1]
    half = 2 * block
    side = pair_side()

    def run(way):
        done = []
        for agg in range(2):
            line = slice(agg * block, (agg + 1) * block)
            for d in offsets:
                places = [(ref, at.index(d)) for ref, at in ((own, OWN_AT), *others) if d in at]
                shares = [ref[line, i * half : (i + 1) * half] for ref, i in places]
                done.append((agg, way * d, sum(shares[1:], shares[0])))
        write_slots(inverse, done, results, out, sems)

    pl.when(side == ABOVE)(lambda: run(1))
    pl.when(side == BELOW)(lambda: run(-1))


VMEM = pl.BlockSpec(memory_space=pltpu.VMEM)
HBM = pl.BlockSpec(memory_space=pltpu.HBM)


def call(body, outs, ins, scratch=(), micros=1.0, in_hbm=(), out_hbm=(), aliases={}):
    def specs(values, in_place):
        return [HBM if i in in_place else VMEM for i, x in enumerate(values)]

    return pl.pallas_call(
        body,
        out_shape=outs,
        in_specs=specs(ins, in_hbm),
        out_specs=specs(outs, out_hbm),
        scratch_shapes=[pltpu.VMEM(*x) if isinstance(x, tuple) else x for x in scratch],
        input_output_aliases=aliases,
        compiler_params=pltpu.CompilerParams(vmem_limit_bytes=24 * 2**20),
        cost_estimate=pl.CostEstimate(flops=int(micros * 1e9), bytes_accessed=2**20, transcendentals=0),
    )(*ins)


def shards(a, a_cols, t_blocks, t_agg, dinv, coarse_inv):
    devices = lax.axis_size(AXES)
    rows, block = t_blocks.shape[:2]
    width, half, deep = rows // 2, 2 * block, rows * block
    shape = jax.ShapeDtypeStruct
    full = lambda *dims: shape(dims, F32)
    pair = lambda *dims: [shape(dims, BF16), shape(dims, BF16)]
    two = lambda *dims: [(dims, BF16)] * 2
    tile = full(width, block, half)
    cols = a_cols.reshape(-1, ROW_CHUNK, 4).transpose(0, 2, 1).reshape(-1)

    near_shapes = [tile, tile, full(rows, block, half)] + pair(2, rows, block, block) + pair(rows, block, half)
    near_shapes += pair(2, width, block, block)
    tab, t_0, t_1, t, *near = call(
        functools.partial(load_kernel, devices),
        [shape((TAB, LANES), jnp.int32)] + [full(width, block, block)] * 2 + [full(*t_blocks.shape)] + near_shapes,
        [pltpu.with_memory_space_constraint(x, pltpu.HBM) for x in (cols, t_agg, t_blocks, dinv, a)],
        [
            pltpu.SMEM((3 * 4 * ROW_CHUNK,), jnp.int32),
            pltpu.SMEM(t_agg.shape, jnp.int32),
            pltpu.SMEM((8 * rows,), jnp.int32),
            (dinv.shape, F32),
            (a.shape, F32),
            pltpu.SemaphoreType.DMA((7,)),
        ],
        micros=3,
        in_hbm=(0, 1, 2, 3, 4),
    )
    t_0 = exchanged(t_0, 0)
    t_1 = exchanged(t_1, 1)
    near_0, near_1, own, a23_high, a23_low, a01_high, a01_low, m_high, m_low = call(
        near_kernel, near_shapes, [tab, a, t, dinv, *near], micros=2, aliases={4 + i: i for i in range(9)}
    )
    near_0 = exchanged(near_0, 0)
    sent = full(width, 2, block, block)
    far_1, t0_high, t0_low = call(
        far_sent_kernel, [sent] + pair(width, block, block), [tab, m_high, m_low, t_0], micros=2
    )
    got_far_1 = exchanged(far_1, 1)

    def own_share(early, done):
        return call(
            functools.partial(own_part_kernel, early),
            [full(rows, block, half)] + pair(width, block, block),
            [tab, a01_high, a01_low, own, t, *done],
            two(rows, block, half),
            micros=1,
            aliases={5 + i: i for i in range(len(done))},
        )

    share = own_share(True, [])
    near_1 = exchanged(near_1, 1)
    far_0, far = call(
        far_kernel,
        [sent, full(rows, 2, block, block)],
        [tab, a23_high, a23_low, dinv, t0_high, t0_low, t_1, far_1],
        two(2, width, block, block),
        micros=1,
    )
    far_0, far_1 = exchanged(far_0, 0), got_far_1
    out_high, out_low, away_high, away_low, ap_e1_high, ap_e1_low, group = call(
        mid_kernel,
        pair(half, deep) + pair(rows, block, half) + pair(deep, half) + [full(half, half)],
        [tab, a01_high, a01_low, a23_high, a23_low, far, near_0],
        two(rows, block, half) + two(width, block, half),
        micros=2,
    )
    part_own, ap_e2_high, ap_e2_low, part_1 = call(
        same_kernel,
        [full(rows, block, half)] + pair(deep, half) + [full(half, 2 * half)],
        [tab, a23_high, a23_low, out_high, out_low, far_0, group],
        two(width, block, half),
        micros=1,
    )
    part_1 = exchanged(part_1, 1)
    share_own, back_high, back_low = own_share(False, share)
    ap_own_high, ap_own_low, ap_o2_high, ap_o2_low, part_2 = call(
        second_kernel,
        pair(deep, half) * 2 + [full(half, 2 * half)],
        [tab, a23_high, a23_low, share_own, part_own, back_high, back_low, out_high, out_low, far_1],
        two(width, block, half),
        micros=2,
    )
    part_2 = exchanged(part_2, 1)
    ap_o1_high, ap_o1_low, part_3 = call(
        first_kernel,
        pair(deep, half) + [full(half, half)],
        [tab, a01_high, a01_low, a23_high, a23_low, away_high, away_low, out_high, out_low, near_1],
        two(width, block, half),
        micros=2,
    )
    part_3 = exchanged(part_3, 1)
    aps = [
        ap_e1_high, ap_e1_low, ap_o1_high, ap_o1_low, ap_e2_high, ap_e2_low,
        ap_own_high, ap_own_low, ap_o2_high, ap_o2_low,
    ]
    (both_0,) = call(other_kernel, [full(half, 5 * half)], [tab, far] + aps, two(half, deep), micros=2)
    total = []
    for early in (True, False):
        total = call(
            functools.partial(own_kernel, early),
            [full(half, 5 * half)],
            [own] + aps + total,
            two(half, deep),
            micros=2,
            aliases={11: 0} if total else {},
        )
        total = list(total)
        if early:
            both_0 = exchanged(both_0, 0)
    (total,) = total
    out = []
    for i, (offsets, got) in enumerate((((-3, -2), part_1), ((-1, 1, 2, 3), part_2), ((0,), part_3))):
        n = 2 * len(offsets)
        out = call(
            functools.partial(finish_kernel, offsets, PARTS_AT[i]),
            [full(2, 14, block, block)],
            [coarse_inv, total] + ([both_0] if i else []) + [got, *out],
            [((n, 2, block, block), F32), pltpu.SemaphoreType.DMA((n,))],
            micros=1,
            in_hbm=(4,),
            out_hbm=(0,),
            aliases={4: 0} if i else {},
        )
    return out[0]


def solution(mesh):
    placed = (
        P(AXES, None, None, None),
        P(),
        P(AXES, None, None),
        P(),
        P(AXES, None, None),
        P(AXES, None, None),
    )
    return jax.shard_map(
        shards,
        mesh=mesh,
        in_specs=placed,
        out_specs=P(AXES, None, None, None),
        check_vma=False,
    )
```
